16 devices in a mesh: dp: 2 (over z), fsdp: 8 (over y, x, core).
Axes of the slice: x: 2, y: 2, z: 2, core: 2. Of those that a mesh axis runs over, the one named last changes fastest.
Arguments:
- emb_grad: float32 [2, 8, 2048, 5376], P('dp', 'fsdp')
- mat_grad: float32 [2, 8, 1024, 5376], P('dp', 'fsdp')
- norm_grad: float32 [2, 8, 9, 5376], P('dp', 'fsdp')
- emb_param: float32 [2048, 5376], P('fsdp')
- emb_mom: float32 [2048, 5376], P('fsdp')
- emb_var: float32 [2048, 5376], P('fsdp')
- mat_param: float32 [1024, 5376], P('fsdp')
- mat_mom: float32 [1024, 5376], P('fsdp')
- mat_var: float32 [1024, 5376], P('fsdp')
- norm_param: float32 [9, 5376], P(None, 'fsdp')
- norm_mom: float32 [9, 5376], P(None, 'fsdp')
- norm_var: float32 [9, 5376], P(None, 'fsdp')
Outputs:
- output 1: float32 [2048, 5376], P('fsdp')
- output 2: float32 [2048, 5376], P('fsdp')
- output 3: float32 [2048, 5376], P('fsdp')
- output 4: bfloat16 [2048, 5376], P('fsdp')
- output 5: float32 [1024, 5376], P('fsdp')
- output 6: float32 [1024, 5376], P('fsdp')
- output 7: float32 [1024, 5376], P('fsdp')
- output 8: bfloat16 [1024, 5376], P('fsdp')
- output 9: float32 [9, 5376], P(None, 'fsdp')
- output 10: float32 [9, 5376], P(None, 'fsdp')
- output 11: float32 [9, 5376], P(None, 'fsdp')
- output 12: bfloat16 [9, 5376], P(None, 'fsdp')
All inputs are finite; a program needn't handle non-finite values.
Results may differ from the reference program's by a relative error of at most 0.001.
Values sent between devices are 32-bit elements.
A program may use at most 1 GiB of HBM per device.

```python
import math
import jax
import jax.numpy as jnp

DP_SIZE = 2
FSDP_SIZE = 8
WIDTH = 5376
EMB_ROWS = 256
MAT_ROWS = 128
NORM_COUNT = 9
ADAM_STEP = 10

LEARN_RATE = 0.003
BETA_ONE = 0.9
BETA_TWO = 0.95
ADAM_EPS = 1e-8
WEIGHT_DECAY = 0.1
CLIP_NORM = 1.0

DEV_COUNT = DP_SIZE * FSDP_SIZE
VOCAB_ROWS = FSDP_SIZE * EMB_ROWS
MATRIX_ROWS = FSDP_SIZE * MAT_ROWS
TOTAL_PARAMS = (VOCAB_ROWS + MATRIX_ROWS + NORM_COUNT) * WIDTH


def setup_inputs(seed: int = 0) -> dict:
    key_list = jax.random.split(jax.random.key(seed), 12)
    grad_unit = 2.0 / math.sqrt(TOTAL_PARAMS)
    spread = math.sqrt(DEV_COUNT)
    mom_unit = 0.5 * grad_unit
    row_frac = jnp.arange(VOCAB_ROWS, dtype=jnp.float32) / VOCAB_ROWS
    emb_scale = (2.0 / jnp.sqrt(1.0 + 15.0 * row_frac))[:, None]
    weight_scale = WIDTH ** -0.5
    emb_shape = (VOCAB_ROWS, WIDTH)
    mat_shape = (MATRIX_ROWS, WIDTH)
    norm_shape = (NORM_COUNT, WIDTH)
    dev_lead = (DP_SIZE, FSDP_SIZE)
    return {
        "emb_grad": spread * grad_unit * emb_scale * jax.random.normal(key_list[0], dev_lead + emb_shape, jnp.float32),
        "mat_grad": spread * grad_unit * jax.random.normal(key_list[1], dev_lead + mat_shape, jnp.float32),
        "norm_grad": spread * grad_unit * jax.random.normal(key_list[2], dev_lead + norm_shape, jnp.float32),
        "emb_param": weight_scale * jax.random.normal(key_list[3], emb_shape, jnp.float32),
        "emb_mom": 0.1 * mom_unit * emb_scale * jax.random.normal(key_list[4], emb_shape, jnp.float32),
        "emb_var": 0.05 * (mom_unit * emb_scale) ** 2 * jax.random.uniform(key_list[5], emb_shape, jnp.float32, 0.5, 1.5),
        "mat_param": weight_scale * jax.random.normal(key_list[6], mat_shape, jnp.float32),
        "mat_mom": 0.1 * mom_unit * jax.random.normal(key_list[7], mat_shape, jnp.float32),
        "mat_var": 0.05 * mom_unit ** 2 * jax.random.uniform(key_list[8], mat_shape, jnp.float32, 0.5, 1.5),
        "norm_param": 0.1 * jax.random.normal(key_list[9], norm_shape, jnp.float32),
        "norm_mom": 0.1 * mom_unit * jax.random.normal(key_list[10], norm_shape, jnp.float32),
        "norm_var": 0.05 * mom_unit ** 2 * jax.random.uniform(key_list[11], norm_shape, jnp.float32, 0.5, 1.5),
    }


def adamw_update(grad_part, param_old, mom_old, var_old, decay_rate):
    new_mom = BETA_ONE * mom_old + (1.0 - BETA_ONE) * grad_part
    new_var = BETA_TWO * var_old + (1.0 - BETA_TWO) * grad_part * grad_part
    mom_hat = new_mom / (1.0 - BETA_ONE ** ADAM_STEP)
    var_hat = new_var / (1.0 - BETA_TWO ** ADAM_STEP)
    step_dir = mom_hat / (jnp.sqrt(var_hat) + ADAM_EPS)
    new_param = param_old - LEARN_RATE * (step_dir + decay_rate * param_old)
    return new_param, new_mom, new_var, new_param.astype(jnp.bfloat16)


def reference(emb_grad, mat_grad, norm_grad, emb_param, emb_mom, emb_var, mat_param, mat_mom, mat_var, norm_param, norm_mom, norm_var):
    emb_mean = jnp.sum(emb_grad, axis=(0, 1)) / DEV_COUNT
    mat_mean = jnp.sum(mat_grad, axis=(0, 1)) / DEV_COUNT
    norm_mean = jnp.sum(norm_grad, axis=(0, 1)) / DEV_COUNT
    total_sq = jnp.sum(emb_mean * emb_mean) + jnp.sum(mat_mean * mat_mean) + jnp.sum(norm_mean * norm_mean)
    clip_scale = jnp.minimum(1.0, CLIP_NORM / jnp.sqrt(total_sq))
    emb_p, emb_m, emb_v, emb_b = adamw_update(emb_mean * clip_scale, emb_param, emb_mom, emb_var, WEIGHT_DECAY)
    mat_p, mat_m, mat_v, mat_b = adamw_update(mat_mean * clip_scale, mat_param, mat_mom, mat_var, WEIGHT_DECAY)
    norm_p, norm_m, norm_v, norm_b = adamw_update(norm_mean * clip_scale, norm_param, norm_mom, norm_var, 0.0)
    return (emb_p, emb_m, emb_v, emb_b, mat_p, mat_m, mat_v, mat_b, norm_p, norm_m, norm_v, norm_b)
```

```python
import functools

import jax
import jax.numpy as jnp
from jax import lax
from jax.experimental import pallas as pl
from jax.experimental.pallas import tpu as pltpu
from jax.sharding import PartitionSpec as P

LEARN_RATE = 0.003
BETA_ONE = 0.9
BETA_TWO = 0.95
ADAM_EPS = 1e-8
WEIGHT_DECAY = 0.1
CLIP_NORM = 1.0
ADAM_STEP = 10

MESH = pl.DeviceIdType.MESH
F32 = jnp.float32

WIDTH = 5376
NORM_ROWS = 9
NORM_COLS = 672
NORM_PAD = (16, 768)
ROWS = 8
SPLIT = 2688
LAG_ZERO = 3
LAG = 2
P_SLOTS = 8
R_SLOTS = 6
SEND_SLOTS = 8


def reduce_kernel(counts, emb, mat, norm, emb_out, mat_out, norm_out, scale_out,
                  part, recv_zero, xa, xb, ya, yb, grad, square,
                  norm_in, norm_part, norm_a, norm_b, norm_c, norm_d, sum_send, sum_recv,
                  load_sem, zero_send, zero_recv, credit,
                  a_send, b_send, xa_recv, xb_recv, ya_send, yb_send, ya_recv, yb_recv,
                  za_send, zb_send, za_recv, zb_recv, out_sem,
                  norm_load, norm_send, norm_recv, norm_store, sum_ssem, sum_rsem, scale_sem):
    emb_count, mat_count = counts
    total = emb_count + mat_count
    z = lax.axis_index("dp")
    f = lax.axis_index("fsdp")
    c = lax.rem(f, 2)
    x = lax.rem(lax.div(f, 2), 2)
    y = lax.div(f, 4)
    core = (z, f + 1 - 2 * c)
    xn = (z, f + 2 - 4 * x)
    yn = (z, f + 4 - 8 * y)
    zn = (1 - z, f)

    def remote(src, dst, ssem, rsem, dev):
        return pltpu.make_async_remote_copy(src_ref=src, dst_ref=dst, send_sem=ssem, recv_sem=rsem,
                                            device_id=dev, device_id_type=MESH)

    barrier = pltpu.get_barrier_semaphore()
    for dev in (core, xn, yn, zn):
        pl.semaphore_signal(barrier, inc=1, device_id=dev, device_id_type=MESH)
    norm_copy = pltpu.make_async_copy(norm, norm_in, norm_load)
    norm_copy.start()
    norm_part[...] = jnp.zeros_like(norm_part)
    square[...] = jnp.zeros_like(square)
    norm_copy.wait()
    for k in range(8):
        norm_part[k // 4, (k // 2) % 2, k % 2, :NORM_ROWS, :NORM_COLS] = norm_in[:, k * NORM_COLS:(k + 1) * NORM_COLS]
    pl.semaphore_wait(barrier, 4)

    def on_rows(j, body):
        @pl.when(j < emb_count)
        def _():
            body(emb, emb_out, pl.multiple_of(j * ROWS, ROWS))

        @pl.when(j >= emb_count)
        def _():
            body(mat, mat_out, pl.multiple_of((j - emb_count) * ROWS, ROWS))

    def load_copy(ref, row, j):
        return pltpu.make_async_copy(ref.at[:, :, c, pl.ds(row, ROWS), :], part.at[lax.rem(j, P_SLOTS)],
                                     load_sem.at[lax.rem(j, P_SLOTS)])

    def zero_copy(ref, row, j):
        return remote(ref.at[:, :, 1 - c, pl.ds(row, ROWS), :], recv_zero.at[lax.rem(j, R_SLOTS)],
                      zero_send.at[lax.rem(j, R_SLOTS)], zero_recv.at[lax.rem(j, R_SLOTS)], core)

    def a_one(j):
        s = lax.rem(j, P_SLOTS)
        return remote(part.at[s, :, 1 - x, :, :SPLIT], xa.at[j], a_send.at[s], xa_recv.at[j], xn)

    def b_one(j):
        s = lax.rem(j, P_SLOTS)
        return remote(part.at[s, 1 - y, :, :, SPLIT:], xb.at[j], b_send.at[s], xb_recv.at[j], yn)

    def a_two(j):
        s = lax.rem(j, SEND_SLOTS)
        return remote(xa.at[j, 1 - y], ya.at[j], ya_send.at[s], ya_recv.at[j], yn)

    def b_two(j):
        s = lax.rem(j, SEND_SLOTS)
        return remote(xb.at[j, 1 - x], yb.at[j], yb_send.at[s], yb_recv.at[j], xn)

    def a_three(j):
        s = lax.rem(j, SEND_SLOTS)
        return remote(ya.at[j], grad.at[j, :, :SPLIT], za_send.at[s], za_recv.at[j], zn)

    def b_three(j):
        s = lax.rem(j, SEND_SLOTS)
        return remote(yb.at[j], grad.at[j, :, SPLIT:], zb_send.at[s], zb_recv.at[j], zn)

    def out_copy(ref, row, j):
        return pltpu.make_async_copy(grad.at[j], ref.at[pl.ds(row, ROWS), :], out_sem.at[lax.rem(j, SEND_SLOTS)])

    norm_zero = remote(norm_part.at[:, :, 1 - c], norm_a, norm_send.at[0], norm_recv.at[0], core)
    norm_one = remote(norm_a.at[:, 1 - x], norm_b, norm_send.at[1], norm_recv.at[1], xn)
    norm_two = remote(norm_b.at[1 - y], norm_c, norm_send.at[2], norm_recv.at[2], yn)
    norm_three = remote(norm_c, norm_d, norm_send.at[3], norm_recv.at[3], zn)
    norm_zero.start()

    def when_in(j, body):
        pl.when(jnp.logical_and(j >= 0, j < total))(functools.partial(body, j))

    def stage_issue(j):
        @pl.when(j >= P_SLOTS)
        def _():
            a_one(j - P_SLOTS).wait_send()
            b_one(j - P_SLOTS).wait_send()

        @pl.when(j >= R_SLOTS)
        def _():
            zero_copy(emb, 0, j - R_SLOTS).wait_send()
            pl.semaphore_wait(credit, 1)

        def body(ref, _, row):
            zero_copy(ref, row, j).start()
            load_copy(ref, row, j).start()

        on_rows(j, body)

    def stage_one(j):
        load_copy(emb, 0, j).wait()
        zero_copy(emb, 0, j).wait_recv()
        s = lax.rem(j, P_SLOTS)
        part[s] += recv_zero[lax.rem(j, R_SLOTS)]

        @pl.when(j + R_SLOTS < total)
        def _():
            pl.semaphore_signal(credit, inc=1, device_id=core, device_id_type=MESH)

        a_one(j).start()
        b_one(j).start()

    def stage_two(j):
        s = lax.rem(j, P_SLOTS)
        a_one(j).wait_recv()
        xa[j] += part[s, :, x, :, :SPLIT]
        b_one(j).wait_recv()
        xb[j] += part[s, y, :, :, SPLIT:]

        @pl.when(j >= SEND_SLOTS)
        def _():
            a_two(j - SEND_SLOTS).wait_send()
            b_two(j - SEND_SLOTS).wait_send()

        a_two(j).start()
        b_two(j).start()

    def stage_three(j):
        a_two(j).wait_recv()
        ya[j] += xa[j, y]
        b_two(j).wait_recv()
        yb[j] += xb[j, x]

        @pl.when(j >= SEND_SLOTS)
        def _():
            a_three(j - SEND_SLOTS).wait_send()
            b_three(j - SEND_SLOTS).wait_send()

        a_three(j).start()
        b_three(j).start()

    def stage_four(j):
        a_three(j).wait_recv()
        b_three(j).wait_recv()
        left = (grad[j, :, :SPLIT] + ya[j]) * (1.0 / 16.0)
        right = (grad[j, :, SPLIT:] + yb[j]) * (1.0 / 16.0)
        grad[j, :, :SPLIT] = left
        grad[j, :, SPLIT:] = right
        square[:, :SPLIT] += left * left
        square[:, SPLIT:] += right * right

        @pl.when(j >= SEND_SLOTS)
        def _():
            out_copy(emb_out, 0, j - SEND_SLOTS).wait()

        def body(_, ref, row):
            out_copy(ref, row, j).start()

        on_rows(j, body)

    def trip(it, carry):
        when_in(it, stage_issue)
        when_in(it - LAG_ZERO, stage_one)
        when_in(it - LAG_ZERO - LAG, stage_two)
        when_in(it - LAG_ZERO - 2 * LAG, stage_three)
        when_in(it - LAG_ZERO - 3 * LAG, stage_four)

        @pl.when(it == 4)
        def _():
            norm_zero.wait_recv()
            norm_a[...] += norm_part[:, :, c]
            norm_one.start()

        @pl.when(it == 8)
        def _():
            norm_one.wait_recv()
            norm_b[...] += norm_a[:, x]
            norm_two.start()

        @pl.when(it == 12)
        def _():
            norm_two.wait_recv()
            norm_c[...] += norm_b[y]
            norm_three.start()

        @pl.when(it == 16)
        def _():
            norm_three.wait_recv()
            norm_d[...] = (norm_d[...] + norm_c[...]) * (1.0 / 16.0)
            pltpu.make_async_copy(norm_d, norm_out, norm_store).start()

        return carry

    lax.fori_loop(0, total + LAG_ZERO + 3 * LAG, trip, 0)

    norm_sq = norm_d[...] * norm_d[...]
    local = jnp.sum(square[...]) + jnp.sum(norm_sq)
    value = jnp.full((8, 128), local, F32)
    for k, dev in enumerate((core, xn, yn)):
        sum_send[k] = value
        copy = remote(sum_send.at[k], sum_recv.at[k], sum_ssem.at[k], sum_rsem.at[k], dev)
        copy.start()
        copy.wait_recv()
        value = value + sum_recv[k]
    sum_send[3] = jnp.minimum(1.0, CLIP_NORM / jnp.sqrt(value))
    scale_copy = pltpu.make_async_copy(sum_send.at[3], scale_out, scale_sem)
    scale_copy.start()

    for k, dev in enumerate((core, xn, yn)):
        remote(sum_send.at[k], sum_recv.at[k], sum_ssem.at[k], sum_rsem.at[k], dev).wait_send()
    for copy in (norm_zero, norm_one, norm_two, norm_three):
        copy.wait_send()
    pltpu.make_async_copy(norm_d, norm_out, norm_store).wait()

    def drain(slots, copies):
        def body(j, carry):
            for copy in copies:
                copy(j).wait_send()
            return carry
        lax.fori_loop(total - slots, total, body, 0)

    drain(P_SLOTS, (a_one, b_one))
    drain(R_SLOTS, (functools.partial(zero_copy, emb, 0),))
    drain(SEND_SLOTS, (a_two, b_two, a_three, b_three))

    def last(j, carry):
        out_copy(emb_out, 0, j).wait()
        return carry

    lax.fori_loop(total - SEND_SLOTS, total, last, 0)
    scale_copy.wait()


def reduce_grads(emb_grad, mat_grad, norm_grad):
    emb_rows = emb_grad.shape[0] // 8
    mat_rows = mat_grad.shape[0] // 8
    counts = (emb_rows // ROWS, mat_rows // ROWS)
    total = sum(counts)
    dma = pltpu.SemaphoreType.DMA
    scratch = [
        pltpu.VMEM((P_SLOTS, 2, 2, ROWS, WIDTH), F32),
        pltpu.VMEM((R_SLOTS, 2, 2, ROWS, WIDTH), F32),
        pltpu.VMEM((total, 2, ROWS, SPLIT), F32),
        pltpu.VMEM((total, 2, ROWS, WIDTH - SPLIT), F32),
        pltpu.VMEM((total, ROWS, SPLIT), F32),
        pltpu.VMEM((total, ROWS, WIDTH - SPLIT), F32),
        pltpu.VMEM((total, ROWS, WIDTH), F32),
        pltpu.VMEM((ROWS, WIDTH), F32),
        pltpu.VMEM((NORM_ROWS, WIDTH), F32),
        pltpu.VMEM((2, 2, 2) + NORM_PAD, F32),
        pltpu.VMEM((2, 2) + NORM_PAD, F32),
        pltpu.VMEM((2,) + NORM_PAD, F32),
        pltpu.VMEM(NORM_PAD, F32),
        pltpu.VMEM(NORM_PAD, F32),
        pltpu.VMEM((4, 8, 128), F32),
        pltpu.VMEM((3, 8, 128), F32),
        dma((P_SLOTS,)), dma((R_SLOTS,)), dma((R_SLOTS,)), pltpu.SemaphoreType.REGULAR,
        dma((P_SLOTS,)), dma((P_SLOTS,)), dma((total,)), dma((total,)),
        dma((SEND_SLOTS,)), dma((SEND_SLOTS,)), dma((total,)), dma((total,)),
        dma((SEND_SLOTS,)), dma((SEND_SLOTS,)), dma((total,)), dma((total,)), dma((SEND_SLOTS,)),
        dma, dma((4,)), dma((4,)), dma, dma((3,)), dma((3,)), dma,
    ]
    hbm = pl.BlockSpec(memory_space=pl.ANY)
    return pl.pallas_call(
        functools.partial(reduce_kernel, counts),
        out_shape=(
            jax.ShapeDtypeStruct((emb_rows, WIDTH), F32),
            jax.ShapeDtypeStruct((mat_rows, WIDTH), F32),
            jax.ShapeDtypeStruct(NORM_PAD, F32),
            jax.ShapeDtypeStruct((8, 128), F32),
        ),
        in_specs=[hbm] * 3,
        out_specs=(hbm,) * 4,
        scratch_shapes=scratch,
        compiler_params=pltpu.CompilerParams(
            collective_id=0, has_side_effects=True, vmem_limit_bytes=50 * 1024 * 1024
        ),
        name="reduce_grads",
    )(emb_grad.reshape(2, 2, 2, emb_rows, WIDTH), mat_grad.reshape(2, 2, 2, mat_rows, WIDTH), norm_grad)


def adamw_update(grad_part, param_old, mom_old, var_old, decay_rate):
    new_mom = BETA_ONE * mom_old + (1.0 - BETA_ONE) * grad_part
    new_var = BETA_TWO * var_old + (1.0 - BETA_TWO) * grad_part * grad_part
    mom_hat = new_mom / (1.0 - BETA_ONE ** ADAM_STEP)
    var_hat = new_var / (1.0 - BETA_TWO ** ADAM_STEP)
    step_dir = mom_hat / (jnp.sqrt(var_hat) + ADAM_EPS)
    new_param = param_old - LEARN_RATE * (step_dir + decay_rate * param_old)
    return (new_param, new_mom, new_var, new_param.astype(jnp.bfloat16))


def solution(mesh):
    def local_step(emb_grad, mat_grad, norm_grad, emb_param, emb_mom, emb_var, mat_param, mat_mom, mat_var, norm_param, norm_mom, norm_var):
        emb_mean, mat_mean, norm_mean, scale = reduce_grads(emb_grad[0, 0], mat_grad[0, 0], norm_grad[0, 0])
        clip_scale = scale[0, 0]
        emb_out = adamw_update(emb_mean * clip_scale, emb_param, emb_mom, emb_var, WEIGHT_DECAY)
        mat_out = adamw_update(mat_mean * clip_scale, mat_param, mat_mom, mat_var, WEIGHT_DECAY)
        norm_out = adamw_update(norm_mean[:NORM_ROWS, :NORM_COLS] * clip_scale, norm_param, norm_mom, norm_var, 0.0)
        return emb_out + mat_out + norm_out

    grad_spec = P("dp", "fsdp", None, None)
    row_spec = P("fsdp", None)
    col_spec = P(None, "fsdp")
    in_list = (grad_spec, grad_spec, grad_spec, row_spec, row_spec, row_spec, row_spec, row_spec, row_spec, col_spec, col_spec, col_spec)
    out_list = (row_spec, row_spec, row_spec, row_spec, row_spec, row_spec, row_spec, row_spec, col_spec, col_spec, col_spec, col_spec)
    return jax.shard_map(local_step, mesh=mesh, in_specs=in_list, out_specs=out_list, check_vma=False)
```

```python
import functools

import jax
import jax.numpy as jnp
from jax import lax
from jax.experimental import pallas as pl
from jax.experimental.pallas import tpu as pltpu
from jax.sharding import PartitionSpec as P

LEARN_RATE = 0.003
BETA_ONE = 0.9
BETA_TWO = 0.95
ADAM_EPS = 1e-8
WEIGHT_DECAY = 0.1
CLIP_NORM = 1.0
ADAM_STEP = 10

MESH = pl.DeviceIdType.MESH
F32 = jnp.float32

WIDTH = 5376
NORM_ROWS = 9
NORM_COLS = 672
NORM_PAD = (16, 768)
ROWS = 8
A_COLS = 2176
B_COLS = 2176
HALF = 256
B_AT = A_COLS
C_AT = A_COLS + B_COLS
D_AT = C_AT + 2 * HALF
LAG_ZERO = 3
LAG = 2
P_SLOTS = 8
R_SLOTS = 6
SEND_SLOTS = 8
RING = 16


def reduce_kernel(counts, emb, mat, norm, emb_out, mat_out, norm_out, scale_out,
                  part, recv_zero, xa, yb, zc, zd, ya, xb, xc, yd, yc, xd, grad, square,
                  norm_in, norm_part, norm_a, norm_b, norm_c, norm_d, sum_send, sum_recv, scale,
                  load_sem, zero_send, zero_recv, credit,
                  one_send, one_recv, two_send, two_recv, three_send, three_recv, four_send, four_recv, out_sem,
                  norm_load, norm_send, norm_recv, norm_store, sum_ssem, sum_rsem, scale_sem):
    emb_count, mat_count = counts
    total = emb_count + mat_count
    z = lax.axis_index("dp")
    f = lax.axis_index("fsdp")
    c = lax.rem(f, 2)
    x = lax.rem(lax.div(f, 2), 2)
    y = lax.div(f, 4)
    core = (z, f + 1 - 2 * c)
    xn = (z, f + 2 - 4 * x)
    yn = (z, f + 4 - 8 * y)
    zn = (1 - z, f)
    peers = [(z, lax.rem(f + k, 8)) for k in range(1, 8)]

    def remote(src, dst, ssem, rsem, dev):
        return pltpu.make_async_remote_copy(src_ref=src, dst_ref=dst, send_sem=ssem, recv_sem=rsem,
                                            device_id=dev, device_id_type=MESH)

    def half_at(base, which):
        return pl.ds(pl.multiple_of(base + which * HALF, 128), HALF)

    c_keep, c_give = half_at(C_AT, z), half_at(C_AT, 1 - z)
    d_keep, d_give = half_at(D_AT, z), half_at(D_AT, 1 - z)
    a_cols, b_cols = pl.ds(0, A_COLS), pl.ds(B_AT, B_COLS)

    barrier = pltpu.get_barrier_semaphore()
    for dev in peers + [zn]:
        pl.semaphore_signal(barrier, inc=1, device_id=dev, device_id_type=MESH)
    norm_copy = pltpu.make_async_copy(norm, norm_in, norm_load)
    norm_copy.start()

    def on_rows(j, body):
        @pl.when(j < emb_count)
        def _():
            body(emb, emb_out, pl.multiple_of(j * ROWS, ROWS))

        @pl.when(j >= emb_count)
        def _():
            body(mat, mat_out, pl.multiple_of((j - emb_count) * ROWS, ROWS))

    def load_copy(ref, row, j):
        s = lax.rem(j, P_SLOTS)
        return pltpu.make_async_copy(ref.at[:, :, c, pl.ds(row, ROWS), :], part.at[s], load_sem.at[s])

    def zero_copy(ref, row, j):
        s = lax.rem(j, R_SLOTS)
        return remote(ref.at[:, :, 1 - c, pl.ds(row, ROWS), :], recv_zero.at[s], zero_send.at[s], zero_recv.at[s], core)

    def ones(j):
        s, r = lax.rem(j, P_SLOTS), lax.rem(j, RING)
        return (remote(part.at[s, :, :, :, c_give], zc.at[r], one_send.at[2, s], one_recv.at[2, r], zn),
                remote(part.at[s, :, :, :, d_give], zd.at[r], one_send.at[3, s], one_recv.at[3, r], zn),
                remote(part.at[s, :, 1 - x, :, a_cols], xa.at[r], one_send.at[0, s], one_recv.at[0, r], xn),
                remote(part.at[s, 1 - y, :, :, b_cols], yb.at[r], one_send.at[1, s], one_recv.at[1, r], yn))

    def twos(j):
        s, r = lax.rem(j, SEND_SLOTS), lax.rem(j, RING)
        return (remote(zc.at[r, :, 1 - x], xc.at[r], two_send.at[2, s], two_recv.at[2, r], xn),
                remote(zd.at[r, 1 - y], yd.at[r], two_send.at[3, s], two_recv.at[3, r], yn),
                remote(xa.at[r, 1 - y], ya.at[r], two_send.at[0, s], two_recv.at[0, r], yn),
                remote(yb.at[r, 1 - x], xb.at[r], two_send.at[1, s], two_recv.at[1, r], xn))

    def threes(j):
        s, r = lax.rem(j, SEND_SLOTS), lax.rem(j, RING)
        return (remote(xc.at[r, 1 - y], yc.at[r], three_send.at[2, s], three_recv.at[2, r], yn),
                remote(yd.at[r, 1 - x], xd.at[r], three_send.at[3, s], three_recv.at[3, r], xn),
                remote(ya.at[r], grad.at[r, :, a_cols], three_send.at[0, s], three_recv.at[0, r], zn),
                remote(xb.at[r], grad.at[r, :, b_cols], three_send.at[1, s], three_recv.at[1, r], zn))

    def fours(j, c_at, d_at):
        s, r = lax.rem(j, SEND_SLOTS), lax.rem(j, RING)
        return (remote(grad.at[r, :, c_at], grad.at[r, :, c_at], four_send.at[0, s], four_recv.at[0, r], zn),
                remote(grad.at[r, :, d_at], grad.at[r, :, d_at], four_send.at[1, s], four_recv.at[1, r], zn))

    def out_copy(ref, row, j):
        return pltpu.make_async_copy(grad.at[lax.rem(j, RING)], ref.at[pl.ds(row, ROWS), :],
                                     out_sem.at[lax.rem(j, SEND_SLOTS)])

    norm_zero = remote(norm_part.at[:, :, 1 - c], norm_a, norm_send.at[0], norm_recv.at[0], core)
    norm_one = remote(norm_a.at[:, 1 - x], norm_b, norm_send.at[1], norm_recv.at[1], xn)
    norm_two = remote(norm_b.at[1 - y], norm_c, norm_send.at[2], norm_recv.at[2], yn)
    norm_three = remote(norm_c, norm_d, norm_send.at[3], norm_recv.at[3], zn)

    def when_in(j, body):
        pl.when(jnp.logical_and(j >= 0, j < total))(functools.partial(body, j))

    def start(copies):
        for copy in copies:
            copy.start()

    def wait_send(copies):
        for copy in copies:
            copy.wait_send()

    def stage_issue(j):
        @pl.when(j >= P_SLOTS)
        def _():
            wait_send(ones(j - P_SLOTS))

        @pl.when(j >= R_SLOTS)
        def _():
            zero_copy(emb, 0, j - R_SLOTS).wait_send()
            pl.semaphore_wait(credit, 1)

        def body(ref, _, row):
            zero_copy(ref, row, j).start()
            load_copy(ref, row, j).start()

        on_rows(j, body)

    def stage_one(j):
        load_copy(emb, 0, j).wait()
        zero_copy(emb, 0, j).wait_recv()
        part[lax.rem(j, P_SLOTS)] += recv_zero[lax.rem(j, R_SLOTS)]

        @pl.when(j + R_SLOTS < total)
        def _():
            pl.semaphore_signal(credit, inc=1, device_id=core, device_id_type=MESH)

        start(ones(j))

    def stage_two(j):
        s, r = lax.rem(j, P_SLOTS), lax.rem(j, RING)
        for copy in ones(j):
            copy.wait_recv()
        zc[r] += part[s, :, :, :, c_keep]
        zd[r] += part[s, :, :, :, d_keep]
        xa[r] += part[s, :, x, :, a_cols]
        yb[r] += part[s, y, :, :, b_cols]

        @pl.when(j >= SEND_SLOTS)
        def _():
            wait_send(twos(j - SEND_SLOTS))

        start(twos(j))

    def stage_three(j):
        r = lax.rem(j, RING)
        for copy in twos(j):
            copy.wait_recv()
        xc[r] += zc[r, :, x]
        yd[r] += zd[r, y]
        ya[r] += xa[r, y]
        xb[r] += yb[r, x]

        @pl.when(j >= SEND_SLOTS)
        def _():
            wait_send(threes(j - SEND_SLOTS))

        start(threes(j))

    def stage_four(j):
        r = lax.rem(j, RING)
        for copy in threes(j):
            copy.wait_recv()

        @pl.when(j >= SEND_SLOTS)
        def _():
            wait_send(fours(j - SEND_SLOTS, c_keep, d_keep))

        grad[r, :, c_keep] = (yc[r] + xc[r, y]) * (1.0 / 16.0)
        grad[r, :, d_keep] = (xd[r] + yd[r, x]) * (1.0 / 16.0)
        left = (grad[r, :, a_cols] + ya[r]) * (1.0 / 16.0)
        right = (grad[r, :, b_cols] + xb[r]) * (1.0 / 16.0)
        grad[r, :, a_cols] = left
        grad[r, :, b_cols] = right
        square[:, a_cols] += left * left
        square[:, b_cols] += right * right
        start(fours(j, c_keep, d_keep))

    def stage_five(j):
        r = lax.rem(j, RING)
        for copy in fours(j, c_give, d_give):
            copy.wait_recv()
        rest = grad[r, :, C_AT:]
        square[:, C_AT:] += rest * rest

        @pl.when(j >= SEND_SLOTS)
        def _():
            out_copy(emb_out, 0, j - SEND_SLOTS).wait()

        def body(_, ref, row):
            out_copy(ref, row, j).start()

        on_rows(j, body)

    def trip(it, carry):
        when_in(it, stage_issue)
        when_in(it - LAG_ZERO, stage_one)
        when_in(it - LAG_ZERO - LAG, stage_two)
        when_in(it - LAG_ZERO - 2 * LAG, stage_three)
        when_in(it - LAG_ZERO - 3 * LAG, stage_four)
        when_in(it - LAG_ZERO - 4 * LAG, stage_five)

        @pl.when(it == 5)
        def _():
            norm_copy.wait()
            for k in range(8):
                norm_part[k // 4, (k // 2) % 2, k % 2, :NORM_ROWS, :NORM_COLS] = norm_in[:, k * NORM_COLS:(k + 1) * NORM_COLS]
            norm_zero.start()

        @pl.when(it == 8)
        def _():
            norm_zero.wait_recv()
            norm_a[...] += norm_part[:, :, c]
            norm_one.start()

        @pl.when(it == 12)
        def _():
            norm_one.wait_recv()
            norm_b[...] += norm_a[:, x]
            norm_two.start()

        @pl.when(it == 16)
        def _():
            norm_two.wait_recv()
            norm_c[...] += norm_b[y]
            norm_three.start()

        @pl.when(it == 20)
        def _():
            norm_three.wait_recv()
            norm_d[...] = (norm_d[...] + norm_c[...]) * (1.0 / 16.0)
            pltpu.make_async_copy(norm_d, norm_out, norm_store).start()

        return carry

    pl.semaphore_wait(barrier, 8)
    norm_part[...] = jnp.zeros_like(norm_part)
    square[...] = jnp.zeros_like(square)
    lax.fori_loop(0, total + LAG_ZERO + 4 * LAG, trip, 0)

    norm_sq = norm_d[...] * norm_d[...]
    local = jnp.sum(square[...]) + jnp.sum(norm_sq)
    value = jnp.full((8, 128), local, F32)
    sum_send[...] = value
    sum_recv[f] = value
    sums = [remote(sum_send, sum_recv.at[f], sum_ssem.at[k], sum_rsem.at[f], dev) for k, dev in enumerate(peers)]
    start(sums)
    for k in range(1, 8):
        s = lax.rem(f + k, 8)
        remote(sum_send, sum_recv.at[s], sum_ssem.at[0], sum_rsem.at[s], core).wait_recv()
    whole = sum_recv[0]
    for k in range(1, 8):
        whole = whole + sum_recv[k]
    scale[...] = jnp.minimum(1.0, CLIP_NORM / jnp.sqrt(whole))
    scale_copy = pltpu.make_async_copy(scale, scale_out, scale_sem)
    scale_copy.start()

    wait_send(sums)
    wait_send((norm_zero, norm_one, norm_two, norm_three))
    pltpu.make_async_copy(norm_d, norm_out, norm_store).wait()

    def drain(slots, copies):
        def body(j, carry):
            wait_send(copies(j))
            return carry
        lax.fori_loop(total - slots, total, body, 0)

    drain(P_SLOTS, ones)
    drain(R_SLOTS, lambda j: (zero_copy(emb, 0, j),))
    drain(SEND_SLOTS, lambda j: twos(j) + threes(j) + fours(j, c_keep, d_keep))

    def last(j, carry):
        out_copy(emb_out, 0, j).wait()
        return carry

    lax.fori_loop(total - SEND_SLOTS, total, last, 0)
    scale_copy.wait()


def reduce_grads(emb_grad, mat_grad, norm_grad):
    emb_rows = emb_grad.shape[0] // 8
    mat_rows = mat_grad.shape[0] // 8
    counts = (emb_rows // ROWS, mat_rows // ROWS)
    dma = pltpu.SemaphoreType.DMA
    scratch = [
        pltpu.VMEM((P_SLOTS, 2, 2, ROWS, WIDTH), F32),
        pltpu.VMEM((R_SLOTS, 2, 2, ROWS, WIDTH), F32),
        pltpu.VMEM((RING, 2, ROWS, A_COLS), F32),
        pltpu.VMEM((RING, 2, ROWS, B_COLS), F32),
        pltpu.VMEM((RING, 2, 2, ROWS, HALF), F32),
        pltpu.VMEM((RING, 2, 2, ROWS, HALF), F32),
        pltpu.VMEM((RING, ROWS, A_COLS), F32),
        pltpu.VMEM((RING, ROWS, B_COLS), F32),
        pltpu.VMEM((RING, 2, ROWS, HALF), F32),
        pltpu.VMEM((RING, 2, ROWS, HALF), F32),
        pltpu.VMEM((RING, ROWS, HALF), F32),
        pltpu.VMEM((RING, ROWS, HALF), F32),
        pltpu.VMEM((RING, ROWS, WIDTH), F32),
        pltpu.VMEM((ROWS, WIDTH), F32),
        pltpu.VMEM((NORM_ROWS, WIDTH), F32),
        pltpu.VMEM((2, 2, 2) + NORM_PAD, F32),
        pltpu.VMEM((2, 2) + NORM_PAD, F32),
        pltpu.VMEM((2,) + NORM_PAD, F32),
        pltpu.VMEM(NORM_PAD, F32),
        pltpu.VMEM(NORM_PAD, F32),
        pltpu.VMEM((8, 128), F32),
        pltpu.VMEM((8, 8, 128), F32),
        pltpu.VMEM((8, 128), F32),
        dma((P_SLOTS,)), dma((R_SLOTS,)), dma((R_SLOTS,)), pltpu.SemaphoreType.REGULAR,
        dma((4, P_SLOTS)), dma((4, RING)), dma((4, SEND_SLOTS)), dma((4, RING)),
        dma((4, SEND_SLOTS)), dma((4, RING)), dma((2, SEND_SLOTS)), dma((2, RING)), dma((SEND_SLOTS,)),
        dma, dma((4,)), dma((4,)), dma, dma((7,)), dma((8,)), dma,
    ]
    hbm = pl.BlockSpec(memory_space=pl.ANY)
    return pl.pallas_call(
        functools.partial(reduce_kernel, counts),
        out_shape=(
            jax.ShapeDtypeStruct((emb_rows, WIDTH), F32),
            jax.ShapeDtypeStruct((mat_rows, WIDTH), F32),
            jax.ShapeDtypeStruct(NORM_PAD, F32),
            jax.ShapeDtypeStruct((8, 128), F32),
        ),
        in_specs=[hbm] * 3,
        out_specs=(hbm,) * 4,
        scratch_shapes=scratch,
        compiler_params=pltpu.CompilerParams(
            collective_id=0, has_side_effects=True, vmem_limit_bytes=25 * 1024 * 1024
        ),
        name="reduce_grads",
    )(emb_grad.reshape(2, 2, 2, emb_rows, WIDTH), mat_grad.reshape(2, 2, 2, mat_rows, WIDTH), norm_grad)


def adamw_update(grad_part, param_old, mom_old, var_old, decay_rate):
    new_mom = BETA_ONE * mom_old + (1.0 - BETA_ONE) * grad_part
    new_var = BETA_TWO * var_old + (1.0 - BETA_TWO) * grad_part * grad_part
    mom_hat = new_mom / (1.0 - BETA_ONE ** ADAM_STEP)
    var_hat = new_var / (1.0 - BETA_TWO ** ADAM_STEP)
    step_dir = mom_hat / (jnp.sqrt(var_hat) + ADAM_EPS)
    new_param = param_old - LEARN_RATE * (step_dir + decay_rate * param_old)
    return (new_param, new_mom, new_var, new_param.astype(jnp.bfloat16))


def solution(mesh):
    def local_step(emb_grad, mat_grad, norm_grad, emb_param, emb_mom, emb_var, mat_param, mat_mom, mat_var, norm_param, norm_mom, norm_var):
        emb_mean, mat_mean, norm_mean, scale = reduce_grads(emb_grad[0, 0], mat_grad[0, 0], norm_grad[0, 0])
        clip_scale = scale[0, 0]
        emb_out = adamw_update(emb_mean * clip_scale, emb_param, emb_mom, emb_var, WEIGHT_DECAY)
        mat_out = adamw_update(mat_mean * clip_scale, mat_param, mat_mom, mat_var, WEIGHT_DECAY)
        norm_out = adamw_update(norm_mean[:NORM_ROWS, :NORM_COLS] * clip_scale, norm_param, norm_mom, norm_var, 0.0)
        return emb_out + mat_out + norm_out

    grad_spec = P("dp", "fsdp", None, None)
    row_spec = P("fsdp", None)
    col_spec = P(None, "fsdp")
    in_list = (grad_spec, grad_spec, grad_spec, row_spec, row_spec, row_spec, row_spec, row_spec, row_spec, col_spec, col_spec, col_spec)
    out_list = (row_spec, row_spec, row_spec, row_spec, row_spec, row_spec, row_spec, row_spec, col_spec, col_spec, col_spec, col_spec)
    return jax.shard_map(local_step, mesh=mesh, in_specs=in_list, out_specs=out_list, check_vma=False)
```

```python
import functools
import math

import jax
import jax.numpy as jnp
from jax import lax
from jax.experimental import pallas as pl
from jax.experimental.pallas import tpu as pltpu
from jax.sharding import PartitionSpec as P

LEARN_RATE = 0.003
BETA_ONE = 0.9
BETA_TWO = 0.95
ADAM_EPS = 1e-8
WEIGHT_DECAY = 0.1
CLIP_NORM = 1.0
ADAM_STEP = 10

MESH = pl.DeviceIdType.MESH
F32 = jnp.float32

WIDTH = 5376
NORM_ROWS = 9
NORM_COLS = 672
NORM_PAD = (16, 768)
ROWS = 8
A_COLS = 2176
B_COLS = 2176
HALF = 256
B_AT = A_COLS
C_AT = A_COLS + B_COLS
D_AT = C_AT + 2 * HALF
LAG_ZERO = 3
LAG = 2
P_SLOTS = 8
R_SLOTS = 6
SEND_SLOTS = 8
RING = 16


def reduce_kernel(counts, emb, mat, norm, emb_out, mat_out, norm_out, scale_out,
                  part, recv_zero, xa, yb, zc, zd, ya, xb, xc, yd, yc, xd, grad, square,
                  norm_in, norm_part, norm_a, norm_b, norm_c, norm_d, sum_send, sum_recv, scale,
                  load_sem, zero_send, zero_recv, credit,
                  one_send, one_recv, two_send, two_recv, three_send, three_recv, four_send, four_recv, out_sem,
                  norm_load, norm_send, norm_recv, norm_store, sum_ssem, sum_rsem, scale_sem):
    emb_count, mat_count = counts
    total = emb_count + mat_count
    z = lax.axis_index("dp")
    f = lax.axis_index("fsdp")
    c = lax.rem(f, 2)
    x = lax.rem(lax.div(f, 2), 2)
    y = lax.div(f, 4)
    core = (z, f + 1 - 2 * c)
    xn = (z, f + 2 - 4 * x)
    yn = (z, f + 4 - 8 * y)
    zn = (1 - z, f)
    peers = [(z, lax.rem(f + k, 8)) for k in range(1, 8)]

    def remote(src, dst, ssem, rsem, dev):
        return pltpu.make_async_remote_copy(src_ref=src, dst_ref=dst, send_sem=ssem, recv_sem=rsem,
                                            device_id=dev, device_id_type=MESH)

    def half_at(base, which):
        return pl.ds(pl.multiple_of(base + which * HALF, 128), HALF)

    c_keep, c_give = half_at(C_AT, z), half_at(C_AT, 1 - z)
    d_keep, d_give = half_at(D_AT, z), half_at(D_AT, 1 - z)
    a_cols, b_cols = pl.ds(0, A_COLS), pl.ds(B_AT, B_COLS)

    barrier = pltpu.get_barrier_semaphore()
    for dev in peers + [zn]:
        pl.semaphore_signal(barrier, inc=1, device_id=dev, device_id_type=MESH)
    norm_copy = pltpu.make_async_copy(norm, norm_in, norm_load)
    norm_copy.start()

    def on_rows(j, body):
        @pl.when(j < emb_count)
        def _():
            body(emb, emb_out, pl.multiple_of(j * ROWS, ROWS))

        @pl.when(j >= emb_count)
        def _():
            body(mat, mat_out, pl.multiple_of((j - emb_count) * ROWS, ROWS))

    def load_copy(ref, row, j):
        s = lax.rem(j, P_SLOTS)
        return pltpu.make_async_copy(ref.at[:, :, c, pl.ds(row, ROWS), :], part.at[s], load_sem.at[s])

    def zero_copy(ref, row, j):
        s = lax.rem(j, R_SLOTS)
        return remote(ref.at[:, :, 1 - c, pl.ds(row, ROWS), :], recv_zero.at[s], zero_send.at[s], zero_recv.at[s], core)

    def ones(j):
        s, r = lax.rem(j, P_SLOTS), lax.rem(j, RING)
        return (remote(part.at[s, :, :, :, c_give], zc.at[r], one_send.at[2, s], one_recv.at[2, r], zn),
                remote(part.at[s, :, :, :, d_give], zd.at[r], one_send.at[3, s], one_recv.at[3, r], zn),
                remote(part.at[s, :, 1 - x, :, a_cols], xa.at[r], one_send.at[0, s], one_recv.at[0, r], xn),
                remote(part.at[s, 1 - y, :, :, b_cols], yb.at[r], one_send.at[1, s], one_recv.at[1, r], yn))

    def twos(j):
        s, r = lax.rem(j, SEND_SLOTS), lax.rem(j, RING)
        return (remote(zc.at[r, :, 1 - x], xc.at[r], two_send.at[2, s], two_recv.at[2, r], xn),
                remote(zd.at[r, 1 - y], yd.at[r], two_send.at[3, s], two_recv.at[3, r], yn),
                remote(xa.at[r, 1 - y], ya.at[r], two_send.at[0, s], two_recv.at[0, r], yn),
                remote(yb.at[r, 1 - x], xb.at[r], two_send.at[1, s], two_recv.at[1, r], xn))

    def threes(j):
        s, r = lax.rem(j, SEND_SLOTS), lax.rem(j, RING)
        return (remote(xc.at[r, 1 - y], yc.at[r], three_send.at[2, s], three_recv.at[2, r], yn),
                remote(yd.at[r, 1 - x], xd.at[r], three_send.at[3, s], three_recv.at[3, r], xn),
                remote(ya.at[r], grad.at[r, :, a_cols], three_send.at[0, s], three_recv.at[0, r], zn),
                remote(xb.at[r], grad.at[r, :, b_cols], three_send.at[1, s], three_recv.at[1, r], zn))

    def fours(j, c_at, d_at):
        s, r = lax.rem(j, SEND_SLOTS), lax.rem(j, RING)
        return (remote(grad.at[r, :, c_at], grad.at[r, :, c_at], four_send.at[0, s], four_recv.at[0, r], zn),
                remote(grad.at[r, :, d_at], grad.at[r, :, d_at], four_send.at[1, s], four_recv.at[1, r], zn))

    def out_copy(ref, row, j):
        return pltpu.make_async_copy(grad.at[lax.rem(j, RING)], ref.at[pl.ds(row, ROWS), :],
                                     out_sem.at[lax.rem(j, SEND_SLOTS)])

    norm_zero = remote(norm_part.at[:, :, 1 - c], norm_a, norm_send.at[0], norm_recv.at[0], core)
    norm_one = remote(norm_a.at[:, 1 - x], norm_b, norm_send.at[1], norm_recv.at[1], xn)
    norm_two = remote(norm_b.at[1 - y], norm_c, norm_send.at[2], norm_recv.at[2], yn)
    norm_three = remote(norm_c, norm_d, norm_send.at[3], norm_recv.at[3], zn)

    def when_in(j, body):
        pl.when(jnp.logical_and(j >= 0, j < total))(functools.partial(body, j))

    def start(copies):
        for copy in copies:
            copy.start()

    def wait_send(copies):
        for copy in copies:
            copy.wait_send()

    def stage_issue(j):
        @pl.when(j >= P_SLOTS)
        def _():
            wait_send(ones(j - P_SLOTS))

        @pl.when(j >= R_SLOTS)
        def _():
            zero_copy(emb, 0, j - R_SLOTS).wait_send()
            pl.semaphore_wait(credit, 1)

        def body(ref, _, row):
            zero_copy(ref, row, j).start()
            load_copy(ref, row, j).start()

        on_rows(j, body)

    def stage_one(j):
        load_copy(emb, 0, j).wait()
        zero_copy(emb, 0, j).wait_recv()
        part[lax.rem(j, P_SLOTS)] += recv_zero[lax.rem(j, R_SLOTS)]

        @pl.when(j + R_SLOTS < total)
        def _():
            pl.semaphore_signal(credit, inc=1, device_id=core, device_id_type=MESH)

        start(ones(j))

    def stage_two(j):
        s, r = lax.rem(j, P_SLOTS), lax.rem(j, RING)
        for copy in ones(j):
            copy.wait_recv()
        zc[r] += part[s, :, :, :, c_keep]
        zd[r] += part[s, :, :, :, d_keep]
        xa[r] += part[s, :, x, :, a_cols]
        yb[r] += part[s, y, :, :, b_cols]

        @pl.when(j >= SEND_SLOTS)
        def _():
            wait_send(twos(j - SEND_SLOTS))

        start(twos(j))

    def stage_three(j):
        r = lax.rem(j, RING)
        for copy in twos(j):
            copy.wait_recv()
        xc[r] += zc[r, :, x]
        yd[r] += zd[r, y]
        ya[r] += xa[r, y]
        xb[r] += yb[r, x]

        @pl.when(j >= SEND_SLOTS)
        def _():
            wait_send(threes(j - SEND_SLOTS))

        start(threes(j))

    def stage_four(j):
        r = lax.rem(j, RING)
        for copy in threes(j):
            copy.wait_recv()

        @pl.when(j >= SEND_SLOTS)
        def _():
            wait_send(fours(j - SEND_SLOTS, c_keep, d_keep))

        grad[r, :, c_keep] = (yc[r] + xc[r, y]) * (1.0 / 16.0)
        grad[r, :, d_keep] = (xd[r] + yd[r, x]) * (1.0 / 16.0)
        left = (grad[r, :, a_cols] + ya[r]) * (1.0 / 16.0)
        right = (grad[r, :, b_cols] + xb[r]) * (1.0 / 16.0)
        grad[r, :, a_cols] = left
        grad[r, :, b_cols] = right
        square[:, a_cols] += left * left
        square[:, b_cols] += right * right
        start(fours(j, c_keep, d_keep))

    def stage_five(j):
        r = lax.rem(j, RING)
        for copy in fours(j, c_give, d_give):
            copy.wait_recv()
        rest = grad[r, :, C_AT:]
        square[:, C_AT:] += rest * rest

        @pl.when(j >= SEND_SLOTS)
        def _():
            out_copy(emb_out, 0, j - SEND_SLOTS).wait()

        def body(_, ref, row):
            out_copy(ref, row, j).start()

        on_rows(j, body)

    def trip(it, carry):
        when_in(it, stage_issue)
        when_in(it - LAG_ZERO, stage_one)
        when_in(it - LAG_ZERO - LAG, stage_two)
        when_in(it - LAG_ZERO - 2 * LAG, stage_three)
        when_in(it - LAG_ZERO - 3 * LAG, stage_four)
        when_in(it - LAG_ZERO - 4 * LAG, stage_five)

        @pl.when(it == 5)
        def _():
            norm_copy.wait()
            for k in range(8):
                for row in range(NORM_ROWS):
                    norm_part[k // 4, (k // 2) % 2, k % 2, row:row + 1, :NORM_COLS] = norm_in[row, :, k * NORM_COLS:(k + 1) * NORM_COLS]
            norm_zero.start()

        @pl.when(it == 8)
        def _():
            norm_zero.wait_recv()
            norm_a[...] += norm_part[:, :, c]
            norm_one.start()

        @pl.when(it == 12)
        def _():
            norm_one.wait_recv()
            norm_b[...] += norm_a[:, x]
            norm_two.start()

        @pl.when(it == 16)
        def _():
            norm_two.wait_recv()
            norm_c[...] += norm_b[y]
            norm_three.start()

        @pl.when(it == 20)
        def _():
            norm_three.wait_recv()
            norm_d[...] = (norm_d[...] + norm_c[...]) * (1.0 / 16.0)
            pltpu.make_async_copy(norm_d, norm_out, norm_store).start()

        return carry

    pl.semaphore_wait(barrier, 8)
    norm_part[...] = jnp.zeros_like(norm_part)
    square[...] = jnp.zeros_like(square)
    lax.fori_loop(0, total + LAG_ZERO + 4 * LAG, trip, 0)

    norm_sq = norm_d[...] * norm_d[...]
    local = jnp.sum(square[...]) + jnp.sum(norm_sq)
    value = jnp.full((8, 128), local, F32)
    sum_send[...] = value
    sum_recv[f] = value
    sums = [remote(sum_send, sum_recv.at[f], sum_ssem.at[k], sum_rsem.at[f], dev) for k, dev in enumerate(peers)]
    start(sums)
    for k in range(1, 8):
        s = lax.rem(f + k, 8)
        remote(sum_send, sum_recv.at[s], sum_ssem.at[0], sum_rsem.at[s], core).wait_recv()
    whole = sum_recv[0]
    for k in range(1, 8):
        whole = whole + sum_recv[k]
    scale[...] = jnp.minimum(1.0, CLIP_NORM / jnp.sqrt(whole))
    scale_copy = pltpu.make_async_copy(scale, scale_out, scale_sem)
    scale_copy.start()

    wait_send(sums)
    wait_send((norm_zero, norm_one, norm_two, norm_three))
    pltpu.make_async_copy(norm_d, norm_out, norm_store).wait()

    def drain(slots, copies):
        def body(j, carry):
            wait_send(copies(j))
            return carry
        lax.fori_loop(total - slots, total, body, 0)

    drain(P_SLOTS, ones)
    drain(R_SLOTS, lambda j: (zero_copy(emb, 0, j),))
    drain(SEND_SLOTS, lambda j: twos(j) + threes(j) + fours(j, c_keep, d_keep))

    def last(j, carry):
        out_copy(emb_out, 0, j).wait()
        return carry

    lax.fori_loop(total - SEND_SLOTS, total, last, 0)
    scale_copy.wait()


def reduce_grads(emb_grad, mat_grad, norm_grad):
    emb_rows = emb_grad.shape[0] // 8
    mat_rows = mat_grad.shape[0] // 8
    counts = (emb_rows // ROWS, mat_rows // ROWS)
    dma = pltpu.SemaphoreType.DMA
    scratch = [
        pltpu.VMEM((P_SLOTS, 2, 2, ROWS, WIDTH), F32),
        pltpu.VMEM((R_SLOTS, 2, 2, ROWS, WIDTH), F32),
        pltpu.VMEM((RING, 2, ROWS, A_COLS), F32),
        pltpu.VMEM((RING, 2, ROWS, B_COLS), F32),
        pltpu.VMEM((RING, 2, 2, ROWS, HALF), F32),
        pltpu.VMEM((RING, 2, 2, ROWS, HALF), F32),
        pltpu.VMEM((RING, ROWS, A_COLS), F32),
        pltpu.VMEM((RING, ROWS, B_COLS), F32),
        pltpu.VMEM((RING, 2, ROWS, HALF), F32),
        pltpu.VMEM((RING, 2, ROWS, HALF), F32),
        pltpu.VMEM((RING, ROWS, HALF), F32),
        pltpu.VMEM((RING, ROWS, HALF), F32),
        pltpu.VMEM((RING, ROWS, WIDTH), F32),
        pltpu.VMEM((ROWS, WIDTH), F32),
        pltpu.VMEM((NORM_ROWS, 1, WIDTH), F32),
        pltpu.VMEM((2, 2, 2) + NORM_PAD, F32),
        pltpu.VMEM((2, 2) + NORM_PAD, F32),
        pltpu.VMEM((2,) + NORM_PAD, F32),
        pltpu.VMEM(NORM_PAD, F32),
        pltpu.VMEM(NORM_PAD, F32),
        pltpu.VMEM((8, 128), F32),
        pltpu.VMEM((8, 8, 128), F32),
        pltpu.VMEM((8, 128), F32),
        dma((P_SLOTS,)), dma((R_SLOTS,)), dma((R_SLOTS,)), pltpu.SemaphoreType.REGULAR,
        dma((4, P_SLOTS)), dma((4, RING)), dma((4, SEND_SLOTS)), dma((4, RING)),
        dma((4, SEND_SLOTS)), dma((4, RING)), dma((2, SEND_SLOTS)), dma((2, RING)), dma((SEND_SLOTS,)),
        dma, dma((4,)), dma((4,)), dma, dma((7,)), dma((8,)), dma,
    ]
    hbm = pl.BlockSpec(memory_space=pl.ANY)
    return pl.pallas_call(
        functools.partial(reduce_kernel, counts),
        out_shape=(
            jax.ShapeDtypeStruct((emb_rows, WIDTH), F32),
            jax.ShapeDtypeStruct((mat_rows, WIDTH), F32),
            jax.ShapeDtypeStruct(NORM_PAD, F32),
            jax.ShapeDtypeStruct((8, 128), F32),
        ),
        in_specs=[pl.BlockSpec(memory_space=pltpu.HBM)] * 3,
        out_specs=(hbm,) * 4,
        scratch_shapes=scratch,
        compiler_params=pltpu.CompilerParams(
            collective_id=0, has_side_effects=True, vmem_limit_bytes=25 * 1024 * 1024
        ),
        name="reduce_grads",
    )(emb_grad.reshape(2, 2, 2, emb_rows, WIDTH), mat_grad.reshape(2, 2, 2, mat_rows, WIDTH),
      norm_grad.reshape(NORM_ROWS, 1, WIDTH))


BLOCK = 16
COLS = 384
STORE_SLOTS = 4


def adamw_block(grad, param, mom, var, decay_rate):
    new_mom = BETA_ONE * mom + (1.0 - BETA_ONE) * grad
    new_var = BETA_TWO * var + (1.0 - BETA_TWO) * grad * grad
    root = math.sqrt(1.0 - BETA_TWO ** ADAM_STEP)
    step_dir = new_mom / (jnp.sqrt(new_var) + ADAM_EPS * root)
    rate = LEARN_RATE * root / (1.0 - BETA_ONE ** ADAM_STEP)
    return param - (rate * step_dir + (LEARN_RATE * decay_rate) * param), new_mom, new_var


def adamw_kernel(scale, eg, ep, em, ev, mg, mp, mm, mv, ng, np_, nm, nv,
                 ep_out, em_out, ev_out, eb_out, mp_out, mm_out, mv_out, mb_out, np_out, nm_out, nv_out, nb_out,
                 p_buf, m_buf, v_buf, b_buf, n_bufs, nb_buf, sems, n_sems):
    clip = scale[0:1, 0:1]

    def copies(outs, slot, row):
        return [pltpu.make_async_copy(buf.at[slot], out.at[pl.ds(row, BLOCK), :], sems.at[k, slot])
                for k, (buf, out) in enumerate(zip((p_buf, m_buf, v_buf, b_buf), outs))]

    emb_outs = (ep_out, em_out, ev_out, eb_out)
    mat_outs = (mp_out, mm_out, mv_out, mb_out)
    emb_blocks = eg.shape[0] // BLOCK
    mat_blocks = mg.shape[0] // BLOCK

    def run(first, count, ins, outs):
        def body(i, carry):
            j = first + i
            slot = lax.rem(j, STORE_SLOTS)

            @pl.when(j >= STORE_SLOTS)
            def _():
                for copy in copies(emb_outs, slot, 0):
                    copy.wait()

            row = pl.multiple_of(i * BLOCK, BLOCK)
            for col in range(0, WIDTH, COLS):
                cols = pl.ds(col, COLS)
                g, p, m, v = (ref[pl.ds(row, BLOCK), cols] for ref in ins)
                new_p, new_m, new_v = adamw_block(g * clip, p, m, v, WEIGHT_DECAY)
                p_buf[slot, :, cols] = new_p
                m_buf[slot, :, cols] = new_m
                v_buf[slot, :, cols] = new_v
                b_buf[slot, :, cols] = new_p.astype(jnp.bfloat16)
            for copy in copies(outs, slot, row):
                copy.start()
            return carry

        lax.fori_loop(0, count, body, 0)

    run(0, emb_blocks, (eg, ep, em, ev), emb_outs)
    run(emb_blocks, mat_blocks, (mg, mp, mm, mv), mat_outs)
    new_p, new_m, new_v = adamw_block(ng[:NORM_ROWS, :NORM_COLS] * clip, np_[...], nm[...], nv[...], 0.0)
    for k, value in enumerate((new_p, new_m, new_v)):
        n_bufs[k] = value
    nb_buf[...] = new_p.astype(jnp.bfloat16)
    norm_copies = [pltpu.make_async_copy(n_bufs.at[k], out, n_sems.at[k]) for k, out in enumerate((np_out, nm_out, nv_out))]
    norm_copies.append(pltpu.make_async_copy(nb_buf, nb_out, n_sems.at[3]))
    for copy in norm_copies:
        copy.start()
    for slot in range(STORE_SLOTS):
        for copy in copies(emb_outs, slot, 0):
            copy.wait()
    for copy in norm_copies:
        copy.wait()


def adamw(scale, emb, mat, norm):
    shapes = []
    for ref in (emb[1], mat[1], norm[1]):
        shapes += [jax.ShapeDtypeStruct(ref.shape, F32)] * 3 + [jax.ShapeDtypeStruct(ref.shape, jnp.bfloat16)]
    buf = (STORE_SLOTS, BLOCK, WIDTH)
    vmem = pl.BlockSpec(memory_space=pltpu.VMEM)
    hbm = pl.BlockSpec(memory_space=pl.ANY)
    elements = emb[1].size + mat[1].size
    return pl.pallas_call(
        adamw_kernel,
        out_shape=tuple(shapes),
        in_specs=[vmem] * 13,
        out_specs=(hbm,) * 12,
        scratch_shapes=[
            pltpu.VMEM(buf, F32), pltpu.VMEM(buf, F32), pltpu.VMEM(buf, F32), pltpu.VMEM(buf, jnp.bfloat16),
            pltpu.VMEM((3, NORM_ROWS, NORM_COLS), F32), pltpu.VMEM((NORM_ROWS, NORM_COLS), jnp.bfloat16),
            pltpu.SemaphoreType.DMA((4, STORE_SLOTS)), pltpu.SemaphoreType.DMA((4,)),
        ],
        compiler_params=pltpu.CompilerParams(vmem_limit_bytes=8 * 1024 * 1024),
        cost_estimate=pl.CostEstimate(flops=20 * elements, bytes_accessed=30 * elements, transcendentals=2 * elements),
        name="adamw",
    )(scale, *emb, *mat, *norm)


def solution(mesh):
    def local_step(emb_grad, mat_grad, norm_grad, emb_param, emb_mom, emb_var, mat_param, mat_mom, mat_var, norm_param, norm_mom, norm_var):
        emb_mean, mat_mean, norm_mean, scale = reduce_grads(emb_grad[0, 0], mat_grad[0, 0], norm_grad[0, 0])
        return adamw(scale, (emb_mean, emb_param, emb_mom, emb_var), (mat_mean, mat_param, mat_mom, mat_var),
                     (norm_mean, norm_param, norm_mom, norm_var))

    grad_spec = P("dp", "fsdp", None, None)
    row_spec = P("fsdp", None)
    col_spec = P(None, "fsdp")
    in_list = (grad_spec, grad_spec, grad_spec, row_spec, row_spec, row_spec, row_spec, row_spec, row_spec, col_spec, col_spec, col_spec)
    out_list = (row_spec, row_spec, row_spec, row_spec, row_spec, row_spec, row_spec, row_spec, col_spec, col_spec, col_spec, col_spec)
    return jax.shard_map(local_step, mesh=mesh, in_specs=in_list, out_specs=out_list, check_vma=False)
```

```python
import functools
import math

import jax
import jax.numpy as jnp
from jax import lax
from jax.experimental import pallas as pl
from jax.experimental.pallas import tpu as pltpu
from jax.sharding import PartitionSpec as P

LEARN_RATE = 0.003
BETA_ONE = 0.9
BETA_TWO = 0.95
ADAM_EPS = 1e-8
WEIGHT_DECAY = 0.1
CLIP_NORM = 1.0
ADAM_STEP = 10

MESH = pl.DeviceIdType.MESH
F32 = jnp.float32

WIDTH = 5376
NORM_ROWS = 9
NORM_COLS = 672
NORM_PAD = (16, 768)
ROWS = 8
A_COLS = 2048
B_COLS = 2048
HALF = 640
B_AT = A_COLS
C_AT = A_COLS + B_COLS
LAG_ZERO = 3
LAG = 2
P_SLOTS = 8
R_SLOTS = 6
SEND_SLOTS = 8
RING = 16


def reduce_kernel(counts, emb, mat, norm, emb_out, mat_out, norm_out, scale_out,
                  part, recv_zero, xa, yb, zc, mid, wc, tc, grad, square,
                  norm_in, norm_part, norm_a, norm_b, norm_c, norm_d, sum_send, sum_recv, scale,
                  load_sem, zero_send, zero_recv, credit,
                  one_send, one_recv, two_send, two_recv, three_send, three_recv, four_send, four_recv, out_sem,
                  norm_load, norm_send, norm_recv, norm_store, sum_ssem, sum_rsem, scale_sem):
    emb_count, mat_count = counts
    total = emb_count + mat_count
    z = lax.axis_index("dp")
    f = lax.axis_index("fsdp")
    c = lax.rem(f, 2)
    x = lax.rem(lax.div(f, 2), 2)
    y = lax.div(f, 4)
    core = (z, f + 1 - 2 * c)
    xn = (z, f + 2 - 4 * x)
    yn = (z, f + 4 - 8 * y)
    zn = (1 - z, f)
    peers = [(z, lax.rem(f + k, 8)) for k in range(1, 8)]

    def remote(src, dst, ssem, rsem, dev):
        return pltpu.make_async_remote_copy(src_ref=src, dst_ref=dst, send_sem=ssem, recv_sem=rsem,
                                            device_id=dev, device_id_type=MESH)

    def half_at(base, which):
        return pl.ds(pl.multiple_of(base + which * HALF, 128), HALF)

    c_keep, c_give = half_at(C_AT, z), half_at(C_AT, 1 - z)
    a_cols, b_cols, ab_cols = pl.ds(0, A_COLS), pl.ds(B_AT, B_COLS), pl.ds(0, C_AT)

    barrier = pltpu.get_barrier_semaphore()
    for dev in peers + [zn]:
        pl.semaphore_signal(barrier, inc=1, device_id=dev, device_id_type=MESH)
    norm_copy = pltpu.make_async_copy(norm, norm_in, norm_load)
    norm_copy.start()

    def on_rows(j, body):
        @pl.when(j < emb_count)
        def _():
            body(emb, emb_out, pl.multiple_of(j * ROWS, ROWS))

        @pl.when(j >= emb_count)
        def _():
            body(mat, mat_out, pl.multiple_of((j - emb_count) * ROWS, ROWS))

    def load_copy(ref, row, j):
        s = lax.rem(j, P_SLOTS)
        return pltpu.make_async_copy(ref.at[:, :, c, pl.ds(row, ROWS), :], part.at[s], load_sem.at[s])

    def zero_copy(ref, row, j):
        s = lax.rem(j, R_SLOTS)
        return remote(ref.at[:, :, 1 - c, pl.ds(row, ROWS), :], recv_zero.at[s], zero_send.at[s], zero_recv.at[s], core)

    def ones(j):
        s, r = lax.rem(j, P_SLOTS), lax.rem(j, RING)
        return (remote(part.at[s, :, :, :, c_give], zc.at[r], one_send.at[2, s], one_recv.at[2, r], zn),
                remote(part.at[s, :, 1 - x, :, a_cols], xa.at[r], one_send.at[0, s], one_recv.at[0, r], xn),
                remote(part.at[s, 1 - y, :, :, b_cols], yb.at[r], one_send.at[1, s], one_recv.at[1, r], yn))

    def two_c_even(j):
        s, r = lax.rem(j, SEND_SLOTS), lax.rem(j, RING)
        return remote(zc.at[r, :, 1 - x], wc.at[r], two_send.at[2, s], two_recv.at[2, r], xn)

    def two_c_odd(j):
        s, r = lax.rem(j, SEND_SLOTS), lax.rem(j, RING)
        return remote(zc.at[r, 1 - y], wc.at[r], two_send.at[2, s], two_recv.at[2, r], yn)

    def twos(j):
        s, r = lax.rem(j, SEND_SLOTS), lax.rem(j, RING)
        return (remote(xa.at[r, 1 - y], mid.at[r, :, a_cols], two_send.at[0, s], two_recv.at[0, r], yn),
                remote(yb.at[r, 1 - x], mid.at[r, :, b_cols], two_send.at[1, s], two_recv.at[1, r], xn))

    def three_c(j):
        s, r, odd = lax.rem(j, SEND_SLOTS), lax.rem(j, RING), lax.rem(j, 2)
        here = y + odd * (x - y)
        step = (4 - 8 * y) + odd * ((2 - 4 * x) - (4 - 8 * y))
        return remote(wc.at[r, 1 - here], tc.at[r], three_send.at[1, s], three_recv.at[1, r], (z, f + step))

    def three_ab(j):
        s, r = lax.rem(j, SEND_SLOTS), lax.rem(j, RING)
        return remote(mid.at[r], grad.at[r, :, ab_cols], three_send.at[0, s], three_recv.at[0, r], zn)

    def four(j, c_at):
        s, r = lax.rem(j, SEND_SLOTS), lax.rem(j, RING)
        return remote(grad.at[r, :, c_at], grad.at[r, :, c_at], four_send.at[s], four_recv.at[r], zn)

    def out_copy(ref, row, j):
        return pltpu.make_async_copy(grad.at[lax.rem(j, RING)], ref.at[pl.ds(row, ROWS), :],
                                     out_sem.at[lax.rem(j, SEND_SLOTS)])

    norm_zero = remote(norm_part.at[:, :, 1 - c], norm_a, norm_send.at[0], norm_recv.at[0], core)
    norm_one = remote(norm_a.at[:, 1 - x], norm_b, norm_send.at[1], norm_recv.at[1], xn)
    norm_two = remote(norm_b.at[1 - y], norm_c, norm_send.at[2], norm_recv.at[2], yn)
    norm_three = remote(norm_c, norm_d, norm_send.at[3], norm_recv.at[3], zn)

    def when_in(j, body):
        pl.when(jnp.logical_and(j >= 0, j < total))(functools.partial(body, j))

    def start(copies):
        for copy in copies:
            copy.start()

    def wait_send(copies):
        for copy in copies:
            copy.wait_send()

    def stage_issue(j):
        @pl.when(j >= P_SLOTS)
        def _():
            wait_send(ones(j - P_SLOTS))

        @pl.when(j >= R_SLOTS)
        def _():
            zero_copy(emb, 0, j - R_SLOTS).wait_send()
            pl.semaphore_wait(credit, 1)

        def body(ref, _, row):
            zero_copy(ref, row, j).start()
            load_copy(ref, row, j).start()

        on_rows(j, body)

    def stage_one(j):
        load_copy(emb, 0, j).wait()
        zero_copy(emb, 0, j).wait_recv()
        part[lax.rem(j, P_SLOTS)] += recv_zero[lax.rem(j, R_SLOTS)]

        @pl.when(j + R_SLOTS < total)
        def _():
            pl.semaphore_signal(credit, inc=1, device_id=core, device_id_type=MESH)

        start(ones(j))

    def stage_two(j):
        s, r = lax.rem(j, P_SLOTS), lax.rem(j, RING)
        even = lax.rem(j, 2) == 0
        for copy in ones(j):
            copy.wait_recv()
        zc[r] += part[s, :, :, :, c_keep]
        xa[r] += part[s, :, x, :, a_cols]
        yb[r] += part[s, y, :, :, b_cols]

        @pl.when(j >= SEND_SLOTS)
        def _():
            wait_send(twos(j - SEND_SLOTS) + (two_c_even(j - SEND_SLOTS),))

        pl.when(even)(lambda: two_c_even(j).start())
        pl.when(jnp.logical_not(even))(lambda: two_c_odd(j).start())
        start(twos(j))

    def stage_three(j):
        r = lax.rem(j, RING)
        even = lax.rem(j, 2) == 0
        for copy in twos(j) + (two_c_even(j),):
            copy.wait_recv()

        @pl.when(even)
        def _():
            wc[r] += zc[r, :, x]

        @pl.when(jnp.logical_not(even))
        def _():
            wc[r] += zc[r, y]

        mid[r, :, a_cols] += xa[r, y]
        mid[r, :, b_cols] += yb[r, x]

        @pl.when(j >= SEND_SLOTS)
        def _():
            wait_send((three_ab(j - SEND_SLOTS), three_c(j - SEND_SLOTS)))

        start((three_c(j), three_ab(j)))

    def stage_four(j):
        r, odd = lax.rem(j, RING), lax.rem(j, 2)
        here = y + odd * (x - y)
        three_c(j).wait_recv()

        @pl.when(j >= SEND_SLOTS)
        def _():
            four(j - SEND_SLOTS, c_keep).wait_send()

        grad[r, :, c_keep] = (tc[r] + wc[r, here]) * (1.0 / 16.0)
        three_ab(j).wait_recv()
        both = (grad[r, :, ab_cols] + mid[r]) * (1.0 / 16.0)
        grad[r, :, ab_cols] = both
        square[:, ab_cols] += both * both
        four(j, c_keep).start()

    def stage_five(j):
        r = lax.rem(j, RING)
        four(j, c_give).wait_recv()
        rest = grad[r, :, C_AT:]
        square[:, C_AT:] += rest * rest

        @pl.when(j >= SEND_SLOTS)
        def _():
            out_copy(emb_out, 0, j - SEND_SLOTS).wait()

        def body(_, ref, row):
            out_copy(ref, row, j).start()

        on_rows(j, body)

    def trip(it, carry):
        when_in(it, stage_issue)
        when_in(it - LAG_ZERO, stage_one)
        when_in(it - LAG_ZERO - LAG, stage_two)
        when_in(it - LAG_ZERO - 2 * LAG, stage_three)
        when_in(it - LAG_ZERO - 3 * LAG, stage_four)
        when_in(it - LAG_ZERO - 4 * LAG, stage_five)

        @pl.when(it == 5)
        def _():
            norm_copy.wait()
            for k in range(8):
                for row in range(NORM_ROWS):
                    norm_part[k // 4, (k // 2) % 2, k % 2, row:row + 1, :NORM_COLS] = norm_in[row, :, k * NORM_COLS:(k + 1) * NORM_COLS]
            norm_zero.start()

        @pl.when(it == 8)
        def _():
            norm_zero.wait_recv()
            norm_a[...] += norm_part[:, :, c]
            norm_one.start()

        @pl.when(it == 12)
        def _():
            norm_one.wait_recv()
            norm_b[...] += norm_a[:, x]
            norm_two.start()

        @pl.when(it == 16)
        def _():
            norm_two.wait_recv()
            norm_c[...] += norm_b[y]
            norm_three.start()

        @pl.when(it == 20)
        def _():
            norm_three.wait_recv()
            norm_d[...] = (norm_d[...] + norm_c[...]) * (1.0 / 16.0)
            pltpu.make_async_copy(norm_d, norm_out, norm_store).start()

        return carry

    pl.semaphore_wait(barrier, 8)
    norm_part[...] = jnp.zeros_like(norm_part)
    square[...] = jnp.zeros_like(square)
    lax.fori_loop(0, total + LAG_ZERO + 4 * LAG, trip, 0)

    norm_sq = norm_d[...] * norm_d[...]
    local = jnp.sum(square[...]) + jnp.sum(norm_sq)
    value = jnp.full((8, 128), local, F32)
    sum_send[...] = value
    sum_recv[f] = value
    sums = [remote(sum_send, sum_recv.at[f], sum_ssem.at[k], sum_rsem.at[f], dev) for k, dev in enumerate(peers)]
    start(sums)
    for k in range(1, 8):
        s = lax.rem(f + k, 8)
        remote(sum_send, sum_recv.at[s], sum_ssem.at[0], sum_rsem.at[s], core).wait_recv()
    whole = sum_recv[0]
    for k in range(1, 8):
        whole = whole + sum_recv[k]
    scale[...] = jnp.minimum(1.0, CLIP_NORM / jnp.sqrt(whole))
    scale_copy = pltpu.make_async_copy(scale, scale_out, scale_sem)
    scale_copy.start()

    wait_send(sums)
    wait_send((norm_zero, norm_one, norm_two, norm_three))
    pltpu.make_async_copy(norm_d, norm_out, norm_store).wait()

    def drain(slots, copies):
        def body(j, carry):
            wait_send(copies(j))
            return carry
        lax.fori_loop(total - slots, total, body, 0)

    drain(P_SLOTS, ones)
    drain(R_SLOTS, lambda j: (zero_copy(emb, 0, j),))
    drain(SEND_SLOTS, lambda j: twos(j) + (two_c_even(j), three_ab(j), three_c(j), four(j, c_keep)))

    def last(j, carry):
        out_copy(emb_out, 0, j).wait()
        return carry

    lax.fori_loop(total - SEND_SLOTS, total, last, 0)
    scale_copy.wait()


def reduce_grads(emb_grad, mat_grad, norm_grad):
    emb_rows = emb_grad.shape[0] // 8
    mat_rows = mat_grad.shape[0] // 8
    counts = (emb_rows // ROWS, mat_rows // ROWS)
    dma = pltpu.SemaphoreType.DMA
    scratch = [
        pltpu.VMEM((P_SLOTS, 2, 2, ROWS, WIDTH), F32),
        pltpu.VMEM((R_SLOTS, 2, 2, ROWS, WIDTH), F32),
        pltpu.VMEM((RING, 2, ROWS, A_COLS), F32),
        pltpu.VMEM((RING, 2, ROWS, B_COLS), F32),
        pltpu.VMEM((RING, 2, 2, ROWS, HALF), F32),
        pltpu.VMEM((RING, ROWS, C_AT), F32),
        pltpu.VMEM((RING, 2, ROWS, HALF), F32),
        pltpu.VMEM((RING, ROWS, HALF), F32),
        pltpu.VMEM((RING, ROWS, WIDTH), F32),
        pltpu.VMEM((ROWS, WIDTH), F32),
        pltpu.VMEM((NORM_ROWS, 1, WIDTH), F32),
        pltpu.VMEM((2, 2, 2) + NORM_PAD, F32),
        pltpu.VMEM((2, 2) + NORM_PAD, F32),
        pltpu.VMEM((2,) + NORM_PAD, F32),
        pltpu.VMEM(NORM_PAD, F32),
        pltpu.VMEM(NORM_PAD, F32),
        pltpu.VMEM((8, 128), F32),
        pltpu.VMEM((8, 8, 128), F32),
        pltpu.VMEM((8, 128), F32),
        dma((P_SLOTS,)), dma((R_SLOTS,)), dma((R_SLOTS,)), pltpu.SemaphoreType.REGULAR,
        dma((3, P_SLOTS)), dma((3, RING)), dma((3, SEND_SLOTS)), dma((3, RING)),
        dma((2, SEND_SLOTS)), dma((2, RING)), dma((SEND_SLOTS,)), dma((RING,)), dma((SEND_SLOTS,)),
        dma, dma((4,)), dma((4,)), dma, dma((7,)), dma((8,)), dma,
    ]
    hbm = pl.BlockSpec(memory_space=pl.ANY)
    return pl.pallas_call(
        functools.partial(reduce_kernel, counts),
        out_shape=(
            jax.ShapeDtypeStruct((emb_rows, WIDTH), F32),
            jax.ShapeDtypeStruct((mat_rows, WIDTH), F32),
            jax.ShapeDtypeStruct(NORM_PAD, F32),
            jax.ShapeDtypeStruct((8, 128), F32),
        ),
        in_specs=[pl.BlockSpec(memory_space=pltpu.HBM)] * 3,
        out_specs=(hbm,) * 4,
        scratch_shapes=scratch,
        compiler_params=pltpu.CompilerParams(
            collective_id=0, has_side_effects=True, vmem_limit_bytes=25 * 1024 * 1024
        ),
        name="reduce_grads",
    )(*(pltpu.with_memory_space_constraint(grad, pltpu.HBM) for grad in (
        emb_grad.reshape(2, 2, 2, emb_rows, WIDTH), mat_grad.reshape(2, 2, 2, mat_rows, WIDTH),
        norm_grad.reshape(NORM_ROWS, 1, WIDTH))))


BLOCK = 16
COLS = 384
STORE_SLOTS = 4


def adamw_block(grad, param, mom, var, decay_rate):
    new_mom = BETA_ONE * mom + (1.0 - BETA_ONE) * grad
    new_var = BETA_TWO * var + (1.0 - BETA_TWO) * grad * grad
    root = math.sqrt(1.0 - BETA_TWO ** ADAM_STEP)
    step_dir = new_mom / (jnp.sqrt(new_var) + ADAM_EPS * root)
    rate = LEARN_RATE * root / (1.0 - BETA_ONE ** ADAM_STEP)
    return param - (rate * step_dir + (LEARN_RATE * decay_rate) * param), new_mom, new_var


def adamw_kernel(scale, eg, ep, em, ev, mg, mp, mm, mv, ng, np_, nm, nv,
                 ep_out, em_out, ev_out, eb_out, mp_out, mm_out, mv_out, mb_out, np_out, nm_out, nv_out, nb_out,
                 p_buf, m_buf, v_buf, b_buf, n_bufs, nb_buf, sems, n_sems):
    clip = scale[0:1, 0:1]

    def copies(outs, slot, row):
        return [pltpu.make_async_copy(buf.at[slot], out.at[pl.ds(row, BLOCK), :], sems.at[k, slot])
                for k, (buf, out) in enumerate(zip((p_buf, m_buf, v_buf, b_buf), outs))]

    emb_outs = (ep_out, em_out, ev_out, eb_out)
    mat_outs = (mp_out, mm_out, mv_out, mb_out)
    emb_blocks = eg.shape[0] // BLOCK
    mat_blocks = mg.shape[0] // BLOCK

    def run(first, count, ins, outs):
        def body(i, carry):
            j = first + i
            slot = lax.rem(j, STORE_SLOTS)

            @pl.when(j >= STORE_SLOTS)
            def _():
                for copy in copies(emb_outs, slot, 0):
                    copy.wait()

            row = pl.multiple_of(i * BLOCK, BLOCK)
            for col in range(0, WIDTH, COLS):
                cols = pl.ds(col, COLS)
                g, p, m, v = (ref[pl.ds(row, BLOCK), cols] for ref in ins)
                new_p, new_m, new_v = adamw_block(g * clip, p, m, v, WEIGHT_DECAY)
                p_buf[slot, :, cols] = new_p
                m_buf[slot, :, cols] = new_m
                v_buf[slot, :, cols] = new_v
                b_buf[slot, :, cols] = new_p.astype(jnp.bfloat16)
            for copy in copies(outs, slot, row):
                copy.start()
            return carry

        lax.fori_loop(0, count, body, 0)

    run(0, emb_blocks, (eg, ep, em, ev), emb_outs)
    run(emb_blocks, mat_blocks, (mg, mp, mm, mv), mat_outs)
    new_p, new_m, new_v = adamw_block(ng[:NORM_ROWS, :NORM_COLS] * clip, np_[...], nm[...], nv[...], 0.0)
    for k, value in enumerate((new_p, new_m, new_v)):
        n_bufs[k] = value
    nb_buf[...] = new_p.astype(jnp.bfloat16)
    norm_copies = [pltpu.make_async_copy(n_bufs.at[k], out, n_sems.at[k]) for k, out in enumerate((np_out, nm_out, nv_out))]
    norm_copies.append(pltpu.make_async_copy(nb_buf, nb_out, n_sems.at[3]))
    for copy in norm_copies:
        copy.start()
    for slot in range(STORE_SLOTS):
        for copy in copies(emb_outs, slot, 0):
            copy.wait()
    for copy in norm_copies:
        copy.wait()


def adamw(scale, emb, mat, norm):
    shapes = []
    for ref in (emb[1], mat[1], norm[1]):
        shapes += [jax.ShapeDtypeStruct(ref.shape, F32)] * 3 + [jax.ShapeDtypeStruct(ref.shape, jnp.bfloat16)]
    buf = (STORE_SLOTS, BLOCK, WIDTH)
    vmem = pl.BlockSpec(memory_space=pltpu.VMEM)
    hbm = pl.BlockSpec(memory_space=pl.ANY)
    elements = emb[1].size + mat[1].size
    return pl.pallas_call(
        adamw_kernel,
        out_shape=tuple(shapes),
        in_specs=[vmem] * 13,
        out_specs=(hbm,) * 12,
        scratch_shapes=[
            pltpu.VMEM(buf, F32), pltpu.VMEM(buf, F32), pltpu.VMEM(buf, F32), pltpu.VMEM(buf, jnp.bfloat16),
            pltpu.VMEM((3, NORM_ROWS, NORM_COLS), F32), pltpu.VMEM((NORM_ROWS, NORM_COLS), jnp.bfloat16),
            pltpu.SemaphoreType.DMA((4, STORE_SLOTS)), pltpu.SemaphoreType.DMA((4,)),
        ],
        compiler_params=pltpu.CompilerParams(vmem_limit_bytes=8 * 1024 * 1024),
        cost_estimate=pl.CostEstimate(flops=20 * elements, bytes_accessed=30 * elements, transcendentals=2 * elements),
        name="adamw",
    )(scale, *emb, *mat, *norm)


def solution(mesh):
    def local_step(emb_grad, mat_grad, norm_grad, emb_param, emb_mom, emb_var, mat_param, mat_mom, mat_var, norm_param, norm_mom, norm_var):
        emb_mean, mat_mean, norm_mean, scale = reduce_grads(emb_grad[0, 0], mat_grad[0, 0], norm_grad[0, 0])
        return adamw(scale, (emb_mean, emb_param, emb_mom, emb_var), (mat_mean, mat_param, mat_mom, mat_var),
                     (norm_mean, norm_param, norm_mom, norm_var))

    grad_spec = P("dp", "fsdp", None, None)
    row_spec = P("fsdp", None)
    col_spec = P(None, "fsdp")
    in_list = (grad_spec, grad_spec, grad_spec, row_spec, row_spec, row_spec, row_spec, row_spec, row_spec, col_spec, col_spec, col_spec)
    out_list = (row_spec, row_spec, row_spec, row_spec, row_spec, row_spec, row_spec, row_spec, col_spec, col_spec, col_spec, col_spec)
    return jax.shard_map(local_step, mesh=mesh, in_specs=in_list, out_specs=out_list, check_vma=False)
```

```python
import functools
import math

import jax
import jax.numpy as jnp
from jax import lax
from jax.experimental import pallas as pl
from jax.experimental.pallas import tpu as pltpu
from jax.sharding import PartitionSpec as P

LEARN_RATE = 0.003
BETA_ONE = 0.9
BETA_TWO = 0.95
ADAM_EPS = 1e-8
WEIGHT_DECAY = 0.1
CLIP_NORM = 1.0
ADAM_STEP = 10

MESH = pl.DeviceIdType.MESH
F32 = jnp.float32

WIDTH = 5376
NORM_ROWS = 9
NORM_COLS = 672
NORM_PAD = (16, 768)
ROWS = 8
A_COLS = 2048
B_COLS = 2048
HALF = 640
B_AT = A_COLS
C_AT = A_COLS + B_COLS
LAG_ZERO = 3
LAG = 3
P_SLOTS = 10
R_SLOTS = 6
SEND_SLOTS = 8
RING = 20


def reduce_kernel(counts, emb, mat, norm, emb_out, mat_out, norm_out, scale_out,
                  part, recv_zero, xa, yb, zc, mid, wc, tc, grad, square,
                  norm_in, norm_part, norm_a, norm_b, norm_c, norm_d, sum_send, sum_recv, scale,
                  load_sem, zero_send, zero_recv, credit,
                  one_send, one_recv, two_send, two_recv, three_send, three_recv, four_send, four_recv, out_sem,
                  norm_load, norm_send, norm_recv, norm_store, sum_ssem, sum_rsem, scale_sem):
    emb_count, mat_count = counts
    total = emb_count + mat_count
    z = lax.axis_index("dp")
    f = lax.axis_index("fsdp")
    c = lax.rem(f, 2)
    x = lax.rem(lax.div(f, 2), 2)
    y = lax.div(f, 4)
    core = (z, f + 1 - 2 * c)
    xn = (z, f + 2 - 4 * x)
    yn = (z, f + 4 - 8 * y)
    zn = (1 - z, f)
    peers = [(z, lax.rem(f + k, 8)) for k in range(1, 8)]

    def remote(src, dst, ssem, rsem, dev):
        return pltpu.make_async_remote_copy(src_ref=src, dst_ref=dst, send_sem=ssem, recv_sem=rsem,
                                            device_id=dev, device_id_type=MESH)

    def half_at(base, which):
        return pl.ds(pl.multiple_of(base + which * HALF, 128), HALF)

    c_keep, c_give = half_at(C_AT, z), half_at(C_AT, 1 - z)
    a_cols, b_cols, ab_cols = pl.ds(0, A_COLS), pl.ds(B_AT, B_COLS), pl.ds(0, C_AT)

    barrier = pltpu.get_barrier_semaphore()
    for dev in peers + [zn]:
        pl.semaphore_signal(barrier, inc=1, device_id=dev, device_id_type=MESH)
    norm_copy = pltpu.make_async_copy(norm, norm_in, norm_load)
    norm_copy.start()

    def on_rows(j, body):
        @pl.when(j < emb_count)
        def _():
            body(emb, emb_out, pl.multiple_of(j * ROWS, ROWS))

        @pl.when(j >= emb_count)
        def _():
            body(mat, mat_out, pl.multiple_of((j - emb_count) * ROWS, ROWS))

    def load_copy(ref, row, j):
        s = lax.rem(j, P_SLOTS)
        return pltpu.make_async_copy(ref.at[:, :, c, pl.ds(row, ROWS), :], part.at[s], load_sem.at[s])

    def zero_copy(ref, row, j):
        s = lax.rem(j, R_SLOTS)
        return remote(ref.at[:, :, 1 - c, pl.ds(row, ROWS), :], recv_zero.at[s], zero_send.at[s], zero_recv.at[s], core)

    def ones(j):
        s, r = lax.rem(j, P_SLOTS), lax.rem(j, RING)
        return (remote(part.at[s, :, :, :, c_give], zc.at[r], one_send.at[2, s], one_recv.at[2, r], zn),
                remote(part.at[s, :, 1 - x, :, a_cols], xa.at[r], one_send.at[0, s], one_recv.at[0, r], xn),
                remote(part.at[s, 1 - y, :, :, b_cols], yb.at[r], one_send.at[1, s], one_recv.at[1, r], yn))

    def two_c_even(j):
        s, r = lax.rem(j, SEND_SLOTS), lax.rem(j, RING)
        return remote(zc.at[r, :, 1 - x], wc.at[r], two_send.at[2, s], two_recv.at[2, r], xn)

    def two_c_odd(j):
        s, r = lax.rem(j, SEND_SLOTS), lax.rem(j, RING)
        return remote(zc.at[r, 1 - y], wc.at[r], two_send.at[2, s], two_recv.at[2, r], yn)

    def twos(j):
        s, r = lax.rem(j, SEND_SLOTS), lax.rem(j, RING)
        return (remote(xa.at[r, 1 - y], mid.at[r, :, a_cols], two_send.at[0, s], two_recv.at[0, r], yn),
                remote(yb.at[r, 1 - x], mid.at[r, :, b_cols], two_send.at[1, s], two_recv.at[1, r], xn))

    def three_c(j):
        s, r, odd = lax.rem(j, SEND_SLOTS), lax.rem(j, RING), lax.rem(j, 2)
        here = y + odd * (x - y)
        step = (4 - 8 * y) + odd * ((2 - 4 * x) - (4 - 8 * y))
        return remote(wc.at[r, 1 - here], tc.at[r], three_send.at[1, s], three_recv.at[1, r], (z, f + step))

    def three_ab(j):
        s, r = lax.rem(j, SEND_SLOTS), lax.rem(j, RING)
        return remote(mid.at[r], grad.at[r, :, ab_cols], three_send.at[0, s], three_recv.at[0, r], zn)

    def four(j, c_at):
        s, r = lax.rem(j, SEND_SLOTS), lax.rem(j, RING)
        return remote(grad.at[r, :, c_at], grad.at[r, :, c_at], four_send.at[s], four_recv.at[r], zn)

    def out_copy(ref, row, j):
        return pltpu.make_async_copy(grad.at[lax.rem(j, RING)], ref.at[pl.ds(row, ROWS), :],
                                     out_sem.at[lax.rem(j, SEND_SLOTS)])

    norm_zero = remote(norm_part.at[:, :, 1 - c], norm_a, norm_send.at[0], norm_recv.at[0], core)
    norm_one = remote(norm_a.at[:, 1 - x], norm_b, norm_send.at[1], norm_recv.at[1], xn)
    norm_two = remote(norm_b.at[1 - y], norm_c, norm_send.at[2], norm_recv.at[2], yn)
    norm_three = remote(norm_c, norm_d, norm_send.at[3], norm_recv.at[3], zn)

    def when_in(j, body):
        pl.when(jnp.logical_and(j >= 0, j < total))(functools.partial(body, j))

    def start(copies):
        for copy in copies:
            copy.start()

    def wait_send(copies):
        for copy in copies:
            copy.wait_send()

    def stage_issue(j):
        @pl.when(j >= P_SLOTS)
        def _():
            wait_send(ones(j - P_SLOTS))

        @pl.when(j >= R_SLOTS)
        def _():
            zero_copy(emb, 0, j - R_SLOTS).wait_send()
            pl.semaphore_wait(credit, 1)

        def body(ref, _, row):
            zero_copy(ref, row, j).start()
            load_copy(ref, row, j).start()

        on_rows(j, body)

    def stage_one(j):
        load_copy(emb, 0, j).wait()
        zero_copy(emb, 0, j).wait_recv()
        part[lax.rem(j, P_SLOTS)] += recv_zero[lax.rem(j, R_SLOTS)]

        @pl.when(j + R_SLOTS < total)
        def _():
            pl.semaphore_signal(credit, inc=1, device_id=core, device_id_type=MESH)

        start(ones(j))

    def stage_two(j):
        s, r = lax.rem(j, P_SLOTS), lax.rem(j, RING)
        even = lax.rem(j, 2) == 0
        for copy in ones(j):
            copy.wait_recv()
        zc[r] += part[s, :, :, :, c_keep]
        xa[r] += part[s, :, x, :, a_cols]
        yb[r] += part[s, y, :, :, b_cols]

        @pl.when(j >= SEND_SLOTS)
        def _():
            wait_send(twos(j - SEND_SLOTS) + (two_c_even(j - SEND_SLOTS),))

        pl.when(even)(lambda: two_c_even(j).start())
        pl.when(jnp.logical_not(even))(lambda: two_c_odd(j).start())
        start(twos(j))

    def stage_three(j):
        r = lax.rem(j, RING)
        even = lax.rem(j, 2) == 0
        for copy in twos(j) + (two_c_even(j),):
            copy.wait_recv()

        @pl.when(even)
        def _():
            wc[r] += zc[r, :, x]

        @pl.when(jnp.logical_not(even))
        def _():
            wc[r] += zc[r, y]

        mid[r, :, a_cols] += xa[r, y]
        mid[r, :, b_cols] += yb[r, x]

        @pl.when(j >= SEND_SLOTS)
        def _():
            wait_send((three_ab(j - SEND_SLOTS), three_c(j - SEND_SLOTS)))

        start((three_c(j), three_ab(j)))

    def stage_four(j):
        r, odd = lax.rem(j, RING), lax.rem(j, 2)
        here = y + odd * (x - y)
        three_c(j).wait_recv()

        @pl.when(j >= SEND_SLOTS)
        def _():
            four(j - SEND_SLOTS, c_keep).wait_send()

        grad[r, :, c_keep] = (tc[r] + wc[r, here]) * (1.0 / 16.0)
        four(j, c_keep).start()

    def stage_five(j):
        r = lax.rem(j, RING)
        three_ab(j).wait_recv()
        both = (grad[r, :, ab_cols] + mid[r]) * (1.0 / 16.0)
        grad[r, :, ab_cols] = both
        square[:, ab_cols] += both * both
        four(j, c_give).wait_recv()
        rest = grad[r, :, C_AT:]
        square[:, C_AT:] += rest * rest

        @pl.when(j >= SEND_SLOTS)
        def _():
            out_copy(emb_out, 0, j - SEND_SLOTS).wait()

        def body(_, ref, row):
            out_copy(ref, row, j).start()

        on_rows(j, body)

    def trip(it, carry):
        when_in(it, stage_issue)
        when_in(it - LAG_ZERO - 4 * LAG, stage_five)
        when_in(it - LAG_ZERO - 3 * LAG, stage_four)
        when_in(it - LAG_ZERO - 2 * LAG, stage_three)
        when_in(it - LAG_ZERO - LAG, stage_two)
        when_in(it - LAG_ZERO, stage_one)

        @pl.when(it == 5)
        def _():
            norm_copy.wait()
            for k in range(8):
                for row in range(NORM_ROWS):
                    norm_part[k // 4, (k // 2) % 2, k % 2, row:row + 1, :NORM_COLS] = norm_in[row, :, k * NORM_COLS:(k + 1) * NORM_COLS]
            norm_zero.start()

        @pl.when(it == 8)
        def _():
            norm_zero.wait_recv()
            norm_a[...] += norm_part[:, :, c]
            norm_one.start()

        @pl.when(it == 12)
        def _():
            norm_one.wait_recv()
            norm_b[...] += norm_a[:, x]
            norm_two.start()

        @pl.when(it == 16)
        def _():
            norm_two.wait_recv()
            norm_c[...] += norm_b[y]
            norm_three.start()

        @pl.when(it == 20)
        def _():
            norm_three.wait_recv()
            norm_d[...] = (norm_d[...] + norm_c[...]) * (1.0 / 16.0)
            pltpu.make_async_copy(norm_d, norm_out, norm_store).start()

        return carry

    pl.semaphore_wait(barrier, 8)
    norm_part[...] = jnp.zeros_like(norm_part)
    square[...] = jnp.zeros_like(square)
    lax.fori_loop(0, total + LAG_ZERO + 4 * LAG, trip, 0)

    norm_sq = norm_d[...] * norm_d[...]
    local = jnp.sum(square[...]) + jnp.sum(norm_sq)
    value = jnp.full((8, 128), local, F32)
    sum_send[...] = value
    sum_recv[f] = value
    sums = [remote(sum_send, sum_recv.at[f], sum_ssem.at[k], sum_rsem.at[f], dev) for k, dev in enumerate(peers)]
    start(sums)
    wait_send((norm_zero, norm_one, norm_two, norm_three))
    pltpu.make_async_copy(norm_d, norm_out, norm_store).wait()

    def drain(slots, copies):
        def body(j, carry):
            wait_send(copies(j))
            return carry
        lax.fori_loop(total - slots, total, body, 0)

    drain(P_SLOTS, ones)
    drain(R_SLOTS, lambda j: (zero_copy(emb, 0, j),))
    drain(SEND_SLOTS, lambda j: twos(j) + (two_c_even(j), three_ab(j), three_c(j), four(j, c_keep)))

    def last(j, carry):
        out_copy(emb_out, 0, j).wait()
        return carry

    lax.fori_loop(total - SEND_SLOTS, total, last, 0)

    for k in range(1, 8):
        s = lax.rem(f + k, 8)
        remote(sum_send, sum_recv.at[s], sum_ssem.at[0], sum_rsem.at[s], core).wait_recv()
    whole = sum_recv[0]
    for k in range(1, 8):
        whole = whole + sum_recv[k]
    scale[...] = jnp.minimum(1.0, CLIP_NORM / jnp.sqrt(whole))
    scale_copy = pltpu.make_async_copy(scale, scale_out, scale_sem)
    scale_copy.start()
    wait_send(sums)
    scale_copy.wait()


def reduce_grads(emb_grad, mat_grad, norm_grad):
    emb_rows = emb_grad.shape[0] // 8
    mat_rows = mat_grad.shape[0] // 8
    counts = (emb_rows // ROWS, mat_rows // ROWS)
    dma = pltpu.SemaphoreType.DMA
    scratch = [
        pltpu.VMEM((P_SLOTS, 2, 2, ROWS, WIDTH), F32),
        pltpu.VMEM((R_SLOTS, 2, 2, ROWS, WIDTH), F32),
        pltpu.VMEM((RING, 2, ROWS, A_COLS), F32),
        pltpu.VMEM((RING, 2, ROWS, B_COLS), F32),
        pltpu.VMEM((RING, 2, 2, ROWS, HALF), F32),
        pltpu.VMEM((RING, ROWS, C_AT), F32),
        pltpu.VMEM((RING, 2, ROWS, HALF), F32),
        pltpu.VMEM((RING, ROWS, HALF), F32),
        pltpu.VMEM((RING, ROWS, WIDTH), F32),
        pltpu.VMEM((ROWS, WIDTH), F32),
        pltpu.VMEM((NORM_ROWS, 1, WIDTH), F32),
        pltpu.VMEM((2, 2, 2) + NORM_PAD, F32),
        pltpu.VMEM((2, 2) + NORM_PAD, F32),
        pltpu.VMEM((2,) + NORM_PAD, F32),
        pltpu.VMEM(NORM_PAD, F32),
        pltpu.VMEM(NORM_PAD, F32),
        pltpu.VMEM((8, 128), F32),
        pltpu.VMEM((8, 8, 128), F32),
        pltpu.VMEM((8, 128), F32),
        dma((P_SLOTS,)), dma((R_SLOTS,)), dma((R_SLOTS,)), pltpu.SemaphoreType.REGULAR,
        dma((3, P_SLOTS)), dma((3, RING)), dma((3, SEND_SLOTS)), dma((3, RING)),
        dma((2, SEND_SLOTS)), dma((2, RING)), dma((SEND_SLOTS,)), dma((RING,)), dma((SEND_SLOTS,)),
        dma, dma((4,)), dma((4,)), dma, dma((7,)), dma((8,)), dma,
    ]
    hbm = pl.BlockSpec(memory_space=pl.ANY)
    return pl.pallas_call(
        functools.partial(reduce_kernel, counts),
        out_shape=(
            jax.ShapeDtypeStruct((emb_rows, WIDTH), F32),
            jax.ShapeDtypeStruct((mat_rows, WIDTH), F32),
            jax.ShapeDtypeStruct(NORM_PAD, F32),
            jax.ShapeDtypeStruct((8, 128), F32),
        ),
        in_specs=[pl.BlockSpec(memory_space=pltpu.HBM)] * 3,
        out_specs=(hbm,) * 4,
        scratch_shapes=scratch,
        compiler_params=pltpu.CompilerParams(
            collective_id=0, has_side_effects=True, vmem_limit_bytes=28 * 1024 * 1024
        ),
        name="reduce_grads",
    )(*(pltpu.with_memory_space_constraint(grad, pltpu.HBM) for grad in (
        emb_grad.reshape(2, 2, 2, emb_rows, WIDTH), mat_grad.reshape(2, 2, 2, mat_rows, WIDTH),
        norm_grad.reshape(NORM_ROWS, 1, WIDTH))))


BLOCK = 16
COLS = 384
STORE_SLOTS = 4


def adamw_block(grad, param, mom, var, decay_rate):
    new_mom = BETA_ONE * mom + (1.0 - BETA_ONE) * grad
    new_var = BETA_TWO * var + (1.0 - BETA_TWO) * grad * grad
    root = math.sqrt(1.0 - BETA_TWO ** ADAM_STEP)
    step_dir = new_mom / (jnp.sqrt(new_var) + ADAM_EPS * root)
    rate = LEARN_RATE * root / (1.0 - BETA_ONE ** ADAM_STEP)
    return param - (rate * step_dir + (LEARN_RATE * decay_rate) * param), new_mom, new_var


def adamw_kernel(scale, eg, ep, em, ev, mg, mp, mm, mv, ng, np_, nm, nv,
                 ep_out, em_out, ev_out, eb_out, mp_out, mm_out, mv_out, mb_out, np_out, nm_out, nv_out, nb_out,
                 p_buf, m_buf, v_buf, b_buf, n_bufs, nb_buf, sems, n_sems):
    clip = scale[0:1, 0:1]

    def copies(outs, slot, row):
        return [pltpu.make_async_copy(buf.at[slot], out.at[pl.ds(row, BLOCK), :], sems.at[k, slot])
                for k, (buf, out) in enumerate(zip((p_buf, m_buf, v_buf, b_buf), outs))]

    emb_outs = (ep_out, em_out, ev_out, eb_out)
    mat_outs = (mp_out, mm_out, mv_out, mb_out)
    emb_blocks = eg.shape[0] // BLOCK
    mat_blocks = mg.shape[0] // BLOCK

    def run(first, count, ins, outs):
        def body(i, carry):
            j = first + i
            slot = lax.rem(j, STORE_SLOTS)

            @pl.when(j >= STORE_SLOTS)
            def _():
                for copy in copies(emb_outs, slot, 0):
                    copy.wait()

            row = pl.multiple_of(i * BLOCK, BLOCK)
            for col in range(0, WIDTH, COLS):
                cols = pl.ds(col, COLS)
                g, p, m, v = (ref[pl.ds(row, BLOCK), cols] for ref in ins)
                new_p, new_m, new_v = adamw_block(g * clip, p, m, v, WEIGHT_DECAY)
                p_buf[slot, :, cols] = new_p
                m_buf[slot, :, cols] = new_m
                v_buf[slot, :, cols] = new_v
                b_buf[slot, :, cols] = new_p.astype(jnp.bfloat16)
            for copy in copies(outs, slot, row):
                copy.start()
            return carry

        lax.fori_loop(0, count, body, 0)

    run(0, emb_blocks, (eg, ep, em, ev), emb_outs)
    run(emb_blocks, mat_blocks, (mg, mp, mm, mv), mat_outs)
    new_p, new_m, new_v = adamw_block(ng[:NORM_ROWS, :NORM_COLS] * clip, np_[...], nm[...], nv[...], 0.0)
    for k, value in enumerate((new_p, new_m, new_v)):
        n_bufs[k] = value
    nb_buf[...] = new_p.astype(jnp.bfloat16)
    norm_copies = [pltpu.make_async_copy(n_bufs.at[k], out, n_sems.at[k]) for k, out in enumerate((np_out, nm_out, nv_out))]
    norm_copies.append(pltpu.make_async_copy(nb_buf, nb_out, n_sems.at[3]))
    for copy in norm_copies:
        copy.start()
    for slot in range(STORE_SLOTS):
        for copy in copies(emb_outs, slot, 0):
            copy.wait()
    for copy in norm_copies:
        copy.wait()


def adamw(scale, emb, mat, norm):
    shapes = []
    for ref in (emb[1], mat[1], norm[1]):
        shapes += [jax.ShapeDtypeStruct(ref.shape, F32)] * 3 + [jax.ShapeDtypeStruct(ref.shape, jnp.bfloat16)]
    buf = (STORE_SLOTS, BLOCK, WIDTH)
    vmem = pl.BlockSpec(memory_space=pltpu.VMEM)
    hbm = pl.BlockSpec(memory_space=pl.ANY)
    elements = emb[1].size + mat[1].size
    return pl.pallas_call(
        adamw_kernel,
        out_shape=tuple(shapes),
        in_specs=[vmem] * 13,
        out_specs=(hbm,) * 12,
        scratch_shapes=[
            pltpu.VMEM(buf, F32), pltpu.VMEM(buf, F32), pltpu.VMEM(buf, F32), pltpu.VMEM(buf, jnp.bfloat16),
            pltpu.VMEM((3, NORM_ROWS, NORM_COLS), F32), pltpu.VMEM((NORM_ROWS, NORM_COLS), jnp.bfloat16),
            pltpu.SemaphoreType.DMA((4, STORE_SLOTS)), pltpu.SemaphoreType.DMA((4,)),
        ],
        compiler_params=pltpu.CompilerParams(vmem_limit_bytes=8 * 1024 * 1024),
        cost_estimate=pl.CostEstimate(flops=20 * elements, bytes_accessed=30 * elements, transcendentals=2 * elements),
        name="adamw",
    )(scale, *emb, *mat, *norm)


def solution(mesh):
    def local_step(emb_grad, mat_grad, norm_grad, emb_param, emb_mom, emb_var, mat_param, mat_mom, mat_var, norm_param, norm_mom, norm_var):
        emb_mean, mat_mean, norm_mean, scale = reduce_grads(emb_grad[0, 0], mat_grad[0, 0], norm_grad[0, 0])
        return adamw(scale, (emb_mean, emb_param, emb_mom, emb_var), (mat_mean, mat_param, mat_mom, mat_var),
                     (norm_mean, norm_param, norm_mom, norm_var))

    grad_spec = P("dp", "fsdp", None, None)
    row_spec = P("fsdp", None)
    col_spec = P(None, "fsdp")
    in_list = (grad_spec, grad_spec, grad_spec, row_spec, row_spec, row_spec, row_spec, row_spec, row_spec, col_spec, col_spec, col_spec)
    out_list = (row_spec, row_spec, row_spec, row_spec, row_spec, row_spec, row_spec, row_spec, col_spec, col_spec, col_spec, col_spec)
    return jax.shard_map(local_step, mesh=mesh, in_specs=in_list, out_specs=out_list, check_vma=False)
```

```python
import functools
import math

import jax
import jax.numpy as jnp
from jax import lax
from jax.experimental import pallas as pl
from jax.experimental.pallas import tpu as pltpu
from jax.sharding import PartitionSpec as P

LEARN_RATE = 0.003
BETA_ONE = 0.9
BETA_TWO = 0.95
ADAM_EPS = 1e-8
WEIGHT_DECAY = 0.1
CLIP_NORM = 1.0
ADAM_STEP = 10

MESH = pl.DeviceIdType.MESH
F32 = jnp.float32

WIDTH = 5376
NORM_ROWS = 9
NORM_COLS = 672
NORM_PAD = (16, 768)
ROWS = 8
A_COLS = 2048
B_COLS = 2048
HALF = 640
B_AT = A_COLS
C_AT = A_COLS + B_COLS
LAG_ZERO = 3
LAG = 2
P_SLOTS = 10
R_SLOTS = 6
SEND_SLOTS = 8
RING = 20


def reduce_kernel(counts, emb, mat, norm, emb_out, mat_out, norm_out, scale_out,
                  part, recv_zero, xa, yb, zc, mid, wc, tc, grad, square,
                  norm_in, norm_part, norm_a, norm_b, norm_c, norm_d, sum_send, sum_recv,
                  load_sem, zero_send, zero_recv, credit,
                  one_send, one_recv, two_send, two_recv, three_send, three_recv, four_send, four_recv, out_sem,
                  norm_load, norm_send, norm_recv, sum_ssem, sum_rsem):
    emb_count, mat_count = counts
    total = emb_count + mat_count
    z = lax.axis_index("dp")
    f = lax.axis_index("fsdp")
    c = lax.rem(f, 2)
    x = lax.rem(lax.div(f, 2), 2)
    y = lax.div(f, 4)
    core = (z, f + 1 - 2 * c)
    xn = (z, f + 2 - 4 * x)
    yn = (z, f + 4 - 8 * y)
    zn = (1 - z, f)
    peers = [(z, lax.rem(f + k, 8)) for k in range(1, 8)]

    def remote(src, dst, ssem, rsem, dev):
        return pltpu.make_async_remote_copy(src_ref=src, dst_ref=dst, send_sem=ssem, recv_sem=rsem,
                                            device_id=dev, device_id_type=MESH)

    def half_at(base, which):
        return pl.ds(pl.multiple_of(base + which * HALF, 128), HALF)

    c_keep, c_give = half_at(C_AT, z), half_at(C_AT, 1 - z)
    a_cols, b_cols, ab_cols = pl.ds(0, A_COLS), pl.ds(B_AT, B_COLS), pl.ds(0, C_AT)

    barrier = pltpu.get_barrier_semaphore()
    for dev in (core, xn, yn, zn):
        pl.semaphore_signal(barrier, inc=1, device_id=dev, device_id_type=MESH)
    norm_copy = pltpu.make_async_copy(norm, norm_in, norm_load)
    norm_copy.start()

    def on_rows(j, body):
        @pl.when(j < emb_count)
        def _():
            body(emb, emb_out, pl.multiple_of(j * ROWS, ROWS))

        @pl.when(j >= emb_count)
        def _():
            body(mat, mat_out, pl.multiple_of((j - emb_count) * ROWS, ROWS))

    def load_copy(ref, row, j):
        s = lax.rem(j, P_SLOTS)
        return pltpu.make_async_copy(ref.at[:, :, c, pl.ds(row, ROWS), :], part.at[s], load_sem.at[s])

    def zero_copy(ref, row, j):
        s = lax.rem(j, R_SLOTS)
        return remote(ref.at[:, :, 1 - c, pl.ds(row, ROWS), :], recv_zero.at[s], zero_send.at[s], zero_recv.at[s], core)

    def ones(j):
        s, r = lax.rem(j, P_SLOTS), lax.rem(j, RING)
        return (remote(part.at[s, :, :, :, c_give], zc.at[r], one_send.at[2, s], one_recv.at[2, r], zn),
                remote(part.at[s, :, 1 - x, :, a_cols], xa.at[r], one_send.at[0, s], one_recv.at[0, r], xn),
                remote(part.at[s, 1 - y, :, :, b_cols], yb.at[r], one_send.at[1, s], one_recv.at[1, r], yn))

    def two_c_even(j):
        s, r = lax.rem(j, SEND_SLOTS), lax.rem(j, RING)
        return remote(zc.at[r, :, 1 - x], wc.at[r], two_send.at[2, s], two_recv.at[2, r], xn)

    def two_c_odd(j):
        s, r = lax.rem(j, SEND_SLOTS), lax.rem(j, RING)
        return remote(zc.at[r, 1 - y], wc.at[r], two_send.at[2, s], two_recv.at[2, r], yn)

    def twos(j):
        s, r = lax.rem(j, SEND_SLOTS), lax.rem(j, RING)
        return (remote(xa.at[r, 1 - y], mid.at[r, :, a_cols], two_send.at[0, s], two_recv.at[0, r], yn),
                remote(yb.at[r, 1 - x], mid.at[r, :, b_cols], two_send.at[1, s], two_recv.at[1, r], xn))

    def three_c(j):
        s, r, odd = lax.rem(j, SEND_SLOTS), lax.rem(j, RING), lax.rem(j, 2)
        here = y + odd * (x - y)
        step = (4 - 8 * y) + odd * ((2 - 4 * x) - (4 - 8 * y))
        return remote(wc.at[r, 1 - here], tc.at[r], three_send.at[1, s], three_recv.at[1, r], (z, f + step))

    def three_ab(j):
        s, r = lax.rem(j, SEND_SLOTS), lax.rem(j, RING)
        return remote(mid.at[r], grad.at[r, :, ab_cols], three_send.at[0, s], three_recv.at[0, r], zn)

    def four(j, c_at):
        s, r = lax.rem(j, SEND_SLOTS), lax.rem(j, RING)
        return remote(grad.at[r, :, c_at], grad.at[r, :, c_at], four_send.at[s], four_recv.at[r], zn)

    def out_copy(ref, row, j):
        return pltpu.make_async_copy(grad.at[lax.rem(j, RING)], ref.at[pl.ds(row, ROWS), :],
                                     out_sem.at[lax.rem(j, SEND_SLOTS)])

    norm_zero = remote(norm_part.at[:, :, 1 - c], norm_a, norm_send.at[0], norm_recv.at[0], core)
    norm_one = remote(norm_a.at[:, 1 - x], norm_b, norm_send.at[1], norm_recv.at[1], xn)
    norm_two = remote(norm_b.at[1 - y], norm_c, norm_send.at[2], norm_recv.at[2], yn)
    norm_three = remote(norm_c, norm_d, norm_send.at[3], norm_recv.at[3], zn)

    def when_in(j, body):
        pl.when(jnp.logical_and(j >= 0, j < total))(functools.partial(body, j))

    def start(copies):
        for copy in copies:
            copy.start()

    def wait_send(copies):
        for copy in copies:
            copy.wait_send()

    def stage_issue(j):
        @pl.when(j >= P_SLOTS)
        def _():
            wait_send(ones(j - P_SLOTS))

        @pl.when(j >= R_SLOTS)
        def _():
            zero_copy(emb, 0, j - R_SLOTS).wait_send()
            pl.semaphore_wait(credit, 1)

        def body(ref, _, row):
            zero_copy(ref, row, j).start()
            load_copy(ref, row, j).start()

        on_rows(j, body)

    def stage_one(j):
        load_copy(emb, 0, j).wait()
        zero_copy(emb, 0, j).wait_recv()
        part[lax.rem(j, P_SLOTS)] += recv_zero[lax.rem(j, R_SLOTS)]

        @pl.when(j + R_SLOTS < total)
        def _():
            pl.semaphore_signal(credit, inc=1, device_id=core, device_id_type=MESH)

        start(ones(j)[:1])

    def stage_one_more(j):
        start(ones(j)[1:])

    def stage_two(j):
        s, r = lax.rem(j, P_SLOTS), lax.rem(j, RING)
        even = lax.rem(j, 2) == 0
        for copy in ones(j):
            copy.wait_recv()
        zc[r] += part[s, :, :, :, c_keep]
        xa[r] += part[s, :, x, :, a_cols]
        yb[r] += part[s, y, :, :, b_cols]

        @pl.when(j >= SEND_SLOTS)
        def _():
            wait_send(twos(j - SEND_SLOTS) + (two_c_even(j - SEND_SLOTS),))

        pl.when(even)(lambda: two_c_even(j).start())
        pl.when(jnp.logical_not(even))(lambda: two_c_odd(j).start())
        start(twos(j))

    def stage_three(j):
        r = lax.rem(j, RING)
        even = lax.rem(j, 2) == 0
        for copy in twos(j) + (two_c_even(j),):
            copy.wait_recv()

        @pl.when(even)
        def _():
            wc[r] += zc[r, :, x]

        @pl.when(jnp.logical_not(even))
        def _():
            wc[r] += zc[r, y]

        mid[r, :, a_cols] += xa[r, y]
        mid[r, :, b_cols] += yb[r, x]

        @pl.when(j >= SEND_SLOTS)
        def _():
            wait_send((three_ab(j - SEND_SLOTS), three_c(j - SEND_SLOTS)))

        start((three_c(j), three_ab(j)))

    def stage_four(j):
        r, odd = lax.rem(j, RING), lax.rem(j, 2)
        here = y + odd * (x - y)
        three_c(j).wait_recv()

        @pl.when(j >= SEND_SLOTS)
        def _():
            four(j - SEND_SLOTS, c_keep).wait_send()

        grad[r, :, c_keep] = (tc[r] + wc[r, here]) * (1.0 / 16.0)
        four(j, c_keep).start()

    def stage_five(j):
        r = lax.rem(j, RING)
        three_ab(j).wait_recv()
        both = (grad[r, :, ab_cols] + mid[r]) * (1.0 / 16.0)
        grad[r, :, ab_cols] = both
        square[:, ab_cols] += both * both
        four(j, c_give).wait_recv()
        rest = grad[r, :, C_AT:]
        square[:, C_AT:] += rest * rest

        @pl.when(j >= SEND_SLOTS)
        def _():
            out_copy(emb_out, 0, j - SEND_SLOTS).wait()

        def body(_, ref, row):
            out_copy(ref, row, j).start()

        on_rows(j, body)

    def trip(it, carry):
        when_in(it, stage_issue)
        when_in(it - LAG_ZERO, stage_one)
        when_in(it - LAG_ZERO - 4 * LAG, stage_five)
        when_in(it - LAG_ZERO - 3 * LAG, stage_four)
        when_in(it - LAG_ZERO - 2 * LAG, stage_three)
        when_in(it - LAG_ZERO - LAG, stage_two)
        when_in(it - LAG_ZERO, stage_one_more)

        @pl.when(it == 5)
        def _():
            norm_copy.wait()
            for k in range(8):
                for row in range(NORM_ROWS):
                    norm_part[k // 4, (k // 2) % 2, k % 2, row:row + 1, :NORM_COLS] = norm_in[row, :, k * NORM_COLS:(k + 1) * NORM_COLS]
            norm_zero.start()

        @pl.when(it == 8)
        def _():
            norm_zero.wait_recv()
            norm_a[...] += norm_part[:, :, c]
            norm_one.start()

        @pl.when(it == 12)
        def _():
            norm_one.wait_recv()
            norm_b[...] += norm_a[:, x]
            norm_two.start()

        @pl.when(it == 16)
        def _():
            norm_two.wait_recv()
            norm_c[...] += norm_b[y]
            norm_three.start()

        @pl.when(it == 20)
        def _():
            norm_three.wait_recv()
            norm_d[...] = (norm_d[...] + norm_c[...]) * (1.0 / 16.0)
            norm_out[...] = norm_d[...]

        return carry

    norm_part[...] = jnp.zeros_like(norm_part)
    square[...] = jnp.zeros_like(square)
    pl.semaphore_wait(barrier, 4)
    lax.fori_loop(0, total + LAG_ZERO + 4 * LAG, trip, 0)

    norm_sq = norm_d[...] * norm_d[...]
    local = jnp.sum(square[...]) + jnp.sum(norm_sq)
    value = jnp.full((8, 128), local, F32)
    sum_send[...] = value
    sum_recv[f] = value
    sums = [remote(sum_send, sum_recv.at[f], sum_ssem.at[k], sum_rsem.at[f], dev) for k, dev in enumerate(peers)]
    start(sums)
    wait_send((norm_zero, norm_one, norm_two, norm_three))

    def drain(slots, copies):
        def body(j, carry):
            wait_send(copies(j))
            return carry
        lax.fori_loop(total - slots, total, body, 0)

    drain(P_SLOTS, ones)
    drain(R_SLOTS, lambda j: (zero_copy(emb, 0, j),))
    drain(SEND_SLOTS, lambda j: twos(j) + (two_c_even(j), three_ab(j), three_c(j), four(j, c_keep)))

    def last(j, carry):
        out_copy(emb_out, 0, j).wait()
        return carry

    lax.fori_loop(total - SEND_SLOTS, total, last, 0)

    for k in range(1, 8):
        s = lax.rem(f + k, 8)
        remote(sum_send, sum_recv.at[s], sum_ssem.at[0], sum_rsem.at[s], core).wait_recv()
    whole = sum_recv[0]
    for k in range(1, 8):
        whole = whole + sum_recv[k]
    scale_out[...] = jnp.minimum(1.0, CLIP_NORM / jnp.sqrt(whole))
    wait_send(sums)


def reduce_grads(emb_grad, mat_grad, norm_grad):
    emb_rows = emb_grad.shape[0] // 8
    mat_rows = mat_grad.shape[0] // 8
    counts = (emb_rows // ROWS, mat_rows // ROWS)
    dma = pltpu.SemaphoreType.DMA
    scratch = [
        pltpu.VMEM((P_SLOTS, 2, 2, ROWS, WIDTH), F32),
        pltpu.VMEM((R_SLOTS, 2, 2, ROWS, WIDTH), F32),
        pltpu.VMEM((RING, 2, ROWS, A_COLS), F32),
        pltpu.VMEM((RING, 2, ROWS, B_COLS), F32),
        pltpu.VMEM((RING, 2, 2, ROWS, HALF), F32),
        pltpu.VMEM((RING, ROWS, C_AT), F32),
        pltpu.VMEM((RING, 2, ROWS, HALF), F32),
        pltpu.VMEM((RING, ROWS, HALF), F32),
        pltpu.VMEM((RING, ROWS, WIDTH), F32),
        pltpu.VMEM((ROWS, WIDTH), F32),
        pltpu.VMEM((NORM_ROWS, 1, WIDTH), F32),
        pltpu.VMEM((2, 2, 2) + NORM_PAD, F32),
        pltpu.VMEM((2, 2) + NORM_PAD, F32),
        pltpu.VMEM((2,) + NORM_PAD, F32),
        pltpu.VMEM(NORM_PAD, F32),
        pltpu.VMEM(NORM_PAD, F32),
        pltpu.VMEM((8, 128), F32),
        pltpu.VMEM((8, 8, 128), F32),
        dma((P_SLOTS,)), dma((R_SLOTS,)), dma((R_SLOTS,)), pltpu.SemaphoreType.REGULAR,
        dma((3, P_SLOTS)), dma((3, RING)), dma((3, SEND_SLOTS)), dma((3, RING)),
        dma((2, SEND_SLOTS)), dma((2, RING)), dma((SEND_SLOTS,)), dma((RING,)), dma((SEND_SLOTS,)),
        dma, dma((4,)), dma((4,)), dma((7,)), dma((8,)),
    ]
    hbm = pl.BlockSpec(memory_space=pl.ANY)
    vmem = pl.BlockSpec(memory_space=pltpu.VMEM)
    return pl.pallas_call(
        functools.partial(reduce_kernel, counts),
        out_shape=(
            jax.ShapeDtypeStruct((emb_rows, WIDTH), F32),
            jax.ShapeDtypeStruct((mat_rows, WIDTH), F32),
            jax.ShapeDtypeStruct(NORM_PAD, F32),
            jax.ShapeDtypeStruct((8, 128), F32),
        ),
        in_specs=[pl.BlockSpec(memory_space=pltpu.HBM)] * 3,
        out_specs=(hbm, hbm, vmem, vmem),
        scratch_shapes=scratch,
        compiler_params=pltpu.CompilerParams(
            collective_id=0, has_side_effects=True, vmem_limit_bytes=28 * 1024 * 1024
        ),
        name="reduce_grads",
    )(*(pltpu.with_memory_space_constraint(grad, pltpu.HBM) for grad in (
        emb_grad.reshape(2, 2, 2, emb_rows, WIDTH), mat_grad.reshape(2, 2, 2, mat_rows, WIDTH),
        norm_grad.reshape(NORM_ROWS, 1, WIDTH))))


BLOCK = 16
COLS = 384
STORE_SLOTS = 4


def adamw_block(grad, param, mom, var, decay_rate):
    new_mom = BETA_ONE * mom + (1.0 - BETA_ONE) * grad
    new_var = BETA_TWO * var + (1.0 - BETA_TWO) * grad * grad
    root = math.sqrt(1.0 - BETA_TWO ** ADAM_STEP)
    step_dir = new_mom / (jnp.sqrt(new_var) + ADAM_EPS * root)
    rate = LEARN_RATE * root / (1.0 - BETA_ONE ** ADAM_STEP)
    return param - (rate * step_dir + (LEARN_RATE * decay_rate) * param), new_mom, new_var


def adamw_kernel(scale, eg, ep, em, ev, mg, mp, mm, mv, ng, np_, nm, nv,
                 ep_out, em_out, ev_out, eb_out, mp_out, mm_out, mv_out, mb_out, np_out, nm_out, nv_out, nb_out,
                 p_buf, m_buf, v_buf, b_buf, n_bufs, nb_buf, sems, n_sems):
    clip = scale[0:1, 0:1]

    def copies(outs, slot, row):
        return [pltpu.make_async_copy(buf.at[slot], out.at[pl.ds(row, BLOCK), :], sems.at[k, slot])
                for k, (buf, out) in enumerate(zip((p_buf, m_buf, v_buf, b_buf), outs))]

    emb_outs = (ep_out, em_out, ev_out, eb_out)
    mat_outs = (mp_out, mm_out, mv_out, mb_out)
    emb_blocks = eg.shape[0] // BLOCK
    mat_blocks = mg.shape[0] // BLOCK

    def run(first, count, ins, outs):
        def body(i, carry):
            j = first + i
            slot = lax.rem(j, STORE_SLOTS)

            @pl.when(j >= STORE_SLOTS)
            def _():
                for copy in copies(emb_outs, slot, 0):
                    copy.wait()

            row = pl.multiple_of(i * BLOCK, BLOCK)
            for col in range(0, WIDTH, COLS):
                cols = pl.ds(col, COLS)
                g, p, m, v = (ref[pl.ds(row, BLOCK), cols] for ref in ins)
                new_p, new_m, new_v = adamw_block(g * clip, p, m, v, WEIGHT_DECAY)
                p_buf[slot, :, cols] = new_p
                m_buf[slot, :, cols] = new_m
                v_buf[slot, :, cols] = new_v
                b_buf[slot, :, cols] = new_p.astype(jnp.bfloat16)
            for copy in copies(outs, slot, row):
                copy.start()
            return carry

        lax.fori_loop(0, count, body, 0)

    run(0, emb_blocks, (eg, ep, em, ev), emb_outs)
    run(emb_blocks, mat_blocks, (mg, mp, mm, mv), mat_outs)
    new_p, new_m, new_v = adamw_block(ng[:NORM_ROWS, :NORM_COLS] * clip, np_[...], nm[...], nv[...], 0.0)
    for k, value in enumerate((new_p, new_m, new_v)):
        n_bufs[k] = value
    nb_buf[...] = new_p.astype(jnp.bfloat16)
    norm_copies = [pltpu.make_async_copy(n_bufs.at[k], out, n_sems.at[k]) for k, out in enumerate((np_out, nm_out, nv_out))]
    norm_copies.append(pltpu.make_async_copy(nb_buf, nb_out, n_sems.at[3]))
    for copy in norm_copies:
        copy.start()
    for slot in range(STORE_SLOTS):
        for copy in copies(emb_outs, slot, 0):
            copy.wait()
    for copy in norm_copies:
        copy.wait()


def adamw(scale, emb, mat, norm):
    shapes = []
    for ref in (emb[1], mat[1], norm[1]):
        shapes += [jax.ShapeDtypeStruct(ref.shape, F32)] * 3 + [jax.ShapeDtypeStruct(ref.shape, jnp.bfloat16)]
    buf = (STORE_SLOTS, BLOCK, WIDTH)
    vmem = pl.BlockSpec(memory_space=pltpu.VMEM)
    hbm = pl.BlockSpec(memory_space=pl.ANY)
    elements = emb[1].size + mat[1].size
    return pl.pallas_call(
        adamw_kernel,
        out_shape=tuple(shapes),
        in_specs=[vmem] * 13,
        out_specs=(hbm,) * 12,
        scratch_shapes=[
            pltpu.VMEM(buf, F32), pltpu.VMEM(buf, F32), pltpu.VMEM(buf, F32), pltpu.VMEM(buf, jnp.bfloat16),
            pltpu.VMEM((3, NORM_ROWS, NORM_COLS), F32), pltpu.VMEM((NORM_ROWS, NORM_COLS), jnp.bfloat16),
            pltpu.SemaphoreType.DMA((4, STORE_SLOTS)), pltpu.SemaphoreType.DMA((4,)),
        ],
        compiler_params=pltpu.CompilerParams(vmem_limit_bytes=8 * 1024 * 1024),
        cost_estimate=pl.CostEstimate(flops=20 * elements, bytes_accessed=30 * elements, transcendentals=2 * elements),
        name="adamw",
    )(scale, *emb, *mat, *norm)


def solution(mesh):
    def local_step(emb_grad, mat_grad, norm_grad, emb_param, emb_mom, emb_var, mat_param, mat_mom, mat_var, norm_param, norm_mom, norm_var):
        emb_mean, mat_mean, norm_mean, scale = reduce_grads(emb_grad[0, 0], mat_grad[0, 0], norm_grad[0, 0])
        return adamw(scale, (emb_mean, emb_param, emb_mom, emb_var), (mat_mean, mat_param, mat_mom, mat_var),
                     (norm_mean, norm_param, norm_mom, norm_var))

    grad_spec = P("dp", "fsdp", None, None)
    row_spec = P("fsdp", None)
    col_spec = P(None, "fsdp")
    in_list = (grad_spec, grad_spec, grad_spec, row_spec, row_spec, row_spec, row_spec, row_spec, row_spec, col_spec, col_spec, col_spec)
    out_list = (row_spec, row_spec, row_spec, row_spec, row_spec, row_spec, row_spec, row_spec, col_spec, col_spec, col_spec, col_spec)
    return jax.shard_map(local_step, mesh=mesh, in_specs=in_list, out_specs=out_list, check_vma=False)
```

```python
import functools
import math

import jax
import jax.numpy as jnp
from jax import lax
from jax.experimental import pallas as pl
from jax.experimental.pallas import tpu as pltpu
from jax.sharding import PartitionSpec as P

LEARN_RATE = 0.003
BETA_ONE = 0.9
BETA_TWO = 0.95
ADAM_EPS = 1e-8
WEIGHT_DECAY = 0.1
CLIP_NORM = 1.0
ADAM_STEP = 10

MESH = pl.DeviceIdType.MESH
F32 = jnp.float32

WIDTH = 5376
NORM_ROWS = 9
NORM_COLS = 672
NORM_PAD = (16, 768)
ROWS = 8
A_COLS = 2048
B_COLS = 2048
HALF = 640
B_AT = A_COLS
C_AT = A_COLS + B_COLS
LAG_ZERO = 1
LAG = 2
P_SLOTS = 10
R_SLOTS = 6
SEND_SLOTS = 8
RING = 20


def reduce_kernel(counts, emb, mat, norm, emb_out, mat_out, norm_out, scale_out,
                  part, recv_zero, xa, yb, zc, mid, wc, tc, grad, square,
                  norm_in, norm_part, norm_a, norm_b, norm_c, norm_d, sum_send, sum_recv,
                  load_sem, zero_send, zero_recv, credit,
                  one_send, one_recv, two_send, two_recv, three_send, three_recv, four_send, four_recv, out_sem,
                  norm_load, norm_send, norm_recv, sum_ssem, sum_rsem):
    emb_count, mat_count = counts
    total = emb_count + mat_count
    z = lax.axis_index("dp")
    f = lax.axis_index("fsdp")
    c = lax.rem(f, 2)
    x = lax.rem(lax.div(f, 2), 2)
    y = lax.div(f, 4)
    core = (z, f + 1 - 2 * c)
    xn = (z, f + 2 - 4 * x)
    yn = (z, f + 4 - 8 * y)
    zn = (1 - z, f)
    peers = [(z, lax.rem(f + k, 8)) for k in range(1, 8)]

    def remote(src, dst, ssem, rsem, dev):
        return pltpu.make_async_remote_copy(src_ref=src, dst_ref=dst, send_sem=ssem, recv_sem=rsem,
                                            device_id=dev, device_id_type=MESH)

    def half_at(base, which):
        return pl.ds(pl.multiple_of(base + which * HALF, 128), HALF)

    c_keep, c_give = half_at(C_AT, z), half_at(C_AT, 1 - z)
    a_cols, b_cols, ab_cols = pl.ds(0, A_COLS), pl.ds(B_AT, B_COLS), pl.ds(0, C_AT)

    barrier = pltpu.get_barrier_semaphore()
    for dev in (core, xn, yn, zn):
        pl.semaphore_signal(barrier, inc=1, device_id=dev, device_id_type=MESH)
    norm_copy = pltpu.make_async_copy(norm, norm_in, norm_load)
    norm_copy.start()

    def on_rows(j, body):
        @pl.when(j < emb_count)
        def _():
            body(emb, emb_out, pl.multiple_of(j * ROWS, ROWS))

        @pl.when(j >= emb_count)
        def _():
            body(mat, mat_out, pl.multiple_of((j - emb_count) * ROWS, ROWS))

    def load_copy(ref, row, j):
        s = lax.rem(j, P_SLOTS)
        return pltpu.make_async_copy(ref.at[:, :, c, pl.ds(row, ROWS), :], part.at[s], load_sem.at[s])

    def zero_copy(ref, row, j):
        s = lax.rem(j, R_SLOTS)
        return remote(ref.at[:, :, 1 - c, pl.ds(row, ROWS), :], recv_zero.at[s], zero_send.at[s], zero_recv.at[s], core)

    def ones(j):
        s, r = lax.rem(j, P_SLOTS), lax.rem(j, RING)
        return (remote(part.at[s, :, :, :, c_give], zc.at[r], one_send.at[2, s], one_recv.at[2, r], zn),
                remote(part.at[s, :, 1 - x, :, a_cols], xa.at[r], one_send.at[0, s], one_recv.at[0, r], xn),
                remote(part.at[s, 1 - y, :, :, b_cols], yb.at[r], one_send.at[1, s], one_recv.at[1, r], yn))

    def two_c_even(j):
        s, r = lax.rem(j, SEND_SLOTS), lax.rem(j, RING)
        return remote(zc.at[r, :, 1 - x], wc.at[r], two_send.at[2, s], two_recv.at[2, r], xn)

    def two_c_odd(j):
        s, r = lax.rem(j, SEND_SLOTS), lax.rem(j, RING)
        return remote(zc.at[r, 1 - y], wc.at[r], two_send.at[2, s], two_recv.at[2, r], yn)

    def twos(j):
        s, r = lax.rem(j, SEND_SLOTS), lax.rem(j, RING)
        return (remote(xa.at[r, 1 - y], mid.at[r, :, a_cols], two_send.at[0, s], two_recv.at[0, r], yn),
                remote(yb.at[r, 1 - x], mid.at[r, :, b_cols], two_send.at[1, s], two_recv.at[1, r], xn))

    def three_c(j):
        s, r, odd = lax.rem(j, SEND_SLOTS), lax.rem(j, RING), lax.rem(j, 2)
        here = y + odd * (x - y)
        step = (4 - 8 * y) + odd * ((2 - 4 * x) - (4 - 8 * y))
        return remote(wc.at[r, 1 - here], tc.at[r], three_send.at[1, s], three_recv.at[1, r], (z, f + step))

    def three_ab(j):
        s, r = lax.rem(j, SEND_SLOTS), lax.rem(j, RING)
        return remote(mid.at[r], grad.at[r, :, ab_cols], three_send.at[0, s], three_recv.at[0, r], zn)

    def four(j, c_at):
        s, r = lax.rem(j, SEND_SLOTS), lax.rem(j, RING)
        return remote(grad.at[r, :, c_at], grad.at[r, :, c_at], four_send.at[s], four_recv.at[r], zn)

    def out_copy(ref, row, j):
        return pltpu.make_async_copy(grad.at[lax.rem(j, RING)], ref.at[pl.ds(row, ROWS), :],
                                     out_sem.at[lax.rem(j, SEND_SLOTS)])

    norm_zero = remote(norm_part.at[:, :, 1 - c], norm_a, norm_send.at[0], norm_recv.at[0], core)
    norm_one = remote(norm_a.at[:, 1 - x], norm_b, norm_send.at[1], norm_recv.at[1], xn)
    norm_two = remote(norm_b.at[1 - y], norm_c, norm_send.at[2], norm_recv.at[2], yn)
    norm_three = remote(norm_c, norm_d, norm_send.at[3], norm_recv.at[3], zn)

    def when_in(j, body):
        pl.when(jnp.logical_and(j >= 0, j < total))(functools.partial(body, j))

    def start(copies):
        for copy in copies:
            copy.start()

    def wait_send(copies):
        for copy in copies:
            copy.wait_send()

    def stage_issue(j):
        @pl.when(j >= P_SLOTS)
        def _():
            wait_send(ones(j - P_SLOTS))

        @pl.when(j >= R_SLOTS)
        def _():
            zero_copy(emb, 0, j - R_SLOTS).wait_send()
            pl.semaphore_wait(credit, 1)

        def body(ref, _, row):
            zero_copy(ref, row, j).start()
            load_copy(ref, row, j).start()

        on_rows(j, body)

    def stage_one(j):
        load_copy(emb, 0, j).wait()
        zero_copy(emb, 0, j).wait_recv()
        part[lax.rem(j, P_SLOTS)] += recv_zero[lax.rem(j, R_SLOTS)]

        @pl.when(j + R_SLOTS < total)
        def _():
            pl.semaphore_signal(credit, inc=1, device_id=core, device_id_type=MESH)

        start(ones(j)[:1])

    def stage_one_more(j):
        start(ones(j)[1:])

    def stage_two(j):
        s, r = lax.rem(j, P_SLOTS), lax.rem(j, RING)
        even = lax.rem(j, 2) == 0
        for copy in ones(j):
            copy.wait_recv()
        zc[r] += part[s, :, :, :, c_keep]
        xa[r] += part[s, :, x, :, a_cols]
        yb[r] += part[s, y, :, :, b_cols]

        @pl.when(j >= SEND_SLOTS)
        def _():
            wait_send(twos(j - SEND_SLOTS) + (two_c_even(j - SEND_SLOTS),))

        pl.when(even)(lambda: two_c_even(j).start())
        pl.when(jnp.logical_not(even))(lambda: two_c_odd(j).start())
        start(twos(j))

    def stage_three(j):
        r = lax.rem(j, RING)
        even = lax.rem(j, 2) == 0
        for copy in twos(j) + (two_c_even(j),):
            copy.wait_recv()

        @pl.when(even)
        def _():
            wc[r] += zc[r, :, x]

        @pl.when(jnp.logical_not(even))
        def _():
            wc[r] += zc[r, y]

        mid[r, :, a_cols] += xa[r, y]
        mid[r, :, b_cols] += yb[r, x]

        @pl.when(j >= SEND_SLOTS)
        def _():
            wait_send((three_ab(j - SEND_SLOTS), three_c(j - SEND_SLOTS)))

        start((three_c(j), three_ab(j)))

    def stage_four(j):
        r, odd = lax.rem(j, RING), lax.rem(j, 2)
        here = y + odd * (x - y)
        three_c(j).wait_recv()

        @pl.when(j >= SEND_SLOTS)
        def _():
            four(j - SEND_SLOTS, c_keep).wait_send()

        grad[r, :, c_keep] = (tc[r] + wc[r, here]) * (1.0 / 16.0)
        four(j, c_keep).start()

    def stage_five(j):
        r = lax.rem(j, RING)
        three_ab(j).wait_recv()
        both = (grad[r, :, ab_cols] + mid[r]) * (1.0 / 16.0)
        grad[r, :, ab_cols] = both
        square[:, ab_cols] += both * both
        four(j, c_give).wait_recv()
        rest = grad[r, :, C_AT:]
        square[:, C_AT:] += rest * rest

        @pl.when(j >= SEND_SLOTS)
        def _():
            out_copy(emb_out, 0, j - SEND_SLOTS).wait()

        def body(_, ref, row):
            out_copy(ref, row, j).start()

        on_rows(j, body)

    def trip(it, carry):
        when_in(it, stage_issue)
        when_in(it - LAG_ZERO, stage_one)
        when_in(it - LAG_ZERO - 4 * LAG, stage_five)
        when_in(it - LAG_ZERO - 3 * LAG, stage_four)
        when_in(it - LAG_ZERO - 2 * LAG, stage_three)
        when_in(it - LAG_ZERO - LAG, stage_two)
        when_in(it - LAG_ZERO, stage_one_more)

        @pl.when(it == 5)
        def _():
            norm_copy.wait()
            for k in range(8):
                for row in range(NORM_ROWS):
                    norm_part[k // 4, (k // 2) % 2, k % 2, row:row + 1, :NORM_COLS] = norm_in[row, :, k * NORM_COLS:(k + 1) * NORM_COLS]
            norm_zero.start()

        @pl.when(it == 8)
        def _():
            norm_zero.wait_recv()
            norm_a[...] += norm_part[:, :, c]
            norm_one.start()

        @pl.when(it == 12)
        def _():
            norm_one.wait_recv()
            norm_b[...] += norm_a[:, x]
            norm_two.start()

        @pl.when(it == 16)
        def _():
            norm_two.wait_recv()
            norm_c[...] += norm_b[y]
            norm_three.start()

        @pl.when(it == 20)
        def _():
            norm_three.wait_recv()
            norm_d[...] = (norm_d[...] + norm_c[...]) * (1.0 / 16.0)
            norm_out[...] = norm_d[...]
            norm_sq = norm_d[...] * norm_d[...]
            square[:, :NORM_PAD[1]] += norm_sq[:ROWS] + norm_sq[ROWS:]

        return carry

    norm_part[...] = jnp.zeros_like(norm_part)
    square[...] = jnp.zeros_like(square)
    pl.semaphore_wait(barrier, 4)
    lax.fori_loop(0, total + LAG_ZERO + 4 * LAG, trip, 0)

    value = jnp.full((8, 128), jnp.sum(square[...]), F32)
    sum_send[...] = value
    sum_recv[f] = value
    sums = [remote(sum_send, sum_recv.at[f], sum_ssem.at[k], sum_rsem.at[f], dev) for k, dev in enumerate(peers)]
    start(sums)
    wait_send((norm_zero, norm_one, norm_two, norm_three))

    def drain(slots, copies):
        def body(j, carry):
            wait_send(copies(j))
            return carry
        lax.fori_loop(total - slots, total, body, 0)

    drain(P_SLOTS, ones)
    drain(R_SLOTS, lambda j: (zero_copy(emb, 0, j),))
    drain(SEND_SLOTS, lambda j: twos(j) + (two_c_even(j), three_ab(j), three_c(j), four(j, c_keep)))

    def last(j, carry):
        out_copy(emb_out, 0, j).wait()
        return carry

    lax.fori_loop(total - SEND_SLOTS, total, last, 0)

    for k in range(1, 8):
        s = lax.rem(f + k, 8)
        remote(sum_send, sum_recv.at[s], sum_ssem.at[0], sum_rsem.at[s], core).wait_recv()
    whole = sum_recv[0]
    for k in range(1, 8):
        whole = whole + sum_recv[k]
    scale_out[...] = jnp.minimum(1.0, CLIP_NORM / jnp.sqrt(whole))
    wait_send(sums)


def reduce_grads(emb_grad, mat_grad, norm_grad):
    emb_rows = emb_grad.shape[0] // 8
    mat_rows = mat_grad.shape[0] // 8
    counts = (emb_rows // ROWS, mat_rows // ROWS)
    dma = pltpu.SemaphoreType.DMA
    scratch = [
        pltpu.VMEM((P_SLOTS, 2, 2, ROWS, WIDTH), F32),
        pltpu.VMEM((R_SLOTS, 2, 2, ROWS, WIDTH), F32),
        pltpu.VMEM((RING, 2, ROWS, A_COLS), F32),
        pltpu.VMEM((RING, 2, ROWS, B_COLS), F32),
        pltpu.VMEM((RING, 2, 2, ROWS, HALF), F32),
        pltpu.VMEM((RING, ROWS, C_AT), F32),
        pltpu.VMEM((RING, 2, ROWS, HALF), F32),
        pltpu.VMEM((RING, ROWS, HALF), F32),
        pltpu.VMEM((RING, ROWS, WIDTH), F32),
        pltpu.VMEM((ROWS, WIDTH), F32),
        pltpu.VMEM((NORM_ROWS, 1, WIDTH), F32),
        pltpu.VMEM((2, 2, 2) + NORM_PAD, F32),
        pltpu.VMEM((2, 2) + NORM_PAD, F32),
        pltpu.VMEM((2,) + NORM_PAD, F32),
        pltpu.VMEM(NORM_PAD, F32),
        pltpu.VMEM(NORM_PAD, F32),
        pltpu.VMEM((8, 128), F32),
        pltpu.VMEM((8, 8, 128), F32),
        dma((P_SLOTS,)), dma((R_SLOTS,)), dma((R_SLOTS,)), pltpu.SemaphoreType.REGULAR,
        dma((3, P_SLOTS)), dma((3, RING)), dma((3, SEND_SLOTS)), dma((3, RING)),
        dma((2, SEND_SLOTS)), dma((2, RING)), dma((SEND_SLOTS,)), dma((RING,)), dma((SEND_SLOTS,)),
        dma, dma((4,)), dma((4,)), dma((7,)), dma((8,)),
    ]
    hbm = pl.BlockSpec(memory_space=pl.ANY)
    vmem = pl.BlockSpec(memory_space=pltpu.VMEM)
    return pl.pallas_call(
        functools.partial(reduce_kernel, counts),
        out_shape=(
            jax.ShapeDtypeStruct((emb_rows, WIDTH), F32),
            jax.ShapeDtypeStruct((mat_rows, WIDTH), F32),
            jax.ShapeDtypeStruct(NORM_PAD, F32),
            jax.ShapeDtypeStruct((8, 128), F32),
        ),
        in_specs=[pl.BlockSpec(memory_space=pltpu.HBM)] * 3,
        out_specs=(hbm, hbm, vmem, vmem),
        scratch_shapes=scratch,
        compiler_params=pltpu.CompilerParams(
            collective_id=0, has_side_effects=True, vmem_limit_bytes=28 * 1024 * 1024
        ),
        name="reduce_grads",
    )(*(pltpu.with_memory_space_constraint(grad, pltpu.HBM) for grad in (
        emb_grad.reshape(2, 2, 2, emb_rows, WIDTH), mat_grad.reshape(2, 2, 2, mat_rows, WIDTH),
        norm_grad.reshape(NORM_ROWS, 1, WIDTH))))


BLOCK = 16
COLS = 384
STORE_SLOTS = 4


def adamw_block(grad, param, mom, var, decay_rate):
    new_mom = BETA_ONE * mom + (1.0 - BETA_ONE) * grad
    new_var = BETA_TWO * var + (1.0 - BETA_TWO) * grad * grad
    root = math.sqrt(1.0 - BETA_TWO ** ADAM_STEP)
    step_dir = new_mom / (jnp.sqrt(new_var) + ADAM_EPS * root)
    rate = LEARN_RATE * root / (1.0 - BETA_ONE ** ADAM_STEP)
    return param - (rate * step_dir + (LEARN_RATE * decay_rate) * param), new_mom, new_var


def adamw_kernel(scale, eg, ep, em, ev, mg, mp, mm, mv, ng, np_, nm, nv,
                 ep_out, em_out, ev_out, eb_out, mp_out, mm_out, mv_out, mb_out, np_out, nm_out, nv_out, nb_out,
                 p_buf, m_buf, v_buf, b_buf, n_bufs, nb_buf, sems, n_sems):
    clip = scale[0:1, 0:1]

    def copies(outs, slot, row):
        return [pltpu.make_async_copy(buf.at[slot], out.at[pl.ds(row, BLOCK), :], sems.at[k, slot])
                for k, (buf, out) in enumerate(zip((p_buf, m_buf, v_buf, b_buf), outs))]

    emb_outs = (ep_out, em_out, ev_out, eb_out)
    mat_outs = (mp_out, mm_out, mv_out, mb_out)
    emb_blocks = eg.shape[0] // BLOCK
    mat_blocks = mg.shape[0] // BLOCK

    def run(first, count, ins, outs):
        def body(i, carry):
            j = first + i
            slot = lax.rem(j, STORE_SLOTS)

            @pl.when(j >= STORE_SLOTS)
            def _():
                for copy in copies(emb_outs, slot, 0):
                    copy.wait()

            row = pl.multiple_of(i * BLOCK, BLOCK)
            for col in range(0, WIDTH, COLS):
                cols = pl.ds(col, COLS)
                g, p, m, v = (ref[pl.ds(row, BLOCK), cols] for ref in ins)
                new_p, new_m, new_v = adamw_block(g * clip, p, m, v, WEIGHT_DECAY)
                p_buf[slot, :, cols] = new_p
                m_buf[slot, :, cols] = new_m
                v_buf[slot, :, cols] = new_v
                b_buf[slot, :, cols] = new_p.astype(jnp.bfloat16)
            for copy in copies(outs, slot, row):
                copy.start()
            return carry

        lax.fori_loop(0, count, body, 0)

    run(0, emb_blocks, (eg, ep, em, ev), emb_outs)
    run(emb_blocks, mat_blocks, (mg, mp, mm, mv), mat_outs)
    new_p, new_m, new_v = adamw_block(ng[:NORM_ROWS, :NORM_COLS] * clip, np_[...], nm[...], nv[...], 0.0)
    for k, value in enumerate((new_p, new_m, new_v)):
        n_bufs[k] = value
    nb_buf[...] = new_p.astype(jnp.bfloat16)
    norm_copies = [pltpu.make_async_copy(n_bufs.at[k], out, n_sems.at[k]) for k, out in enumerate((np_out, nm_out, nv_out))]
    norm_copies.append(pltpu.make_async_copy(nb_buf, nb_out, n_sems.at[3]))
    for copy in norm_copies:
        copy.start()
    for slot in range(STORE_SLOTS):
        for copy in copies(emb_outs, slot, 0):
            copy.wait()
    for copy in norm_copies:
        copy.wait()


def adamw(scale, emb, mat, norm):
    shapes = []
    for ref in (emb[1], mat[1], norm[1]):
        shapes += [jax.ShapeDtypeStruct(ref.shape, F32)] * 3 + [jax.ShapeDtypeStruct(ref.shape, jnp.bfloat16)]
    buf = (STORE_SLOTS, BLOCK, WIDTH)
    vmem = pl.BlockSpec(memory_space=pltpu.VMEM)
    hbm = pl.BlockSpec(memory_space=pl.ANY)
    elements = emb[1].size + mat[1].size
    return pl.pallas_call(
        adamw_kernel,
        out_shape=tuple(shapes),
        in_specs=[vmem] * 13,
        out_specs=(hbm,) * 12,
        scratch_shapes=[
            pltpu.VMEM(buf, F32), pltpu.VMEM(buf, F32), pltpu.VMEM(buf, F32), pltpu.VMEM(buf, jnp.bfloat16),
            pltpu.VMEM((3, NORM_ROWS, NORM_COLS), F32), pltpu.VMEM((NORM_ROWS, NORM_COLS), jnp.bfloat16),
            pltpu.SemaphoreType.DMA((4, STORE_SLOTS)), pltpu.SemaphoreType.DMA((4,)),
        ],
        compiler_params=pltpu.CompilerParams(vmem_limit_bytes=8 * 1024 * 1024),
        cost_estimate=pl.CostEstimate(flops=20 * elements, bytes_accessed=30 * elements, transcendentals=2 * elements),
        name="adamw",
    )(scale, *emb, *mat, *norm)


def solution(mesh):
    def local_step(emb_grad, mat_grad, norm_grad, emb_param, emb_mom, emb_var, mat_param, mat_mom, mat_var, norm_param, norm_mom, norm_var):
        emb_mean, mat_mean, norm_mean, scale = reduce_grads(emb_grad[0, 0], mat_grad[0, 0], norm_grad[0, 0])
        return adamw(scale, (emb_mean, emb_param, emb_mom, emb_var), (mat_mean, mat_param, mat_mom, mat_var),
                     (norm_mean, norm_param, norm_mom, norm_var))

    grad_spec = P("dp", "fsdp", None, None)
    row_spec = P("fsdp", None)
    col_spec = P(None, "fsdp")
    in_list = (grad_spec, grad_spec, grad_spec, row_spec, row_spec, row_spec, row_spec, row_spec, row_spec, col_spec, col_spec, col_spec)
    out_list = (row_spec, row_spec, row_spec, row_spec, row_spec, row_spec, row_spec, row_spec, col_spec, col_spec, col_spec, col_spec)
    return jax.shard_map(local_step, mesh=mesh, in_specs=in_list, out_specs=out_list, check_vma=False)
```

```python
import functools
import math

import jax
import jax.numpy as jnp
from jax import lax
from jax.experimental import pallas as pl
from jax.experimental.pallas import tpu as pltpu
from jax.sharding import PartitionSpec as P

LEARN_RATE = 0.003
BETA_ONE = 0.9
BETA_TWO = 0.95
ADAM_EPS = 1e-8
WEIGHT_DECAY = 0.1
CLIP_NORM = 1.0
ADAM_STEP = 10

MESH = pl.DeviceIdType.MESH
F32 = jnp.float32

WIDTH = 5376
NORM_ROWS = 9
NORM_COLS = 672
NORM_PAD = (16, 768)
ROWS = 8
A_COLS = 2048
B_COLS = 2048
HALF = 640
B_AT = A_COLS
C_AT = A_COLS + B_COLS
LAG_ZERO = 1
LAG = 3
P_SLOTS = 10
R_SLOTS = 6
SEND_SLOTS = 8
RING = 20


def reduce_kernel(counts, emb, mat, norm, emb_out, mat_out, norm_out, scale_out,
                  part, recv_zero, xa, yb, zc, mid, wc, tc, grad, square,
                  norm_in, norm_part, norm_a, norm_b, norm_c, norm_d, sum_send, sum_recv,
                  load_sem, zero_send, zero_recv, credit,
                  one_send, one_recv, two_send, two_recv, three_send, three_recv, four_send, four_recv, out_sem,
                  norm_load, norm_send, norm_recv, sum_ssem, sum_rsem):
    emb_count, mat_count = counts
    total = emb_count + mat_count
    z = lax.axis_index("dp")
    f = lax.axis_index("fsdp")
    c = lax.rem(f, 2)
    x = lax.rem(lax.div(f, 2), 2)
    y = lax.div(f, 4)
    core = (z, f + 1 - 2 * c)
    xn = (z, f + 2 - 4 * x)
    yn = (z, f + 4 - 8 * y)
    zn = (1 - z, f)
    peers = [(z, lax.rem(f + k, 8)) for k in range(1, 8)]

    def remote(src, dst, ssem, rsem, dev):
        return pltpu.make_async_remote_copy(src_ref=src, dst_ref=dst, send_sem=ssem, recv_sem=rsem,
                                            device_id=dev, device_id_type=MESH)

    def half_at(base, which):
        return pl.ds(pl.multiple_of(base + which * HALF, 128), HALF)

    c_keep, c_give = half_at(C_AT, z), half_at(C_AT, 1 - z)
    a_cols, b_cols, ab_cols = pl.ds(0, A_COLS), pl.ds(B_AT, B_COLS), pl.ds(0, C_AT)

    barrier = pltpu.get_barrier_semaphore()
    for dev in (core, xn, yn, zn):
        pl.semaphore_signal(barrier, inc=1, device_id=dev, device_id_type=MESH)
    norm_copy = pltpu.make_async_copy(norm, norm_in, norm_load)
    norm_copy.start()

    def on_rows(j, body):
        @pl.when(j < emb_count)
        def _():
            body(emb, emb_out, pl.multiple_of(j * ROWS, ROWS))

        @pl.when(j >= emb_count)
        def _():
            body(mat, mat_out, pl.multiple_of((j - emb_count) * ROWS, ROWS))

    def load_copy(ref, row, j):
        s = lax.rem(j, P_SLOTS)
        return pltpu.make_async_copy(ref.at[:, :, c, pl.ds(row, ROWS), :], part.at[s], load_sem.at[s])

    def zero_copy(ref, row, j):
        s = lax.rem(j, R_SLOTS)
        return remote(ref.at[:, :, 1 - c, pl.ds(row, ROWS), :], recv_zero.at[s], zero_send.at[s], zero_recv.at[s], core)

    def ones(j):
        s, r = lax.rem(j, P_SLOTS), lax.rem(j, RING)
        return (remote(part.at[s, :, :, :, c_give], zc.at[r], one_send.at[2, s], one_recv.at[2, r], zn),
                remote(part.at[s, :, 1 - x, :, a_cols], xa.at[r], one_send.at[0, s], one_recv.at[0, r], xn),
                remote(part.at[s, 1 - y, :, :, b_cols], yb.at[r], one_send.at[1, s], one_recv.at[1, r], yn))

    def two_c_even(j):
        s, r = lax.rem(j, SEND_SLOTS), lax.rem(j, RING)
        return remote(zc.at[r, :, 1 - x], wc.at[r], two_send.at[2, s], two_recv.at[2, r], xn)

    def two_c_odd(j):
        s, r = lax.rem(j, SEND_SLOTS), lax.rem(j, RING)
        return remote(zc.at[r, 1 - y], wc.at[r], two_send.at[2, s], two_recv.at[2, r], yn)

    def twos(j):
        s, r = lax.rem(j, SEND_SLOTS), lax.rem(j, RING)
        return (remote(xa.at[r, 1 - y], mid.at[r, :, a_cols], two_send.at[0, s], two_recv.at[0, r], yn),
                remote(yb.at[r, 1 - x], mid.at[r, :, b_cols], two_send.at[1, s], two_recv.at[1, r], xn))

    def three_c(j):
        s, r, odd = lax.rem(j, SEND_SLOTS), lax.rem(j, RING), lax.rem(j, 2)
        here = y + odd * (x - y)
        step = (4 - 8 * y) + odd * ((2 - 4 * x) - (4 - 8 * y))
        return remote(wc.at[r, 1 - here], tc.at[r], three_send.at[1, s], three_recv.at[1, r], (z, f + step))

    def three_ab(j):
        s, r = lax.rem(j, SEND_SLOTS), lax.rem(j, RING)
        return remote(mid.at[r], grad.at[r, :, ab_cols], three_send.at[0, s], three_recv.at[0, r], zn)

    def four(j, c_at):
        s, r = lax.rem(j, SEND_SLOTS), lax.rem(j, RING)
        return remote(grad.at[r, :, c_at], grad.at[r, :, c_at], four_send.at[s], four_recv.at[r], zn)

    def out_copy(ref, row, j):
        return pltpu.make_async_copy(grad.at[lax.rem(j, RING)], ref.at[pl.ds(row, ROWS), :],
                                     out_sem.at[lax.rem(j, SEND_SLOTS)])

    norm_zero = remote(norm_part.at[:, :, 1 - c], norm_a, norm_send.at[0], norm_recv.at[0], core)
    norm_one = remote(norm_a.at[:, 1 - x], norm_b, norm_send.at[1], norm_recv.at[1], xn)
    norm_two = remote(norm_b.at[1 - y], norm_c, norm_send.at[2], norm_recv.at[2], yn)
    norm_three = remote(norm_c, norm_d, norm_send.at[3], norm_recv.at[3], zn)

    def when_in(j, body):
        pl.when(jnp.logical_and(j >= 0, j < total))(functools.partial(body, j))

    def start(copies):
        for copy in copies:
            copy.start()

    def wait_send(copies):
        for copy in copies:
            copy.wait_send()

    def stage_issue(j):
        @pl.when(j >= P_SLOTS)
        def _():
            wait_send(ones(j - P_SLOTS))

        @pl.when(j >= R_SLOTS)
        def _():
            zero_copy(emb, 0, j - R_SLOTS).wait_send()
            pl.semaphore_wait(credit, 1)

        def body(ref, _, row):
            zero_copy(ref, row, j).start()
            load_copy(ref, row, j).start()

        on_rows(j, body)

    def stage_one(j):
        load_copy(emb, 0, j).wait()
        zero_copy(emb, 0, j).wait_recv()
        part[lax.rem(j, P_SLOTS)] += recv_zero[lax.rem(j, R_SLOTS)]

        @pl.when(j + R_SLOTS < total)
        def _():
            pl.semaphore_signal(credit, inc=1, device_id=core, device_id_type=MESH)

        start(ones(j)[:1])

    def stage_one_more(j):
        start(ones(j)[1:])

    def stage_two(j):
        s, r = lax.rem(j, P_SLOTS), lax.rem(j, RING)
        even = lax.rem(j, 2) == 0
        for copy in ones(j):
            copy.wait_recv()
        zc[r] += part[s, :, :, :, c_keep]
        xa[r] += part[s, :, x, :, a_cols]
        yb[r] += part[s, y, :, :, b_cols]

        @pl.when(j >= SEND_SLOTS)
        def _():
            wait_send(twos(j - SEND_SLOTS) + (two_c_even(j - SEND_SLOTS),))

        pl.when(even)(lambda: two_c_even(j).start())
        pl.when(jnp.logical_not(even))(lambda: two_c_odd(j).start())
        start(twos(j))

    def stage_three(j):
        r = lax.rem(j, RING)
        even = lax.rem(j, 2) == 0
        for copy in twos(j) + (two_c_even(j),):
            copy.wait_recv()

        @pl.when(even)
        def _():
            wc[r] += zc[r, :, x]

        @pl.when(jnp.logical_not(even))
        def _():
            wc[r] += zc[r, y]

        mid[r, :, a_cols] += xa[r, y]
        mid[r, :, b_cols] += yb[r, x]

        @pl.when(j >= SEND_SLOTS)
        def _():
            wait_send((three_ab(j - SEND_SLOTS), three_c(j - SEND_SLOTS)))

        start((three_c(j), three_ab(j)))

    def stage_four(j):
        r, odd = lax.rem(j, RING), lax.rem(j, 2)
        here = y + odd * (x - y)
        three_c(j).wait_recv()

        @pl.when(j >= SEND_SLOTS)
        def _():
            four(j - SEND_SLOTS, c_keep).wait_send()

        grad[r, :, c_keep] = (tc[r] + wc[r, here]) * (1.0 / 16.0)
        four(j, c_keep).start()

    def stage_five(j):
        r = lax.rem(j, RING)
        three_ab(j).wait_recv()
        both = (grad[r, :, ab_cols] + mid[r]) * (1.0 / 16.0)
        grad[r, :, ab_cols] = both
        square[:, ab_cols] += both * both
        four(j, c_give).wait_recv()
        rest = grad[r, :, C_AT:]
        square[:, C_AT:] += rest * rest

        @pl.when(j >= SEND_SLOTS)
        def _():
            out_copy(emb_out, 0, j - SEND_SLOTS).wait()

        def body(_, ref, row):
            out_copy(ref, row, j).start()

        on_rows(j, body)

    def trip(it, carry):
        when_in(it, stage_issue)
        when_in(it - LAG_ZERO, stage_one)
        when_in(it - LAG_ZERO - 4 * LAG, stage_five)
        when_in(it - LAG_ZERO - 3 * LAG, stage_four)
        when_in(it - LAG_ZERO - 2 * LAG, stage_three)
        when_in(it - LAG_ZERO - LAG, stage_two)
        when_in(it - LAG_ZERO, stage_one_more)

        @pl.when(it == 5)
        def _():
            norm_copy.wait()
            for k in range(8):
                for row in range(NORM_ROWS):
                    norm_part[k // 4, (k // 2) % 2, k % 2, row:row + 1, :NORM_COLS] = norm_in[row, :, k * NORM_COLS:(k + 1) * NORM_COLS]
            norm_zero.start()

        @pl.when(it == 8)
        def _():
            norm_zero.wait_recv()
            norm_a[...] += norm_part[:, :, c]
            norm_one.start()

        @pl.when(it == 12)
        def _():
            norm_one.wait_recv()
            norm_b[...] += norm_a[:, x]
            norm_two.start()

        @pl.when(it == 16)
        def _():
            norm_two.wait_recv()
            norm_c[...] += norm_b[y]
            norm_three.start()

        @pl.when(it == 20)
        def _():
            norm_three.wait_recv()
            norm_d[...] = (norm_d[...] + norm_c[...]) * (1.0 / 16.0)
            norm_out[...] = norm_d[...]
            norm_sq = norm_d[...] * norm_d[...]
            square[:, :NORM_PAD[1]] += norm_sq[:ROWS] + norm_sq[ROWS:]

        return carry

    norm_part[...] = jnp.zeros_like(norm_part)
    square[...] = jnp.zeros_like(square)
    pl.semaphore_wait(barrier, 4)
    lax.fori_loop(0, total + LAG_ZERO + 4 * LAG, trip, 0)

    value = jnp.full((8, 128), jnp.sum(square[...]), F32)
    sum_send[...] = value
    sum_recv[f] = value
    sums = [remote(sum_send, sum_recv.at[f], sum_ssem.at[k], sum_rsem.at[f], dev) for k, dev in enumerate(peers)]
    start(sums)
    wait_send((norm_zero, norm_one, norm_two, norm_three))

    def drain(slots, copies):
        def body(j, carry):
            wait_send(copies(j))
            return carry
        lax.fori_loop(total - slots, total, body, 0)

    drain(P_SLOTS, ones)
    drain(R_SLOTS, lambda j: (zero_copy(emb, 0, j),))
    drain(SEND_SLOTS, lambda j: twos(j) + (two_c_even(j), three_ab(j), three_c(j), four(j, c_keep)))

    def last(j, carry):
        out_copy(emb_out, 0, j).wait()
        return carry

    lax.fori_loop(total - SEND_SLOTS, total, last, 0)

    for k in range(1, 8):
        s = lax.rem(f + k, 8)
        remote(sum_send, sum_recv.at[s], sum_ssem.at[0], sum_rsem.at[s], core).wait_recv()
    whole = sum_recv[0]
    for k in range(1, 8):
        whole = whole + sum_recv[k]
    scale_out[...] = jnp.minimum(1.0, CLIP_NORM / jnp.sqrt(whole))
    wait_send(sums)


def reduce_grads(emb_grad, mat_grad, norm_grad):
    emb_rows = emb_grad.shape[0] // 8
    mat_rows = mat_grad.shape[0] // 8
    counts = (emb_rows // ROWS, mat_rows // ROWS)
    dma = pltpu.SemaphoreType.DMA
    scratch = [
        pltpu.VMEM((P_SLOTS, 2, 2, ROWS, WIDTH), F32),
        pltpu.VMEM((R_SLOTS, 2, 2, ROWS, WIDTH), F32),
        pltpu.VMEM((RING, 2, ROWS, A_COLS), F32),
        pltpu.VMEM((RING, 2, ROWS, B_COLS), F32),
        pltpu.VMEM((RING, 2, 2, ROWS, HALF), F32),
        pltpu.VMEM((RING, ROWS, C_AT), F32),
        pltpu.VMEM((RING, 2, ROWS, HALF), F32),
        pltpu.VMEM((RING, ROWS, HALF), F32),
        pltpu.VMEM((RING, ROWS, WIDTH), F32),
        pltpu.VMEM((ROWS, WIDTH), F32),
        pltpu.VMEM((NORM_ROWS, 1, WIDTH), F32),
        pltpu.VMEM((2, 2, 2) + NORM_PAD, F32),
        pltpu.VMEM((2, 2) + NORM_PAD, F32),
        pltpu.VMEM((2,) + NORM_PAD, F32),
        pltpu.VMEM(NORM_PAD, F32),
        pltpu.VMEM(NORM_PAD, F32),
        pltpu.VMEM((8, 128), F32),
        pltpu.VMEM((8, 8, 128), F32),
        dma((P_SLOTS,)), dma((R_SLOTS,)), dma((R_SLOTS,)), pltpu.SemaphoreType.REGULAR,
        dma((3, P_SLOTS)), dma((3, RING)), dma((3, SEND_SLOTS)), dma((3, RING)),
        dma((2, SEND_SLOTS)), dma((2, RING)), dma((SEND_SLOTS,)), dma((RING,)), dma((SEND_SLOTS,)),
        dma, dma((4,)), dma((4,)), dma((7,)), dma((8,)),
    ]
    hbm = pl.BlockSpec(memory_space=pl.ANY)
    vmem = pl.BlockSpec(memory_space=pltpu.VMEM)
    return pl.pallas_call(
        functools.partial(reduce_kernel, counts),
        out_shape=(
            jax.ShapeDtypeStruct((emb_rows, WIDTH), F32),
            jax.ShapeDtypeStruct((mat_rows, WIDTH), F32),
            jax.ShapeDtypeStruct(NORM_PAD, F32),
            jax.ShapeDtypeStruct((8, 128), F32),
        ),
        in_specs=[pl.BlockSpec(memory_space=pltpu.HBM)] * 3,
        out_specs=(hbm, hbm, vmem, vmem),
        scratch_shapes=scratch,
        compiler_params=pltpu.CompilerParams(
            collective_id=0, has_side_effects=True, vmem_limit_bytes=28 * 1024 * 1024
        ),
        name="reduce_grads",
    )(*(pltpu.with_memory_space_constraint(grad, pltpu.HBM) for grad in (
        emb_grad.reshape(2, 2, 2, emb_rows, WIDTH), mat_grad.reshape(2, 2, 2, mat_rows, WIDTH),
        norm_grad.reshape(NORM_ROWS, 1, WIDTH))))


BLOCK = 16
COLS = 384
STORE_SLOTS = 4


def adamw_block(grad, param, mom, var, decay_rate):
    new_mom = BETA_ONE * mom + (1.0 - BETA_ONE) * grad
    new_var = BETA_TWO * var + (1.0 - BETA_TWO) * grad * grad
    root = math.sqrt(1.0 - BETA_TWO ** ADAM_STEP)
    step_dir = new_mom / (jnp.sqrt(new_var) + ADAM_EPS * root)
    rate = LEARN_RATE * root / (1.0 - BETA_ONE ** ADAM_STEP)
    return param - (rate * step_dir + (LEARN_RATE * decay_rate) * param), new_mom, new_var


def adamw_kernel(scale, eg, ep, em, ev, mg, mp, mm, mv, ng, np_, nm, nv,
                 ep_out, em_out, ev_out, eb_out, mp_out, mm_out, mv_out, mb_out, np_out, nm_out, nv_out, nb_out,
                 p_buf, m_buf, v_buf, b_buf, n_bufs, nb_buf, sems, n_sems):
    clip = scale[0:1, 0:1]

    def copies(outs, slot, row):
        return [pltpu.make_async_copy(buf.at[slot], out.at[pl.ds(row, BLOCK), :], sems.at[k, slot])
                for k, (buf, out) in enumerate(zip((p_buf, m_buf, v_buf, b_buf), outs))]

    emb_outs = (ep_out, em_out, ev_out, eb_out)
    mat_outs = (mp_out, mm_out, mv_out, mb_out)
    emb_blocks = eg.shape[0] // BLOCK
    mat_blocks = mg.shape[0] // BLOCK

    def run(first, count, ins, outs):
        def body(i, carry):
            j = first + i
            slot = lax.rem(j, STORE_SLOTS)

            @pl.when(j >= STORE_SLOTS)
            def _():
                for copy in copies(emb_outs, slot, 0):
                    copy.wait()

            row = pl.multiple_of(i * BLOCK, BLOCK)
            for col in range(0, WIDTH, COLS):
                cols = pl.ds(col, COLS)
                g, p, m, v = (ref[pl.ds(row, BLOCK), cols] for ref in ins)
                new_p, new_m, new_v = adamw_block(g * clip, p, m, v, WEIGHT_DECAY)
                p_buf[slot, :, cols] = new_p
                m_buf[slot, :, cols] = new_m
                v_buf[slot, :, cols] = new_v
                b_buf[slot, :, cols] = new_p.astype(jnp.bfloat16)
            for copy in copies(outs, slot, row):
                copy.start()
            return carry

        lax.fori_loop(0, count, body, 0)

    run(0, emb_blocks, (eg, ep, em, ev), emb_outs)
    run(emb_blocks, mat_blocks, (mg, mp, mm, mv), mat_outs)
    new_p, new_m, new_v = adamw_block(ng[:NORM_ROWS, :NORM_COLS] * clip, np_[...], nm[...], nv[...], 0.0)
    for k, value in enumerate((new_p, new_m, new_v)):
        n_bufs[k] = value
    nb_buf[...] = new_p.astype(jnp.bfloat16)
    norm_copies = [pltpu.make_async_copy(n_bufs.at[k], out, n_sems.at[k]) for k, out in enumerate((np_out, nm_out, nv_out))]
    norm_copies.append(pltpu.make_async_copy(nb_buf, nb_out, n_sems.at[3]))
    for copy in norm_copies:
        copy.start()
    for slot in range(STORE_SLOTS):
        for copy in copies(emb_outs, slot, 0):
            copy.wait()
    for copy in norm_copies:
        copy.wait()


def adamw(scale, emb, mat, norm):
    shapes = []
    for ref in (emb[1], mat[1], norm[1]):
        shapes += [jax.ShapeDtypeStruct(ref.shape, F32)] * 3 + [jax.ShapeDtypeStruct(ref.shape, jnp.bfloat16)]
    buf = (STORE_SLOTS, BLOCK, WIDTH)
    vmem = pl.BlockSpec(memory_space=pltpu.VMEM)
    hbm = pl.BlockSpec(memory_space=pl.ANY)
    elements = emb[1].size + mat[1].size
    return pl.pallas_call(
        adamw_kernel,
        out_shape=tuple(shapes),
        in_specs=[vmem] * 13,
        out_specs=(hbm,) * 12,
        scratch_shapes=[
            pltpu.VMEM(buf, F32), pltpu.VMEM(buf, F32), pltpu.VMEM(buf, F32), pltpu.VMEM(buf, jnp.bfloat16),
            pltpu.VMEM((3, NORM_ROWS, NORM_COLS), F32), pltpu.VMEM((NORM_ROWS, NORM_COLS), jnp.bfloat16),
            pltpu.SemaphoreType.DMA((4, STORE_SLOTS)), pltpu.SemaphoreType.DMA((4,)),
        ],
        compiler_params=pltpu.CompilerParams(vmem_limit_bytes=8 * 1024 * 1024),
        cost_estimate=pl.CostEstimate(flops=20 * elements, bytes_accessed=30 * elements, transcendentals=2 * elements),
        name="adamw",
    )(scale, *emb, *mat, *norm)


def solution(mesh):
    def local_step(emb_grad, mat_grad, norm_grad, emb_param, emb_mom, emb_var, mat_param, mat_mom, mat_var, norm_param, norm_mom, norm_var):
        emb_mean, mat_mean, norm_mean, scale = reduce_grads(emb_grad[0, 0], mat_grad[0, 0], norm_grad[0, 0])
        return adamw(scale, (emb_mean, emb_param, emb_mom, emb_var), (mat_mean, mat_param, mat_mom, mat_var),
                     (norm_mean, norm_param, norm_mom, norm_var))

    grad_spec = P("dp", "fsdp", None, None)
    row_spec = P("fsdp", None)
    col_spec = P(None, "fsdp")
    in_list = (grad_spec, grad_spec, grad_spec, row_spec, row_spec, row_spec, row_spec, row_spec, row_spec, col_spec, col_spec, col_spec)
    out_list = (row_spec, row_spec, row_spec, row_spec, row_spec, row_spec, row_spec, row_spec, col_spec, col_spec, col_spec, col_spec)
    return jax.shard_map(local_step, mesh=mesh, in_specs=in_list, out_specs=out_list, check_vma=False)
```

```python
import functools
import math

import jax
import jax.numpy as jnp
from jax import lax
from jax.experimental import pallas as pl
from jax.experimental.pallas import tpu as pltpu
from jax.sharding import PartitionSpec as P

LEARN_RATE = 0.003
BETA_ONE = 0.9
BETA_TWO = 0.95
ADAM_EPS = 1e-8
WEIGHT_DECAY = 0.1
CLIP_NORM = 1.0
ADAM_STEP = 10

MESH = pl.DeviceIdType.MESH
F32 = jnp.float32

WIDTH = 5376
NORM_ROWS = 9
NORM_COLS = 672
NORM_PAD = (16, 768)
ROWS = 8
PLANS = ((1920, 768), (2176, 512))
INNER = (20, 44)
SIDE_MAX = max(side for side, _ in PLANS)
HALF_MAX = max(half for _, half in PLANS)
LAG_ZERO = 1
LAG = 2
P_SLOTS = 10
R_SLOTS = 6
SEND_SLOTS = 8
RING = 16


def reduce_kernel(counts, emb, mat, norm, emb_out, mat_out, norm_out, scale_out,
                  part, recv_zero, xa, yb, zc, mid, wc, tc, grad, square,
                  norm_in, norm_part, norm_a, norm_b, norm_c, norm_d, sum_send, sum_recv,
                  load_sem, zero_send, zero_recv, credit,
                  one_send, one_recv, two_send, two_recv, three_send, three_recv, four_send, four_recv, out_sem,
                  norm_load, norm_send, norm_recv, sum_ssem, sum_rsem):
    emb_count, mat_count = counts
    total = emb_count + mat_count
    z = lax.axis_index("dp")
    f = lax.axis_index("fsdp")
    c = lax.rem(f, 2)
    x = lax.rem(lax.div(f, 2), 2)
    y = lax.div(f, 4)
    core = (z, f + 1 - 2 * c)
    xn = (z, f + 2 - 4 * x)
    yn = (z, f + 4 - 8 * y)
    zn = (1 - z, f)
    peers = [(z, lax.rem(f + k, 8)) for k in range(1, 8)]

    def remote(src, dst, ssem, rsem, dev):
        return pltpu.make_async_remote_copy(src_ref=src, dst_ref=dst, send_sem=ssem, recv_sem=rsem,
                                            device_id=dev, device_id_type=MESH)

    def on_plan(j, body):
        inner = jnp.logical_and(j >= INNER[0], j < INNER[1])
        pl.when(jnp.logical_not(inner))(lambda: body(j, *PLANS[0]))
        pl.when(inner)(lambda: body(j, *PLANS[1]))

    def half_at(side, half, which):
        return pl.ds(pl.multiple_of(2 * side + which * half, 128), half)

    barrier = pltpu.get_barrier_semaphore()
    for dev in (core, xn, yn, zn):
        pl.semaphore_signal(barrier, inc=1, device_id=dev, device_id_type=MESH)
    norm_copy = pltpu.make_async_copy(norm, norm_in, norm_load)
    norm_copy.start()

    def on_rows(j, body):
        @pl.when(j < emb_count)
        def _():
            body(emb, emb_out, pl.multiple_of(j * ROWS, ROWS))

        @pl.when(j >= emb_count)
        def _():
            body(mat, mat_out, pl.multiple_of((j - emb_count) * ROWS, ROWS))

    def load_copy(ref, row, j):
        s = lax.rem(j, P_SLOTS)
        return pltpu.make_async_copy(ref.at[:, :, c, pl.ds(row, ROWS), :], part.at[s], load_sem.at[s])

    def zero_copy(ref, row, j):
        s = lax.rem(j, R_SLOTS)
        return remote(ref.at[:, :, 1 - c, pl.ds(row, ROWS), :], recv_zero.at[s], zero_send.at[s], zero_recv.at[s], core)

    def ones(j, side, half):
        s, r = lax.rem(j, P_SLOTS), lax.rem(j, RING)
        return (remote(part.at[s, :, :, :, half_at(side, half, 1 - z)], zc.at[r, :, :, :, :half], one_send.at[2, s], one_recv.at[2, r], zn),
                remote(part.at[s, :, 1 - x, :, :side], xa.at[r, :, :, :side], one_send.at[0, s], one_recv.at[0, r], xn),
                remote(part.at[s, 1 - y, :, :, side:2 * side], yb.at[r, :, :, :side], one_send.at[1, s], one_recv.at[1, r], yn))

    def two_c_even(j, side, half):
        s, r = lax.rem(j, SEND_SLOTS), lax.rem(j, RING)
        return remote(zc.at[r, :, 1 - x, :, :half], wc.at[r, :, :, :half], two_send.at[2, s], two_recv.at[2, r], xn)

    def two_c_odd(j, side, half):
        s, r = lax.rem(j, SEND_SLOTS), lax.rem(j, RING)
        return remote(zc.at[r, 1 - y, :, :, :half], wc.at[r, :, :, :half], two_send.at[2, s], two_recv.at[2, r], yn)

    def twos(j, side, half):
        s, r = lax.rem(j, SEND_SLOTS), lax.rem(j, RING)
        return (remote(xa.at[r, 1 - y, :, :side], mid.at[r, :, :side], two_send.at[0, s], two_recv.at[0, r], yn),
                remote(yb.at[r, 1 - x, :, :side], mid.at[r, :, side:2 * side], two_send.at[1, s], two_recv.at[1, r], xn))

    def three_c(j, side, half):
        s, r, odd = lax.rem(j, SEND_SLOTS), lax.rem(j, RING), lax.rem(j, 2)
        here = y + odd * (x - y)
        step = (4 - 8 * y) + odd * ((2 - 4 * x) - (4 - 8 * y))
        return remote(wc.at[r, 1 - here, :, :half], tc.at[r, :, :half], three_send.at[1, s], three_recv.at[1, r], (z, f + step))

    def three_ab(j, side, half):
        s, r = lax.rem(j, SEND_SLOTS), lax.rem(j, RING)
        return remote(mid.at[r, :, :2 * side], grad.at[r, :, :2 * side], three_send.at[0, s], three_recv.at[0, r], zn)

    def four(j, side, half, which):
        s, r = lax.rem(j, SEND_SLOTS), lax.rem(j, RING)
        cols = half_at(side, half, which)
        return remote(grad.at[r, :, cols], grad.at[r, :, cols], four_send.at[s], four_recv.at[r], zn)

    def out_copy(ref, row, j):
        return pltpu.make_async_copy(grad.at[lax.rem(j, RING)], ref.at[pl.ds(row, ROWS), :],
                                     out_sem.at[lax.rem(j, SEND_SLOTS)])

    norm_zero = remote(norm_part.at[:, :, 1 - c], norm_a, norm_send.at[0], norm_recv.at[0], core)
    norm_one = remote(norm_a.at[:, 1 - x], norm_b, norm_send.at[1], norm_recv.at[1], xn)
    norm_two = remote(norm_b.at[1 - y], norm_c, norm_send.at[2], norm_recv.at[2], yn)
    norm_three = remote(norm_c, norm_d, norm_send.at[3], norm_recv.at[3], zn)

    def when_in(j, body):
        pl.when(jnp.logical_and(j >= 0, j < total))(functools.partial(body, j))

    def after(j, slots, copies):
        @pl.when(j >= slots)
        def _():
            on_plan(j - slots, lambda *args: wait_send(copies(*args)))

    def start(copies):
        for copy in copies:
            copy.start()

    def wait_send(copies):
        for copy in copies:
            copy.wait_send()

    def stage_issue(j):
        after(j, P_SLOTS, ones)

        @pl.when(j >= R_SLOTS)
        def _():
            zero_copy(emb, 0, j - R_SLOTS).wait_send()
            pl.semaphore_wait(credit, 1)

        def body(ref, _, row):
            zero_copy(ref, row, j).start()
            load_copy(ref, row, j).start()

        on_rows(j, body)

    def stage_one(j):
        load_copy(emb, 0, j).wait()
        zero_copy(emb, 0, j).wait_recv()
        part[lax.rem(j, P_SLOTS)] += recv_zero[lax.rem(j, R_SLOTS)]

        @pl.when(j + R_SLOTS < total)
        def _():
            pl.semaphore_signal(credit, inc=1, device_id=core, device_id_type=MESH)

        on_plan(j, lambda *args: start(ones(*args)[:1]))

    def stage_one_more(j):
        on_plan(j, lambda *args: start(ones(*args)[1:]))

    def stage_two(j):
        after(j, SEND_SLOTS, lambda *args: twos(*args) + (two_c_even(*args),))

        def body(j, side, half):
            s, r = lax.rem(j, P_SLOTS), lax.rem(j, RING)
            even = lax.rem(j, 2) == 0
            for copy in ones(j, side, half):
                copy.wait_recv()
            zc[r, :, :, :, :half] += part[s, :, :, :, half_at(side, half, z)]
            xa[r, :, :, :side] += part[s, :, x, :, :side]
            yb[r, :, :, :side] += part[s, y, :, :, side:2 * side]
            pl.when(even)(lambda: two_c_even(j, side, half).start())
            pl.when(jnp.logical_not(even))(lambda: two_c_odd(j, side, half).start())
            start(twos(j, side, half))

        on_plan(j, body)

    def stage_three(j):
        after(j, SEND_SLOTS, lambda *args: (three_ab(*args), three_c(*args)))

        def body(j, side, half):
            r = lax.rem(j, RING)
            even = lax.rem(j, 2) == 0
            for copy in twos(j, side, half) + (two_c_even(j, side, half),):
                copy.wait_recv()

            @pl.when(even)
            def _():
                wc[r, :, :, :half] += zc[r, :, x, :, :half]

            @pl.when(jnp.logical_not(even))
            def _():
                wc[r, :, :, :half] += zc[r, y, :, :, :half]

            mid[r, :, :side] += xa[r, y, :, :side]
            mid[r, :, side:2 * side] += yb[r, x, :, :side]
            start((three_c(j, side, half), three_ab(j, side, half)))

        on_plan(j, body)

    def stage_four(j):
        after(j, SEND_SLOTS, lambda *args: (four(*args, z),))

        def body(j, side, half):
            r, odd = lax.rem(j, RING), lax.rem(j, 2)
            here = y + odd * (x - y)
            three_c(j, side, half).wait_recv()
            grad[r, :, half_at(side, half, z)] = (tc[r, :, :half] + wc[r, here, :, :half]) * (1.0 / 16.0)
            four(j, side, half, z).start()

        on_plan(j, body)

    def stage_five(j):
        def body(j, side, half):
            r = lax.rem(j, RING)
            three_ab(j, side, half).wait_recv()
            both = (grad[r, :, :2 * side] + mid[r, :, :2 * side]) * (1.0 / 16.0)
            grad[r, :, :2 * side] = both
            square[:, :2 * side] += both * both
            four(j, side, half, 1 - z).wait_recv()
            rest = grad[r, :, 2 * side:]
            square[:, 2 * side:] += rest * rest

        on_plan(j, body)

        @pl.when(j >= SEND_SLOTS)
        def _():
            out_copy(emb_out, 0, j - SEND_SLOTS).wait()

        def store(_, ref, row):
            out_copy(ref, row, j).start()

        on_rows(j, store)

    def trip(it, carry):
        when_in(it, stage_issue)
        when_in(it - LAG_ZERO, stage_one)
        when_in(it - LAG_ZERO - 4 * LAG, stage_five)
        when_in(it - LAG_ZERO - 3 * LAG, stage_four)
        when_in(it - LAG_ZERO - 2 * LAG, stage_three)
        when_in(it - LAG_ZERO - LAG, stage_two)
        when_in(it - LAG_ZERO, stage_one_more)

        @pl.when(it == 5)
        def _():
            norm_copy.wait()
            for k in range(8):
                for row in range(NORM_ROWS):
                    norm_part[k // 4, (k // 2) % 2, k % 2, row:row + 1, :NORM_COLS] = norm_in[row, :, k * NORM_COLS:(k + 1) * NORM_COLS]
            norm_zero.start()

        @pl.when(it == 8)
        def _():
            norm_zero.wait_recv()
            norm_a[...] += norm_part[:, :, c]
            norm_one.start()

        @pl.when(it == 12)
        def _():
            norm_one.wait_recv()
            norm_b[...] += norm_a[:, x]
            norm_two.start()

        @pl.when(it == 16)
        def _():
            norm_two.wait_recv()
            norm_c[...] += norm_b[y]
            norm_three.start()

        @pl.when(it == 20)
        def _():
            norm_three.wait_recv()
            norm_d[...] = (norm_d[...] + norm_c[...]) * (1.0 / 16.0)
            norm_out[...] = norm_d[...]
            norm_sq = norm_d[...] * norm_d[...]
            square[:, :NORM_PAD[1]] += norm_sq[:ROWS] + norm_sq[ROWS:]

        return carry

    norm_part[...] = jnp.zeros_like(norm_part)
    square[...] = jnp.zeros_like(square)
    pl.semaphore_wait(barrier, 4)
    lax.fori_loop(0, total + LAG_ZERO + 4 * LAG, trip, 0)

    value = jnp.full((8, 128), jnp.sum(square[...]), F32)
    sum_send[...] = value
    sum_recv[f] = value
    sums = [remote(sum_send, sum_recv.at[f], sum_ssem.at[k], sum_rsem.at[f], dev) for k, dev in enumerate(peers)]
    start(sums)
    wait_send((norm_zero, norm_one, norm_two, norm_three))

    def drain(slots, copies):
        def body(j, carry):
            on_plan(j, lambda *args: wait_send(copies(*args)))
            return carry
        lax.fori_loop(total - slots, total, body, 0)

    drain(P_SLOTS, ones)
    drain(R_SLOTS, lambda j, side, half: (zero_copy(emb, 0, j),))
    drain(SEND_SLOTS, lambda *args: twos(*args) + (two_c_even(*args), three_ab(*args), three_c(*args), four(*args, z)))

    def last(j, carry):
        out_copy(emb_out, 0, j).wait()
        return carry

    lax.fori_loop(total - SEND_SLOTS, total, last, 0)

    for k in range(1, 8):
        s = lax.rem(f + k, 8)
        remote(sum_send, sum_recv.at[s], sum_ssem.at[0], sum_rsem.at[s], core).wait_recv()
    whole = sum_recv[0]
    for k in range(1, 8):
        whole = whole + sum_recv[k]
    scale_out[...] = jnp.minimum(1.0, CLIP_NORM / jnp.sqrt(whole))
    wait_send(sums)


def reduce_grads(emb_grad, mat_grad, norm_grad):
    emb_rows = emb_grad.shape[0] // 8
    mat_rows = mat_grad.shape[0] // 8
    counts = (emb_rows // ROWS, mat_rows // ROWS)
    dma = pltpu.SemaphoreType.DMA
    scratch = [
        pltpu.VMEM((P_SLOTS, 2, 2, ROWS, WIDTH), F32),
        pltpu.VMEM((R_SLOTS, 2, 2, ROWS, WIDTH), F32),
        pltpu.VMEM((RING, 2, ROWS, SIDE_MAX), F32),
        pltpu.VMEM((RING, 2, ROWS, SIDE_MAX), F32),
        pltpu.VMEM((RING, 2, 2, ROWS, HALF_MAX), F32),
        pltpu.VMEM((RING, ROWS, 2 * SIDE_MAX), F32),
        pltpu.VMEM((RING, 2, ROWS, HALF_MAX), F32),
        pltpu.VMEM((RING, ROWS, HALF_MAX), F32),
        pltpu.VMEM((RING, ROWS, WIDTH), F32),
        pltpu.VMEM((ROWS, WIDTH), F32),
        pltpu.VMEM((NORM_ROWS, 1, WIDTH), F32),
        pltpu.VMEM((2, 2, 2) + NORM_PAD, F32),
        pltpu.VMEM((2, 2) + NORM_PAD, F32),
        pltpu.VMEM((2,) + NORM_PAD, F32),
        pltpu.VMEM(NORM_PAD, F32),
        pltpu.VMEM(NORM_PAD, F32),
        pltpu.VMEM((8, 128), F32),
        pltpu.VMEM((8, 8, 128), F32),
        dma((P_SLOTS,)), dma((R_SLOTS,)), dma((R_SLOTS,)), pltpu.SemaphoreType.REGULAR,
        dma((3, P_SLOTS)), dma((3, RING)), dma((3, SEND_SLOTS)), dma((3, RING)),
        dma((2, SEND_SLOTS)), dma((2, RING)), dma((SEND_SLOTS,)), dma((RING,)), dma((SEND_SLOTS,)),
        dma, dma((4,)), dma((4,)), dma((7,)), dma((8,)),
    ]
    hbm = pl.BlockSpec(memory_space=pl.ANY)
    vmem = pl.BlockSpec(memory_space=pltpu.VMEM)
    return pl.pallas_call(
        functools.partial(reduce_kernel, counts),
        out_shape=(
            jax.ShapeDtypeStruct((emb_rows, WIDTH), F32),
            jax.ShapeDtypeStruct((mat_rows, WIDTH), F32),
            jax.ShapeDtypeStruct(NORM_PAD, F32),
            jax.ShapeDtypeStruct((8, 128), F32),
        ),
        in_specs=[pl.BlockSpec(memory_space=pltpu.HBM)] * 3,
        out_specs=(hbm, hbm, vmem, vmem),
        scratch_shapes=scratch,
        compiler_params=pltpu.CompilerParams(
            collective_id=0, has_side_effects=True, vmem_limit_bytes=28 * 1024 * 1024
        ),
        name="reduce_grads",
    )(*(pltpu.with_memory_space_constraint(grad, pltpu.HBM) for grad in (
        emb_grad.reshape(2, 2, 2, emb_rows, WIDTH), mat_grad.reshape(2, 2, 2, mat_rows, WIDTH),
        norm_grad.reshape(NORM_ROWS, 1, WIDTH))))


BLOCK = 16
COLS = 384
STORE_SLOTS = 4


def adamw_block(grad, param, mom, var, decay_rate):
    new_mom = BETA_ONE * mom + (1.0 - BETA_ONE) * grad
    new_var = BETA_TWO * var + (1.0 - BETA_TWO) * grad * grad
    root = math.sqrt(1.0 - BETA_TWO ** ADAM_STEP)
    step_dir = new_mom / (jnp.sqrt(new_var) + ADAM_EPS * root)
    rate = LEARN_RATE * root / (1.0 - BETA_ONE ** ADAM_STEP)
    return param - (rate * step_dir + (LEARN_RATE * decay_rate) * param), new_mom, new_var


def adamw_kernel(scale, eg, ep, em, ev, mg, mp, mm, mv, ng, np_, nm, nv,
                 ep_out, em_out, ev_out, eb_out, mp_out, mm_out, mv_out, mb_out, np_out, nm_out, nv_out, nb_out,
                 p_buf, m_buf, v_buf, b_buf, n_bufs, nb_buf, sems, n_sems):
    clip = scale[0:1, 0:1]

    def copies(outs, slot, row):
        return [pltpu.make_async_copy(buf.at[slot], out.at[pl.ds(row, BLOCK), :], sems.at[k, slot])
                for k, (buf, out) in enumerate(zip((p_buf, m_buf, v_buf, b_buf), outs))]

    emb_outs = (ep_out, em_out, ev_out, eb_out)
    mat_outs = (mp_out, mm_out, mv_out, mb_out)
    emb_blocks = eg.shape[0] // BLOCK
    mat_blocks = mg.shape[0] // BLOCK

    def run(first, count, ins, outs):
        def body(i, carry):
            j = first + i
            slot = lax.rem(j, STORE_SLOTS)

            @pl.when(j >= STORE_SLOTS)
            def _():
                for copy in copies(emb_outs, slot, 0):
                    copy.wait()

            row = pl.multiple_of(i * BLOCK, BLOCK)
            for col in range(0, WIDTH, COLS):
                cols = pl.ds(col, COLS)
                g, p, m, v = (ref[pl.ds(row, BLOCK), cols] for ref in ins)
                new_p, new_m, new_v = adamw_block(g * clip, p, m, v, WEIGHT_DECAY)
                p_buf[slot, :, cols] = new_p
                m_buf[slot, :, cols] = new_m
                v_buf[slot, :, cols] = new_v
                b_buf[slot, :, cols] = new_p.astype(jnp.bfloat16)
            for copy in copies(outs, slot, row):
                copy.start()
            return carry

        lax.fori_loop(0, count, body, 0)

    run(0, emb_blocks, (eg, ep, em, ev), emb_outs)
    new_p, new_m, new_v = adamw_block(ng[:NORM_ROWS, :NORM_COLS] * clip, np_[...], nm[...], nv[...], 0.0)
    for k, value in enumerate((new_p, new_m, new_v)):
        n_bufs[k] = value
    nb_buf[...] = new_p.astype(jnp.bfloat16)
    norm_copies = [pltpu.make_async_copy(n_bufs.at[k], out, n_sems.at[k]) for k, out in enumerate((np_out, nm_out, nv_out))]
    norm_copies.append(pltpu.make_async_copy(nb_buf, nb_out, n_sems.at[3]))
    for copy in norm_copies:
        copy.start()
    run(emb_blocks, mat_blocks, (mg, mp, mm, mv), mat_outs)
    for slot in range(STORE_SLOTS):
        for copy in copies(emb_outs, slot, 0):
            copy.wait()
    for copy in norm_copies:
        copy.wait()


def adamw(scale, emb, mat, norm):
    shapes = []
    for ref in (emb[1], mat[1], norm[1]):
        shapes += [jax.ShapeDtypeStruct(ref.shape, F32)] * 3 + [jax.ShapeDtypeStruct(ref.shape, jnp.bfloat16)]
    buf = (STORE_SLOTS, BLOCK, WIDTH)
    vmem = pl.BlockSpec(memory_space=pltpu.VMEM)
    hbm = pl.BlockSpec(memory_space=pl.ANY)
    elements = emb[1].size + mat[1].size
    return pl.pallas_call(
        adamw_kernel,
        out_shape=tuple(shapes),
        in_specs=[vmem] * 13,
        out_specs=(hbm,) * 12,
        scratch_shapes=[
            pltpu.VMEM(buf, F32), pltpu.VMEM(buf, F32), pltpu.VMEM(buf, F32), pltpu.VMEM(buf, jnp.bfloat16),
            pltpu.VMEM((3, NORM_ROWS, NORM_COLS), F32), pltpu.VMEM((NORM_ROWS, NORM_COLS), jnp.bfloat16),
            pltpu.SemaphoreType.DMA((4, STORE_SLOTS)), pltpu.SemaphoreType.DMA((4,)),
        ],
        compiler_params=pltpu.CompilerParams(vmem_limit_bytes=8 * 1024 * 1024),
        cost_estimate=pl.CostEstimate(flops=20 * elements, bytes_accessed=30 * elements, transcendentals=2 * elements),
        name="adamw",
    )(scale, *emb, *mat, *norm)


def solution(mesh):
    def local_step(emb_grad, mat_grad, norm_grad, emb_param, emb_mom, emb_var, mat_param, mat_mom, mat_var, norm_param, norm_mom, norm_var):
        emb_mean, mat_mean, norm_mean, scale = reduce_grads(emb_grad[0, 0], mat_grad[0, 0], norm_grad[0, 0])
        return adamw(scale, (emb_mean, emb_param, emb_mom, emb_var), (mat_mean, mat_param, mat_mom, mat_var),
                     (norm_mean, norm_param, norm_mom, norm_var))

    grad_spec = P("dp", "fsdp", None, None)
    row_spec = P("fsdp", None)
    col_spec = P(None, "fsdp")
    in_list = (grad_spec, grad_spec, grad_spec, row_spec, row_spec, row_spec, row_spec, row_spec, row_spec, col_spec, col_spec, col_spec)
    out_list = (row_spec, row_spec, row_spec, row_spec, row_spec, row_spec, row_spec, row_spec, col_spec, col_spec, col_spec, col_spec)
    return jax.shard_map(local_step, mesh=mesh, in_specs=in_list, out_specs=out_list, check_vma=False)
```

```python
import functools
import math

import jax
import jax.numpy as jnp
from jax import lax
from jax.experimental import pallas as pl
from jax.experimental.pallas import tpu as pltpu
from jax.sharding import PartitionSpec as P

LEARN_RATE = 0.003
BETA_ONE = 0.9
BETA_TWO = 0.95
ADAM_EPS = 1e-8
WEIGHT_DECAY = 0.1
CLIP_NORM = 1.0
ADAM_STEP = 10

MESH = pl.DeviceIdType.MESH
F32 = jnp.float32

WIDTH = 5376
NORM_ROWS = 9
NORM_COLS = 672
NORM_PAD = (16, 768)
ROWS = 8
PLANS = ((1920, 768), (2176, 512))
INNER = (20, 44)
CUT = 2 * min(side for side, _ in PLANS)
SIDE_MAX = max(side for side, _ in PLANS)
HALF_MAX = max(half for _, half in PLANS)
LAG_ZERO = 1
LAG = 2
P_SLOTS = 10
R_SLOTS = 6
SEND_SLOTS = 8
RING = 16


def reduce_kernel(counts, emb, mat, norm, emb_out, mat_out, norm_out, scale_out,
                  part, recv_zero, xa, yb, zc, mid, wc, tc, grad, square,
                  norm_in, norm_part, norm_a, norm_b, norm_c, norm_d, sum_send, sum_recv,
                  load_sem, zero_send, zero_recv, credit,
                  one_send, one_recv, two_send, two_recv, three_send, three_recv, four_send, four_recv, out_sem,
                  norm_load, norm_send, norm_recv, sum_ssem, sum_rsem):
    emb_count, mat_count = counts
    total = emb_count + mat_count
    z = lax.axis_index("dp")
    f = lax.axis_index("fsdp")
    c = lax.rem(f, 2)
    x = lax.rem(lax.div(f, 2), 2)
    y = lax.div(f, 4)
    core = (z, f + 1 - 2 * c)
    xn = (z, f + 2 - 4 * x)
    yn = (z, f + 4 - 8 * y)
    zn = (1 - z, f)
    peers = [(z, lax.rem(f + k, 8)) for k in range(1, 8)]

    def remote(src, dst, ssem, rsem, dev):
        return pltpu.make_async_remote_copy(src_ref=src, dst_ref=dst, send_sem=ssem, recv_sem=rsem,
                                            device_id=dev, device_id_type=MESH)

    def on_plan(j, body):
        inner = jnp.logical_and(j >= INNER[0], j < INNER[1])
        pl.when(jnp.logical_not(inner))(lambda: body(j, *PLANS[0]))
        pl.when(inner)(lambda: body(j, *PLANS[1]))

    def half_at(side, half, which):
        return pl.ds(pl.multiple_of(2 * side + which * half, 128), half)

    barrier = pltpu.get_barrier_semaphore()
    for dev in (core, xn, yn, zn):
        pl.semaphore_signal(barrier, inc=1, device_id=dev, device_id_type=MESH)
    norm_copy = pltpu.make_async_copy(norm, norm_in, norm_load)
    norm_copy.start()

    def on_rows(j, body):
        @pl.when(j < emb_count)
        def _():
            body(emb, emb_out, pl.multiple_of(j * ROWS, ROWS))

        @pl.when(j >= emb_count)
        def _():
            body(mat, mat_out, pl.multiple_of((j - emb_count) * ROWS, ROWS))

    def load_copy(ref, row, j):
        s = lax.rem(j, P_SLOTS)
        return pltpu.make_async_copy(ref.at[:, :, c, pl.ds(row, ROWS), :], part.at[s], load_sem.at[s])

    def zero_copies(ref, row, j):
        s = lax.rem(j, R_SLOTS)
        return [remote(ref.at[:, :, 1 - c, pl.ds(row, ROWS), cols], recv_zero.at[s, :, :, :, cols],
                       zero_send.at[k, s], zero_recv.at[k, s], core)
                for k, cols in enumerate((pl.ds(CUT, WIDTH - CUT), pl.ds(0, CUT)))]

    def ones(j, side, half):
        s, r = lax.rem(j, P_SLOTS), lax.rem(j, RING)
        return (remote(part.at[s, :, :, :, half_at(side, half, 1 - z)], zc.at[r, :, :, :, :half], one_send.at[2, s], one_recv.at[2, r], zn),
                remote(part.at[s, :, 1 - x, :, :side], xa.at[r, :, :, :side], one_send.at[0, s], one_recv.at[0, r], xn),
                remote(part.at[s, 1 - y, :, :, side:2 * side], yb.at[r, :, :, :side], one_send.at[1, s], one_recv.at[1, r], yn))

    def two_c_even(j, side, half):
        s, r = lax.rem(j, SEND_SLOTS), lax.rem(j, RING)
        return remote(zc.at[r, :, 1 - x, :, :half], wc.at[r, :, :, :half], two_send.at[2, s], two_recv.at[2, r], xn)

    def two_c_odd(j, side, half):
        s, r = lax.rem(j, SEND_SLOTS), lax.rem(j, RING)
        return remote(zc.at[r, 1 - y, :, :, :half], wc.at[r, :, :, :half], two_send.at[2, s], two_recv.at[2, r], yn)

    def twos(j, side, half):
        s, r = lax.rem(j, SEND_SLOTS), lax.rem(j, RING)
        return (remote(xa.at[r, 1 - y, :, :side], mid.at[r, :, :side], two_send.at[0, s], two_recv.at[0, r], yn),
                remote(yb.at[r, 1 - x, :, :side], mid.at[r, :, side:2 * side], two_send.at[1, s], two_recv.at[1, r], xn))

    def three_c(j, side, half):
        s, r, odd = lax.rem(j, SEND_SLOTS), lax.rem(j, RING), lax.rem(j, 2)
        here = y + odd * (x - y)
        step = (4 - 8 * y) + odd * ((2 - 4 * x) - (4 - 8 * y))
        return remote(wc.at[r, 1 - here, :, :half], tc.at[r, :, :half], three_send.at[1, s], three_recv.at[1, r], (z, f + step))

    def three_ab(j, side, half):
        s, r = lax.rem(j, SEND_SLOTS), lax.rem(j, RING)
        return remote(mid.at[r, :, :2 * side], grad.at[r, :, :2 * side], three_send.at[0, s], three_recv.at[0, r], zn)

    def four(j, side, half, which):
        s, r = lax.rem(j, SEND_SLOTS), lax.rem(j, RING)
        cols = half_at(side, half, which)
        return remote(grad.at[r, :, cols], grad.at[r, :, cols], four_send.at[s], four_recv.at[r], zn)

    def out_copy(ref, row, j):
        return pltpu.make_async_copy(grad.at[lax.rem(j, RING)], ref.at[pl.ds(row, ROWS), :],
                                     out_sem.at[lax.rem(j, SEND_SLOTS)])

    norm_zero = remote(norm_part.at[:, :, 1 - c], norm_a, norm_send.at[0], norm_recv.at[0], core)
    norm_one = remote(norm_a.at[:, 1 - x], norm_b, norm_send.at[1], norm_recv.at[1], xn)
    norm_two = remote(norm_b.at[1 - y], norm_c, norm_send.at[2], norm_recv.at[2], yn)
    norm_three = remote(norm_c, norm_d, norm_send.at[3], norm_recv.at[3], zn)

    def when_in(j, body):
        pl.when(jnp.logical_and(j >= 0, j < total))(functools.partial(body, j))

    def after(j, slots, copies):
        @pl.when(j >= slots)
        def _():
            on_plan(j - slots, lambda *args: wait_send(copies(*args)))

    def start(copies):
        for copy in copies:
            copy.start()

    def wait_send(copies):
        for copy in copies:
            copy.wait_send()

    def stage_issue(j):
        after(j, P_SLOTS, ones)

        @pl.when(j >= R_SLOTS)
        def _():
            wait_send(zero_copies(emb, 0, j - R_SLOTS))
            pl.semaphore_wait(credit, 1)

        def body(ref, _, row):
            start(zero_copies(ref, row, j))
            load_copy(ref, row, j).start()

        on_rows(j, body)

    def stage_one(j):
        load_copy(emb, 0, j).wait()
        zero_copies(emb, 0, j)[0].wait_recv()
        part[lax.rem(j, P_SLOTS), :, :, :, CUT:] += recv_zero[lax.rem(j, R_SLOTS), :, :, :, CUT:]
        on_plan(j, lambda *args: start(ones(*args)[:1]))

    def stage_one_more(j):
        zero_copies(emb, 0, j)[1].wait_recv()
        part[lax.rem(j, P_SLOTS), :, :, :, :CUT] += recv_zero[lax.rem(j, R_SLOTS), :, :, :, :CUT]

        @pl.when(j + R_SLOTS < total)
        def _():
            pl.semaphore_signal(credit, inc=1, device_id=core, device_id_type=MESH)

        on_plan(j, lambda *args: start(ones(*args)[1:]))

    def stage_two(j):
        after(j, SEND_SLOTS, lambda *args: twos(*args) + (two_c_even(*args),))

        def body(j, side, half):
            s, r = lax.rem(j, P_SLOTS), lax.rem(j, RING)
            even = lax.rem(j, 2) == 0
            for copy in ones(j, side, half):
                copy.wait_recv()
            zc[r, :, :, :, :half] += part[s, :, :, :, half_at(side, half, z)]
            xa[r, :, :, :side] += part[s, :, x, :, :side]
            yb[r, :, :, :side] += part[s, y, :, :, side:2 * side]
            pl.when(even)(lambda: two_c_even(j, side, half).start())
            pl.when(jnp.logical_not(even))(lambda: two_c_odd(j, side, half).start())
            start(twos(j, side, half))

        on_plan(j, body)

    def stage_three(j):
        after(j, SEND_SLOTS, lambda *args: (three_ab(*args), three_c(*args)))

        def body(j, side, half):
            r = lax.rem(j, RING)
            even = lax.rem(j, 2) == 0
            for copy in twos(j, side, half) + (two_c_even(j, side, half),):
                copy.wait_recv()

            @pl.when(even)
            def _():
                wc[r, :, :, :half] += zc[r, :, x, :, :half]

            @pl.when(jnp.logical_not(even))
            def _():
                wc[r, :, :, :half] += zc[r, y, :, :, :half]

            mid[r, :, :side] += xa[r, y, :, :side]
            mid[r, :, side:2 * side] += yb[r, x, :, :side]
            start((three_c(j, side, half), three_ab(j, side, half)))

        on_plan(j, body)

    def stage_four(j):
        after(j, SEND_SLOTS, lambda *args: (four(*args, z),))

        def body(j, side, half):
            r, odd = lax.rem(j, RING), lax.rem(j, 2)
            here = y + odd * (x - y)
            three_c(j, side, half).wait_recv()
            grad[r, :, half_at(side, half, z)] = (tc[r, :, :half] + wc[r, here, :, :half]) * (1.0 / 16.0)
            four(j, side, half, z).start()

        on_plan(j, body)

    def stage_five(j):
        def body(j, side, half):
            r = lax.rem(j, RING)
            three_ab(j, side, half).wait_recv()
            both = (grad[r, :, :2 * side] + mid[r, :, :2 * side]) * (1.0 / 16.0)
            grad[r, :, :2 * side] = both
            square[:, :2 * side] += both * both
            four(j, side, half, 1 - z).wait_recv()
            rest = grad[r, :, 2 * side:]
            square[:, 2 * side:] += rest * rest

        on_plan(j, body)

        @pl.when(j >= SEND_SLOTS)
        def _():
            out_copy(emb_out, 0, j - SEND_SLOTS).wait()

        def store(_, ref, row):
            out_copy(ref, row, j).start()

        on_rows(j, store)

    def trip(it, carry):
        when_in(it, stage_issue)
        when_in(it - LAG_ZERO, stage_one)
        when_in(it - LAG_ZERO - 4 * LAG, stage_five)
        when_in(it - LAG_ZERO - 3 * LAG, stage_four)
        when_in(it - LAG_ZERO - 2 * LAG, stage_three)
        when_in(it - LAG_ZERO - LAG, stage_two)
        when_in(it - LAG_ZERO, stage_one_more)

        @pl.when(it == 5)
        def _():
            norm_copy.wait()
            for k in range(8):
                for row in range(NORM_ROWS):
                    norm_part[k // 4, (k // 2) % 2, k % 2, row:row + 1, :NORM_COLS] = norm_in[row, :, k * NORM_COLS:(k + 1) * NORM_COLS]
            norm_zero.start()

        @pl.when(it == 8)
        def _():
            norm_zero.wait_recv()
            norm_a[...] += norm_part[:, :, c]
            norm_one.start()

        @pl.when(it == 12)
        def _():
            norm_one.wait_recv()
            norm_b[...] += norm_a[:, x]
            norm_two.start()

        @pl.when(it == 16)
        def _():
            norm_two.wait_recv()
            norm_c[...] += norm_b[y]
            norm_three.start()

        @pl.when(it == 20)
        def _():
            norm_three.wait_recv()
            norm_d[...] = (norm_d[...] + norm_c[...]) * (1.0 / 16.0)
            norm_out[...] = norm_d[...]
            norm_sq = norm_d[...] * norm_d[...]
            square[:, :NORM_PAD[1]] += norm_sq[:ROWS] + norm_sq[ROWS:]

        return carry

    norm_part[...] = jnp.zeros_like(norm_part)
    square[...] = jnp.zeros_like(square)
    pl.semaphore_wait(barrier, 4)
    lax.fori_loop(0, total + LAG_ZERO + 4 * LAG, trip, 0)

    value = jnp.full((8, 128), jnp.sum(square[...]), F32)
    sum_send[...] = value
    sum_recv[f] = value
    sums = [remote(sum_send, sum_recv.at[f], sum_ssem.at[k], sum_rsem.at[f], dev) for k, dev in enumerate(peers)]
    start(sums)
    wait_send((norm_zero, norm_one, norm_two, norm_three))

    def drain(slots, copies):
        def body(j, carry):
            on_plan(j, lambda *args: wait_send(copies(*args)))
            return carry
        lax.fori_loop(total - slots, total, body, 0)

    drain(P_SLOTS, ones)
    drain(R_SLOTS, lambda j, side, half: zero_copies(emb, 0, j))
    drain(SEND_SLOTS, lambda *args: twos(*args) + (two_c_even(*args), three_ab(*args), three_c(*args), four(*args, z)))

    def last(j, carry):
        out_copy(emb_out, 0, j).wait()
        return carry

    lax.fori_loop(total - SEND_SLOTS, total, last, 0)

    for k in range(1, 8):
        s = lax.rem(f + k, 8)
        remote(sum_send, sum_recv.at[s], sum_ssem.at[0], sum_rsem.at[s], core).wait_recv()
    whole = sum_recv[0]
    for k in range(1, 8):
        whole = whole + sum_recv[k]
    scale_out[...] = jnp.minimum(1.0, CLIP_NORM / jnp.sqrt(whole))
    wait_send(sums)


def reduce_grads(emb_grad, mat_grad, norm_grad):
    emb_rows = emb_grad.shape[0] // 8
    mat_rows = mat_grad.shape[0] // 8
    counts = (emb_rows // ROWS, mat_rows // ROWS)
    dma = pltpu.SemaphoreType.DMA
    scratch = [
        pltpu.VMEM((P_SLOTS, 2, 2, ROWS, WIDTH), F32),
        pltpu.VMEM((R_SLOTS, 2, 2, ROWS, WIDTH), F32),
        pltpu.VMEM((RING, 2, ROWS, SIDE_MAX), F32),
        pltpu.VMEM((RING, 2, ROWS, SIDE_MAX), F32),
        pltpu.VMEM((RING, 2, 2, ROWS, HALF_MAX), F32),
        pltpu.VMEM((RING, ROWS, 2 * SIDE_MAX), F32),
        pltpu.VMEM((RING, 2, ROWS, HALF_MAX), F32),
        pltpu.VMEM((RING, ROWS, HALF_MAX), F32),
        pltpu.VMEM((RING, ROWS, WIDTH), F32),
        pltpu.VMEM((ROWS, WIDTH), F32),
        pltpu.VMEM((NORM_ROWS, 1, WIDTH), F32),
        pltpu.VMEM((2, 2, 2) + NORM_PAD, F32),
        pltpu.VMEM((2, 2) + NORM_PAD, F32),
        pltpu.VMEM((2,) + NORM_PAD, F32),
        pltpu.VMEM(NORM_PAD, F32),
        pltpu.VMEM(NORM_PAD, F32),
        pltpu.VMEM((8, 128), F32),
        pltpu.VMEM((8, 8, 128), F32),
        dma((P_SLOTS,)), dma((2, R_SLOTS)), dma((2, R_SLOTS)), pltpu.SemaphoreType.REGULAR,
        dma((3, P_SLOTS)), dma((3, RING)), dma((3, SEND_SLOTS)), dma((3, RING)),
        dma((2, SEND_SLOTS)), dma((2, RING)), dma((SEND_SLOTS,)), dma((RING,)), dma((SEND_SLOTS,)),
        dma, dma((4,)), dma((4,)), dma((7,)), dma((8,)),
    ]
    hbm = pl.BlockSpec(memory_space=pl.ANY)
    vmem = pl.BlockSpec(memory_space=pltpu.VMEM)
    return pl.pallas_call(
        functools.partial(reduce_kernel, counts),
        out_shape=(
            jax.ShapeDtypeStruct((emb_rows, WIDTH), F32),
            jax.ShapeDtypeStruct((mat_rows, WIDTH), F32),
            jax.ShapeDtypeStruct(NORM_PAD, F32),
            jax.ShapeDtypeStruct((8, 128), F32),
        ),
        in_specs=[pl.BlockSpec(memory_space=pltpu.HBM)] * 3,
        out_specs=(hbm, hbm, vmem, vmem),
        scratch_shapes=scratch,
        compiler_params=pltpu.CompilerParams(
            collective_id=0, has_side_effects=True, vmem_limit_bytes=28 * 1024 * 1024
        ),
        name="reduce_grads",
    )(*(pltpu.with_memory_space_constraint(grad, pltpu.HBM) for grad in (
        emb_grad.reshape(2, 2, 2, emb_rows, WIDTH), mat_grad.reshape(2, 2, 2, mat_rows, WIDTH),
        norm_grad.reshape(NORM_ROWS, 1, WIDTH))))


BLOCK = 16
COLS = 384
SIDE = WIDTH // 2
STORE_SLOTS = 4


def adamw_block(grad, param, mom, var, decay_rate):
    new_mom = BETA_ONE * mom + (1.0 - BETA_ONE) * grad
    new_var = BETA_TWO * var + (1.0 - BETA_TWO) * grad * grad
    root = math.sqrt(1.0 - BETA_TWO ** ADAM_STEP)
    step_dir = new_mom / (jnp.sqrt(new_var) + ADAM_EPS * root)
    rate = LEARN_RATE * root / (1.0 - BETA_ONE ** ADAM_STEP)
    return param - (rate * step_dir + (LEARN_RATE * decay_rate) * param), new_mom, new_var


def adamw_kernel(scale, eg, ep, em, ev, mg, mp, mm, mv, ng, np_, nm, nv,
                 ep_out, em_out, ev_out, eb_out, mp_out, mm_out, mv_out, mb_out, np_out, nm_out, nv_out, nb_out,
                 p_buf, m_buf, v_buf, b_buf, n_bufs, nb_buf, sems, n_sems):
    clip = scale[0:1, 0:1]

    def copies(outs, slot, row, side):
        cols = pl.ds(side * SIDE, SIDE)
        return [pltpu.make_async_copy(buf.at[slot, side], out.at[pl.ds(row, BLOCK), cols], sems.at[k, slot, side])
                for k, (buf, out) in enumerate(zip((p_buf, m_buf, v_buf, b_buf), outs))]

    emb_outs = (ep_out, em_out, ev_out, eb_out)
    mat_outs = (mp_out, mm_out, mv_out, mb_out)
    emb_blocks = eg.shape[0] // BLOCK
    mat_blocks = mg.shape[0] // BLOCK

    def run(first, count, ins, outs):
        def body(i, carry):
            j = first + i
            slot = lax.rem(j, STORE_SLOTS)

            row = pl.multiple_of(i * BLOCK, BLOCK)
            for side in range(2):
                @pl.when(j >= STORE_SLOTS)
                def _():
                    for copy in copies(emb_outs, slot, 0, side):
                        copy.wait()

                for col in range(0, SIDE, COLS):
                    here, cols = pl.ds(col, COLS), pl.ds(side * SIDE + col, COLS)
                    g, p, m, v = (ref[pl.ds(row, BLOCK), cols] for ref in ins)
                    new_p, new_m, new_v = adamw_block(g * clip, p, m, v, WEIGHT_DECAY)
                    p_buf[slot, side, :, here] = new_p
                    m_buf[slot, side, :, here] = new_m
                    v_buf[slot, side, :, here] = new_v
                    b_buf[slot, side, :, here] = new_p.astype(jnp.bfloat16)
                for copy in copies(outs, slot, row, side):
                    copy.start()
            return carry

        lax.fori_loop(0, count, body, 0)

    run(0, emb_blocks, (eg, ep, em, ev), emb_outs)
    run(emb_blocks, mat_blocks, (mg, mp, mm, mv), mat_outs)
    new_p, new_m, new_v = adamw_block(ng[:NORM_ROWS, :NORM_COLS] * clip, np_[...], nm[...], nv[...], 0.0)
    for k, value in enumerate((new_p, new_m, new_v)):
        n_bufs[k] = value
    nb_buf[...] = new_p.astype(jnp.bfloat16)
    norm_copies = [pltpu.make_async_copy(n_bufs.at[k], out, n_sems.at[k]) for k, out in enumerate((np_out, nm_out, nv_out))]
    norm_copies.append(pltpu.make_async_copy(nb_buf, nb_out, n_sems.at[3]))
    for copy in norm_copies:
        copy.start()
    for slot in range(STORE_SLOTS):
        for side in range(2):
            for copy in copies(emb_outs, slot, 0, side):
                copy.wait()
    for copy in norm_copies:
        copy.wait()


def adamw(scale, emb, mat, norm):
    shapes = []
    for ref in (emb[1], mat[1], norm[1]):
        shapes += [jax.ShapeDtypeStruct(ref.shape, F32)] * 3 + [jax.ShapeDtypeStruct(ref.shape, jnp.bfloat16)]
    buf = (STORE_SLOTS, 2, BLOCK, SIDE)
    vmem = pl.BlockSpec(memory_space=pltpu.VMEM)
    hbm = pl.BlockSpec(memory_space=pl.ANY)
    elements = emb[1].size + mat[1].size
    return pl.pallas_call(
        adamw_kernel,
        out_shape=tuple(shapes),
        in_specs=[vmem] * 13,
        out_specs=(hbm,) * 12,
        scratch_shapes=[
            pltpu.VMEM(buf, F32), pltpu.VMEM(buf, F32), pltpu.VMEM(buf, F32), pltpu.VMEM(buf, jnp.bfloat16),
            pltpu.VMEM((3, NORM_ROWS, NORM_COLS), F32), pltpu.VMEM((NORM_ROWS, NORM_COLS), jnp.bfloat16),
            pltpu.SemaphoreType.DMA((4, STORE_SLOTS, 2)), pltpu.SemaphoreType.DMA((4,)),
        ],
        compiler_params=pltpu.CompilerParams(vmem_limit_bytes=8 * 1024 * 1024),
        cost_estimate=pl.CostEstimate(flops=20 * elements, bytes_accessed=30 * elements, transcendentals=2 * elements),
        name="adamw",
    )(scale, *emb, *mat, *norm)


def solution(mesh):
    def local_step(emb_grad, mat_grad, norm_grad, emb_param, emb_mom, emb_var, mat_param, mat_mom, mat_var, norm_param, norm_mom, norm_var):
        emb_mean, mat_mean, norm_mean, scale = reduce_grads(emb_grad[0, 0], mat_grad[0, 0], norm_grad[0, 0])
        return adamw(scale, (emb_mean, emb_param, emb_mom, emb_var), (mat_mean, mat_param, mat_mom, mat_var),
                     (norm_mean, norm_param, norm_mom, norm_var))

    grad_spec = P("dp", "fsdp", None, None)
    row_spec = P("fsdp", None)
    col_spec = P(None, "fsdp")
    in_list = (grad_spec, grad_spec, grad_spec, row_spec, row_spec, row_spec, row_spec, row_spec, row_spec, col_spec, col_spec, col_spec)
    out_list = (row_spec, row_spec, row_spec, row_spec, row_spec, row_spec, row_spec, row_spec, col_spec, col_spec, col_spec, col_spec)
    return jax.shard_map(local_step, mesh=mesh, in_specs=in_list, out_specs=out_list, check_vma=False)
```

```python
import functools
import math

import jax
import jax.numpy as jnp
from jax import lax
from jax.experimental import pallas as pl
from jax.experimental.pallas import tpu as pltpu
from jax.sharding import PartitionSpec as P

LEARN_RATE = 0.003
BETA_ONE = 0.9
BETA_TWO = 0.95
ADAM_EPS = 1e-8
WEIGHT_DECAY = 0.1
CLIP_NORM = 1.0
ADAM_STEP = 10

MESH = pl.DeviceIdType.MESH
F32 = jnp.float32

WIDTH = 5376
NORM_ROWS = 9
NORM_COLS = 672
NORM_PAD = (16, 768)
ROWS = 8
PLANS = ((1920, 768), (2176, 512))
INNER = (20, 44)
CUT = 2 * min(side for side, _ in PLANS)
SIDE_MAX = max(side for side, _ in PLANS)
HALF_MAX = max(half for _, half in PLANS)
LAG_ZERO = 0
LAG = 2
P_SLOTS = 10
R_SLOTS = 6
SEND_SLOTS = 8
RING = 16


def reduce_kernel(counts, emb, mat, norm, emb_out, mat_out, norm_out, scale_out,
                  part, recv_zero, xa, yb, zc, mid, wc, tc, grad, square,
                  norm_in, norm_part, norm_a, norm_b, norm_c, norm_d, sum_send, sum_recv,
                  load_sem, zero_send, zero_recv, credit,
                  one_send, one_recv, two_send, two_recv, three_send, three_recv, four_send, four_recv, out_sem,
                  norm_load, norm_send, norm_recv, sum_ssem, sum_rsem):
    emb_count, mat_count = counts
    total = emb_count + mat_count
    z = lax.axis_index("dp")
    f = lax.axis_index("fsdp")
    c = lax.rem(f, 2)
    x = lax.rem(lax.div(f, 2), 2)
    y = lax.div(f, 4)
    core = (z, f + 1 - 2 * c)
    xn = (z, f + 2 - 4 * x)
    yn = (z, f + 4 - 8 * y)
    zn = (1 - z, f)
    peers = [(z, lax.rem(f + k, 8)) for k in range(1, 8)]

    def remote(src, dst, ssem, rsem, dev):
        return pltpu.make_async_remote_copy(src_ref=src, dst_ref=dst, send_sem=ssem, recv_sem=rsem,
                                            device_id=dev, device_id_type=MESH)

    def on_plan(j, body):
        inner = jnp.logical_and(j >= INNER[0], j < INNER[1])
        pl.when(jnp.logical_not(inner))(lambda: body(j, *PLANS[0]))
        pl.when(inner)(lambda: body(j, *PLANS[1]))

    def half_at(side, half, which):
        return pl.ds(pl.multiple_of(2 * side + which * half, 128), half)

    barrier = pltpu.get_barrier_semaphore()
    for dev in (core, xn, yn, zn):
        pl.semaphore_signal(barrier, inc=1, device_id=dev, device_id_type=MESH)
    norm_copy = pltpu.make_async_copy(norm, norm_in, norm_load)
    norm_copy.start()

    def on_rows(j, body):
        @pl.when(j < emb_count)
        def _():
            body(emb, emb_out, pl.multiple_of(j * ROWS, ROWS))

        @pl.when(j >= emb_count)
        def _():
            body(mat, mat_out, pl.multiple_of((j - emb_count) * ROWS, ROWS))

    def load_copy(ref, row, j):
        s = lax.rem(j, P_SLOTS)
        return pltpu.make_async_copy(ref.at[:, :, c, pl.ds(row, ROWS), :], part.at[s], load_sem.at[s])

    def exchange(source, s):
        return [remote(source.at[:, :, :, cols], recv_zero.at[s, :, :, :, cols], zero_send.at[k, s], zero_recv.at[k, s], core)
                for k, cols in enumerate((pl.ds(CUT, WIDTH - CUT), pl.ds(0, CUT)))]

    def zero_copies(ref, row, j):
        return exchange(ref.at[:, :, 1 - c, pl.ds(row, ROWS)], lax.rem(j, R_SLOTS))

    def ones(j, side, half):
        s, r = lax.rem(j, P_SLOTS), lax.rem(j, RING)
        return (remote(part.at[s, :, :, :, half_at(side, half, 1 - z)], zc.at[r, :, :, :, :half], one_send.at[2, s], one_recv.at[2, r], zn),
                remote(part.at[s, :, 1 - x, :, :side], xa.at[r, :, :, :side], one_send.at[0, s], one_recv.at[0, r], xn),
                remote(part.at[s, 1 - y, :, :, side:2 * side], yb.at[r, :, :, :side], one_send.at[1, s], one_recv.at[1, r], yn))

    def two_c_even(j, side, half):
        s, r = lax.rem(j, SEND_SLOTS), lax.rem(j, RING)
        return remote(zc.at[r, :, 1 - x, :, :half], wc.at[r, :, :, :half], two_send.at[2, s], two_recv.at[2, r], xn)

    def two_c_odd(j, side, half):
        s, r = lax.rem(j, SEND_SLOTS), lax.rem(j, RING)
        return remote(zc.at[r, 1 - y, :, :, :half], wc.at[r, :, :, :half], two_send.at[2, s], two_recv.at[2, r], yn)

    def twos(j, side, half):
        s, r = lax.rem(j, SEND_SLOTS), lax.rem(j, RING)
        return (remote(xa.at[r, 1 - y, :, :side], mid.at[r, :, :side], two_send.at[0, s], two_recv.at[0, r], yn),
                remote(yb.at[r, 1 - x, :, :side], mid.at[r, :, side:2 * side], two_send.at[1, s], two_recv.at[1, r], xn))

    def three_c(j, side, half):
        s, r, odd = lax.rem(j, SEND_SLOTS), lax.rem(j, RING), lax.rem(j, 2)
        here = y + odd * (x - y)
        step = (4 - 8 * y) + odd * ((2 - 4 * x) - (4 - 8 * y))
        return remote(wc.at[r, 1 - here, :, :half], tc.at[r, :, :half], three_send.at[1, s], three_recv.at[1, r], (z, f + step))

    def three_ab(j, side, half):
        s, r = lax.rem(j, SEND_SLOTS), lax.rem(j, RING)
        return remote(mid.at[r, :, :2 * side], grad.at[r, :, :2 * side], three_send.at[0, s], three_recv.at[0, r], zn)

    def four(j, side, half, which):
        s, r = lax.rem(j, SEND_SLOTS), lax.rem(j, RING)
        cols = half_at(side, half, which)
        return remote(grad.at[r, :, cols], grad.at[r, :, cols], four_send.at[s], four_recv.at[r], zn)

    def out_copy(ref, row, j):
        return pltpu.make_async_copy(grad.at[lax.rem(j, RING)], ref.at[pl.ds(row, ROWS), :],
                                     out_sem.at[lax.rem(j, SEND_SLOTS)])

    norm_zero = remote(norm_part.at[:, :, 1 - c], norm_a, norm_send.at[0], norm_recv.at[0], core)
    norm_one = remote(norm_a.at[:, 1 - x], norm_b, norm_send.at[1], norm_recv.at[1], xn)
    norm_two = remote(norm_b.at[1 - y], norm_c, norm_send.at[2], norm_recv.at[2], yn)
    norm_three = remote(norm_c, norm_d, norm_send.at[3], norm_recv.at[3], zn)

    def when_in(j, body):
        pl.when(jnp.logical_and(j >= 0, j < total))(functools.partial(body, j))

    def after(j, slots, copies):
        @pl.when(j >= slots)
        def _():
            on_plan(j - slots, lambda *args: wait_send(copies(*args)))

    def start(copies):
        for copy in copies:
            copy.start()

    def wait_send(copies):
        for copy in copies:
            copy.wait_send()

    def stage_issue(j):
        after(j, P_SLOTS, ones)

        @pl.when(j >= R_SLOTS)
        def _():
            wait_send(zero_copies(emb, 0, j - R_SLOTS))
            pl.semaphore_wait(credit, 1)

        def body(ref, _, row):
            start(zero_copies(ref, row, j))
            load_copy(ref, row, j).start()

        on_rows(j, body)

    def stage_one(j):
        load_copy(emb, 0, j).wait()
        zero_copies(emb, 0, j)[0].wait_recv()
        part[lax.rem(j, P_SLOTS), :, :, :, CUT:] += recv_zero[lax.rem(j, R_SLOTS), :, :, :, CUT:]
        on_plan(j, lambda *args: start(ones(*args)[:1]))

    def stage_one_more(j):
        zero_copies(emb, 0, j)[1].wait_recv()
        part[lax.rem(j, P_SLOTS), :, :, :, :CUT] += recv_zero[lax.rem(j, R_SLOTS), :, :, :, :CUT]

        @pl.when(j + R_SLOTS < total)
        def _():
            pl.semaphore_signal(credit, inc=1, device_id=core, device_id_type=MESH)

        on_plan(j, lambda *args: start(ones(*args)[1:]))

    def stage_two(j):
        after(j, SEND_SLOTS, lambda *args: twos(*args) + (two_c_even(*args),))

        def body(j, side, half):
            s, r = lax.rem(j, P_SLOTS), lax.rem(j, RING)
            even = lax.rem(j, 2) == 0
            for copy in ones(j, side, half):
                copy.wait_recv()
            zc[r, :, :, :, :half] += part[s, :, :, :, half_at(side, half, z)]
            xa[r, :, :, :side] += part[s, :, x, :, :side]
            yb[r, :, :, :side] += part[s, y, :, :, side:2 * side]
            pl.when(even)(lambda: two_c_even(j, side, half).start())
            pl.when(jnp.logical_not(even))(lambda: two_c_odd(j, side, half).start())
            start(twos(j, side, half))

        on_plan(j, body)

    def stage_three(j):
        after(j, SEND_SLOTS, lambda *args: (three_ab(*args), three_c(*args)))

        def body(j, side, half):
            r = lax.rem(j, RING)
            even = lax.rem(j, 2) == 0
            for copy in twos(j, side, half) + (two_c_even(j, side, half),):
                copy.wait_recv()

            @pl.when(even)
            def _():
                wc[r, :, :, :half] += zc[r, :, x, :, :half]

            @pl.when(jnp.logical_not(even))
            def _():
                wc[r, :, :, :half] += zc[r, y, :, :, :half]

            mid[r, :, :side] += xa[r, y, :, :side]
            mid[r, :, side:2 * side] += yb[r, x, :, :side]
            start((three_c(j, side, half), three_ab(j, side, half)))

        on_plan(j, body)

    def stage_four(j):
        after(j, SEND_SLOTS, lambda *args: (four(*args, z),))

        def body(j, side, half):
            r, odd = lax.rem(j, RING), lax.rem(j, 2)
            here = y + odd * (x - y)
            three_c(j, side, half).wait_recv()
            grad[r, :, half_at(side, half, z)] = (tc[r, :, :half] + wc[r, here, :, :half]) * (1.0 / 16.0)
            four(j, side, half, z).start()

        on_plan(j, body)

    def stage_five(j):
        def body(j, side, half):
            r = lax.rem(j, RING)
            three_ab(j, side, half).wait_recv()
            both = (grad[r, :, :2 * side] + mid[r, :, :2 * side]) * (1.0 / 16.0)
            grad[r, :, :2 * side] = both
            square[:, :2 * side] += both * both
            four(j, side, half, 1 - z).wait_recv()
            rest = grad[r, :, 2 * side:]
            square[:, 2 * side:] += rest * rest

        on_plan(j, body)

        @pl.when(j >= SEND_SLOTS)
        def _():
            out_copy(emb_out, 0, j - SEND_SLOTS).wait()

        def store(_, ref, row):
            out_copy(ref, row, j).start()

        on_rows(j, store)

    def trip(it, carry):
        when_in(it + 1, stage_issue)
        when_in(it - LAG_ZERO, stage_one)
        when_in(it - LAG_ZERO - 4 * LAG, stage_five)
        when_in(it - LAG_ZERO - 3 * LAG, stage_four)
        when_in(it - LAG_ZERO - 2 * LAG, stage_three)
        when_in(it - LAG_ZERO - LAG, stage_two)
        when_in(it - LAG_ZERO, stage_one_more)

        @pl.when(it == 5)
        def _():
            norm_copy.wait()
            for k in range(8):
                for row in range(NORM_ROWS):
                    norm_part[k // 4, (k // 2) % 2, k % 2, row:row + 1, :NORM_COLS] = norm_in[row, :, k * NORM_COLS:(k + 1) * NORM_COLS]
            norm_zero.start()

        @pl.when(it == 8)
        def _():
            norm_zero.wait_recv()
            norm_a[...] += norm_part[:, :, c]
            norm_one.start()

        @pl.when(it == 12)
        def _():
            norm_one.wait_recv()
            norm_b[...] += norm_a[:, x]
            norm_two.start()

        @pl.when(it == 16)
        def _():
            norm_two.wait_recv()
            norm_c[...] += norm_b[y]
            norm_three.start()

        @pl.when(it == 20)
        def _():
            norm_three.wait_recv()
            norm_d[...] = (norm_d[...] + norm_c[...]) * (1.0 / 16.0)
            norm_out[...] = norm_d[...]
            norm_sq = norm_d[...] * norm_d[...]
            square[:, :NORM_PAD[1]] += norm_sq[:ROWS] + norm_sq[ROWS:]

        return carry

    ahead = pltpu.make_async_copy(emb.at[:, :, 1 - c, pl.ds(0, ROWS), :], part.at[P_SLOTS - 1], load_sem.at[P_SLOTS - 1])
    ahead.start()
    load_copy(emb, 0, 0).start()
    norm_part[...] = jnp.zeros_like(norm_part)
    square[...] = jnp.zeros_like(square)
    ahead.wait()
    pl.semaphore_wait(barrier, 4)
    start(exchange(part.at[P_SLOTS - 1], 0))
    lax.fori_loop(0, total + LAG_ZERO + 4 * LAG, trip, 0)

    value = jnp.full((8, 128), jnp.sum(square[...]), F32)
    sum_send[...] = value
    sum_recv[f] = value
    sums = [remote(sum_send, sum_recv.at[f], sum_ssem.at[k], sum_rsem.at[f], dev) for k, dev in enumerate(peers)]
    start(sums)
    wait_send((norm_zero, norm_one, norm_two, norm_three))

    def drain(slots, copies):
        def body(j, carry):
            on_plan(j, lambda *args: wait_send(copies(*args)))
            return carry
        lax.fori_loop(total - slots, total, body, 0)

    drain(P_SLOTS, ones)
    drain(R_SLOTS, lambda j, side, half: zero_copies(emb, 0, j))
    drain(SEND_SLOTS, lambda *args: twos(*args) + (two_c_even(*args), three_ab(*args), three_c(*args), four(*args, z)))

    def last(j, carry):
        out_copy(emb_out, 0, j).wait()
        return carry

    lax.fori_loop(total - SEND_SLOTS, total, last, 0)

    for k in range(1, 8):
        s = lax.rem(f + k, 8)
        remote(sum_send, sum_recv.at[s], sum_ssem.at[0], sum_rsem.at[s], core).wait_recv()
    whole = sum_recv[0]
    for k in range(1, 8):
        whole = whole + sum_recv[k]
    scale_out[...] = jnp.minimum(1.0, CLIP_NORM / jnp.sqrt(whole))
    wait_send(sums)


def reduce_grads(emb_grad, mat_grad, norm_grad):
    emb_rows = emb_grad.shape[0] // 8
    mat_rows = mat_grad.shape[0] // 8
    counts = (emb_rows // ROWS, mat_rows // ROWS)
    dma = pltpu.SemaphoreType.DMA
    scratch = [
        pltpu.VMEM((P_SLOTS, 2, 2, ROWS, WIDTH), F32),
        pltpu.VMEM((R_SLOTS, 2, 2, ROWS, WIDTH), F32),
        pltpu.VMEM((RING, 2, ROWS, SIDE_MAX), F32),
        pltpu.VMEM((RING, 2, ROWS, SIDE_MAX), F32),
        pltpu.VMEM((RING, 2, 2, ROWS, HALF_MAX), F32),
        pltpu.VMEM((RING, ROWS, 2 * SIDE_MAX), F32),
        pltpu.VMEM((RING, 2, ROWS, HALF_MAX), F32),
        pltpu.VMEM((RING, ROWS, HALF_MAX), F32),
        pltpu.VMEM((RING, ROWS, WIDTH), F32),
        pltpu.VMEM((ROWS, WIDTH), F32),
        pltpu.VMEM((NORM_ROWS, 1, WIDTH), F32),
        pltpu.VMEM((2, 2, 2) + NORM_PAD, F32),
        pltpu.VMEM((2, 2) + NORM_PAD, F32),
        pltpu.VMEM((2,) + NORM_PAD, F32),
        pltpu.VMEM(NORM_PAD, F32),
        pltpu.VMEM(NORM_PAD, F32),
        pltpu.VMEM((8, 128), F32),
        pltpu.VMEM((8, 8, 128), F32),
        dma((P_SLOTS,)), dma((2, R_SLOTS)), dma((2, R_SLOTS)), pltpu.SemaphoreType.REGULAR,
        dma((3, P_SLOTS)), dma((3, RING)), dma((3, SEND_SLOTS)), dma((3, RING)),
        dma((2, SEND_SLOTS)), dma((2, RING)), dma((SEND_SLOTS,)), dma((RING,)), dma((SEND_SLOTS,)),
        dma, dma((4,)), dma((4,)), dma((7,)), dma((8,)),
    ]
    hbm = pl.BlockSpec(memory_space=pl.ANY)
    vmem = pl.BlockSpec(memory_space=pltpu.VMEM)
    return pl.pallas_call(
        functools.partial(reduce_kernel, counts),
        out_shape=(
            jax.ShapeDtypeStruct((emb_rows, WIDTH), F32),
            jax.ShapeDtypeStruct((mat_rows, WIDTH), F32),
            jax.ShapeDtypeStruct(NORM_PAD, F32),
            jax.ShapeDtypeStruct((8, 128), F32),
        ),
        in_specs=[pl.BlockSpec(memory_space=pltpu.HBM)] * 3,
        out_specs=(hbm, hbm, vmem, vmem),
        scratch_shapes=scratch,
        compiler_params=pltpu.CompilerParams(
            collective_id=0, has_side_effects=True, vmem_limit_bytes=28 * 1024 * 1024
        ),
        name="reduce_grads",
    )(*(pltpu.with_memory_space_constraint(grad, pltpu.HBM) for grad in (
        emb_grad.reshape(2, 2, 2, emb_rows, WIDTH), mat_grad.reshape(2, 2, 2, mat_rows, WIDTH),
        norm_grad.reshape(NORM_ROWS, 1, WIDTH))))


BLOCK = 16
COLS = 384
SIDE = WIDTH // 2
STORE_SLOTS = 4


def adamw_block(grad, param, mom, var, decay_rate):
    new_mom = BETA_ONE * mom + (1.0 - BETA_ONE) * grad
    new_var = BETA_TWO * var + (1.0 - BETA_TWO) * grad * grad
    root = math.sqrt(1.0 - BETA_TWO ** ADAM_STEP)
    step_dir = new_mom / (jnp.sqrt(new_var) + ADAM_EPS * root)
    rate = LEARN_RATE * root / (1.0 - BETA_ONE ** ADAM_STEP)
    return param - (rate * step_dir + (LEARN_RATE * decay_rate) * param), new_mom, new_var


def adamw_kernel(scale, eg, ep, em, ev, mg, mp, mm, mv, ng, np_, nm, nv,
                 ep_out, em_out, ev_out, eb_out, mp_out, mm_out, mv_out, mb_out, np_out, nm_out, nv_out, nb_out,
                 p_buf, m_buf, v_buf, b_buf, n_bufs, nb_buf, sems, n_sems):
    clip = scale[0:1, 0:1]

    def copies(outs, slot, row, side):
        cols = pl.ds(side * SIDE, SIDE)
        return [pltpu.make_async_copy(buf.at[slot, side], out.at[pl.ds(row, BLOCK), cols], sems.at[k, slot, side])
                for k, (buf, out) in enumerate(zip((p_buf, m_buf, v_buf, b_buf), outs))]

    emb_outs = (ep_out, em_out, ev_out, eb_out)
    mat_outs = (mp_out, mm_out, mv_out, mb_out)
    emb_blocks = eg.shape[0] // BLOCK
    mat_blocks = mg.shape[0] // BLOCK

    def run(first, count, ins, outs):
        def body(i, carry):
            j = first + i
            slot = lax.rem(j, STORE_SLOTS)

            row = pl.multiple_of(i * BLOCK, BLOCK)
            for side in range(2):
                @pl.when(j >= STORE_SLOTS)
                def _():
                    for copy in copies(emb_outs, slot, 0, side):
                        copy.wait()

                for col in range(0, SIDE, COLS):
                    here, cols = pl.ds(col, COLS), pl.ds(side * SIDE + col, COLS)
                    g, p, m, v = (ref[pl.ds(row, BLOCK), cols] for ref in ins)
                    new_p, new_m, new_v = adamw_block(g * clip, p, m, v, WEIGHT_DECAY)
                    p_buf[slot, side, :, here] = new_p
                    m_buf[slot, side, :, here] = new_m
                    v_buf[slot, side, :, here] = new_v
                    b_buf[slot, side, :, here] = new_p.astype(jnp.bfloat16)
                for copy in copies(outs, slot, row, side):
                    copy.start()
            return carry

        lax.fori_loop(0, count, body, 0)

    run(0, emb_blocks, (eg, ep, em, ev), emb_outs)
    run(emb_blocks, mat_blocks, (mg, mp, mm, mv), mat_outs)
    new_p, new_m, new_v = adamw_block(ng[:NORM_ROWS, :NORM_COLS] * clip, np_[...], nm[...], nv[...], 0.0)
    for k, value in enumerate((new_p, new_m, new_v)):
        n_bufs[k] = value
    nb_buf[...] = new_p.astype(jnp.bfloat16)
    norm_copies = [pltpu.make_async_copy(n_bufs.at[k], out, n_sems.at[k]) for k, out in enumerate((np_out, nm_out, nv_out))]
    norm_copies.append(pltpu.make_async_copy(nb_buf, nb_out, n_sems.at[3]))
    for copy in norm_copies:
        copy.start()
    for slot in range(STORE_SLOTS):
        for side in range(2):
            for copy in copies(emb_outs, slot, 0, side):
                copy.wait()
    for copy in norm_copies:
        copy.wait()


def adamw(scale, emb, mat, norm):
    shapes = []
    for ref in (emb[1], mat[1], norm[1]):
        shapes += [jax.ShapeDtypeStruct(ref.shape, F32)] * 3 + [jax.ShapeDtypeStruct(ref.shape, jnp.bfloat16)]
    buf = (STORE_SLOTS, 2, BLOCK, SIDE)
    vmem = pl.BlockSpec(memory_space=pltpu.VMEM)
    hbm = pl.BlockSpec(memory_space=pl.ANY)
    elements = emb[1].size + mat[1].size
    return pl.pallas_call(
        adamw_kernel,
        out_shape=tuple(shapes),
        in_specs=[vmem] * 13,
        out_specs=(hbm,) * 12,
        scratch_shapes=[
            pltpu.VMEM(buf, F32), pltpu.VMEM(buf, F32), pltpu.VMEM(buf, F32), pltpu.VMEM(buf, jnp.bfloat16),
            pltpu.VMEM((3, NORM_ROWS, NORM_COLS), F32), pltpu.VMEM((NORM_ROWS, NORM_COLS), jnp.bfloat16),
            pltpu.SemaphoreType.DMA((4, STORE_SLOTS, 2)), pltpu.SemaphoreType.DMA((4,)),
        ],
        compiler_params=pltpu.CompilerParams(vmem_limit_bytes=8 * 1024 * 1024),
        cost_estimate=pl.CostEstimate(flops=20 * elements, bytes_accessed=30 * elements, transcendentals=2 * elements),
        name="adamw",
    )(scale, *emb, *mat, *norm)


def solution(mesh):
    def local_step(emb_grad, mat_grad, norm_grad, emb_param, emb_mom, emb_var, mat_param, mat_mom, mat_var, norm_param, norm_mom, norm_var):
        emb_mean, mat_mean, norm_mean, scale = reduce_grads(emb_grad[0, 0], mat_grad[0, 0], norm_grad[0, 0])
        return adamw(scale, (emb_mean, emb_param, emb_mom, emb_var), (mat_mean, mat_param, mat_mom, mat_var),
                     (norm_mean, norm_param, norm_mom, norm_var))

    grad_spec = P("dp", "fsdp", None, None)
    row_spec = P("fsdp", None)
    col_spec = P(None, "fsdp")
    in_list = (grad_spec, grad_spec, grad_spec, row_spec, row_spec, row_spec, row_spec, row_spec, row_spec, col_spec, col_spec, col_spec)
    out_list = (row_spec, row_spec, row_spec, row_spec, row_spec, row_spec, row_spec, row_spec, col_spec, col_spec, col_spec, col_spec)
    return jax.shard_map(local_step, mesh=mesh, in_specs=in_list, out_specs=out_list, check_vma=False)
```

```python
import functools
import math

import jax
import jax.numpy as jnp
from jax import lax
from jax.experimental import pallas as pl
from jax.experimental.pallas import tpu as pltpu
from jax.sharding import PartitionSpec as P

LEARN_RATE = 0.003
BETA_ONE = 0.9
BETA_TWO = 0.95
ADAM_EPS = 1e-8
WEIGHT_DECAY = 0.1
CLIP_NORM = 1.0
ADAM_STEP = 10

MESH = pl.DeviceIdType.MESH
F32 = jnp.float32

WIDTH = 5376
NORM_ROWS = 9
NORM_COLS = 672
NORM_PAD = (16, 768)
ROWS = 8
PLANS = ((1920, 768), (2176, 512))
INNER = (24, 44)
CUT = 2 * min(side for side, _ in PLANS)
SIDE_MAX = max(side for side, _ in PLANS)
HALF_MAX = max(half for _, half in PLANS)
LAG_ZERO = 0
LAG = 2
P_SLOTS = 10
R_SLOTS = 6
SEND_SLOTS = 8
RING = 16


def reduce_kernel(counts, emb, mat, norm, emb_out, mat_out, norm_out, scale_out,
                  part, recv_zero, xa, yb, zc, mid, wc, tc, grad, square,
                  norm_in, norm_part, norm_a, norm_b, norm_c, norm_d, sum_send, sum_recv,
                  load_sem, zero_send, zero_recv, credit,
                  one_send, one_recv, two_send, two_recv, three_send, three_recv, four_send, four_recv, out_sem,
                  norm_load, norm_send, norm_recv, sum_ssem, sum_rsem):
    emb_count, mat_count = counts
    total = emb_count + mat_count
    z = lax.axis_index("dp")
    f = lax.axis_index("fsdp")
    c = lax.rem(f, 2)
    x = lax.rem(lax.div(f, 2), 2)
    y = lax.div(f, 4)
    core = (z, f + 1 - 2 * c)
    xn = (z, f + 2 - 4 * x)
    yn = (z, f + 4 - 8 * y)
    zn = (1 - z, f)
    peers = [(z, lax.rem(f + k, 8)) for k in range(1, 8)]

    def remote(src, dst, ssem, rsem, dev):
        return pltpu.make_async_remote_copy(src_ref=src, dst_ref=dst, send_sem=ssem, recv_sem=rsem,
                                            device_id=dev, device_id_type=MESH)

    def on_plan(j, body):
        inner = jnp.logical_and(j >= INNER[0], j < INNER[1])
        pl.when(jnp.logical_not(inner))(lambda: body(j, *PLANS[0]))
        pl.when(inner)(lambda: body(j, *PLANS[1]))

    def half_at(side, half, which):
        return pl.ds(pl.multiple_of(2 * side + which * half, 128), half)

    barrier = pltpu.get_barrier_semaphore()
    for dev in (core, xn, yn, zn):
        pl.semaphore_signal(barrier, inc=1, device_id=dev, device_id_type=MESH)
    norm_copy = pltpu.make_async_copy(norm, norm_in, norm_load)
    norm_copy.start()

    def on_rows(j, body):
        @pl.when(j < emb_count)
        def _():
            body(emb, emb_out, pl.multiple_of(j * ROWS, ROWS))

        @pl.when(j >= emb_count)
        def _():
            body(mat, mat_out, pl.multiple_of((j - emb_count) * ROWS, ROWS))

    def load_copy(ref, row, j):
        s = lax.rem(j, P_SLOTS)
        return pltpu.make_async_copy(ref.at[:, :, c, pl.ds(row, ROWS), :], part.at[s], load_sem.at[s])

    def exchange(source, s):
        return [remote(source.at[:, :, :, cols], recv_zero.at[s, :, :, :, cols], zero_send.at[k, s], zero_recv.at[k, s], core)
                for k, cols in enumerate((pl.ds(CUT, WIDTH - CUT), pl.ds(0, CUT)))]

    def zero_copies(ref, row, j):
        return exchange(ref.at[:, :, 1 - c, pl.ds(row, ROWS)], lax.rem(j, R_SLOTS))

    def ones(j, side, half):
        s, r = lax.rem(j, P_SLOTS), lax.rem(j, RING)
        return (remote(part.at[s, :, :, :, half_at(side, half, 1 - z)], zc.at[r, :, :, :, :half], one_send.at[2, s], one_recv.at[2, r], zn),
                remote(part.at[s, :, 1 - x, :, :side], xa.at[r, :, :, :side], one_send.at[0, s], one_recv.at[0, r], xn),
                remote(part.at[s, 1 - y, :, :, side:2 * side], yb.at[r, :, :, :side], one_send.at[1, s], one_recv.at[1, r], yn))

    def two_c_even(j, side, half):
        s, r = lax.rem(j, SEND_SLOTS), lax.rem(j, RING)
        return remote(zc.at[r, :, 1 - x, :, :half], wc.at[r, :, :, :half], two_send.at[2, s], two_recv.at[2, r], xn)

    def two_c_odd(j, side, half):
        s, r = lax.rem(j, SEND_SLOTS), lax.rem(j, RING)
        return remote(zc.at[r, 1 - y, :, :, :half], wc.at[r, :, :, :half], two_send.at[2, s], two_recv.at[2, r], yn)

    def twos(j, side, half):
        s, r = lax.rem(j, SEND_SLOTS), lax.rem(j, RING)
        return (remote(xa.at[r, 1 - y, :, :side], mid.at[r, :, :side], two_send.at[0, s], two_recv.at[0, r], yn),
                remote(yb.at[r, 1 - x, :, :side], mid.at[r, :, side:2 * side], two_send.at[1, s], two_recv.at[1, r], xn))

    def three_c(j, side, half):
        s, r, odd = lax.rem(j, SEND_SLOTS), lax.rem(j, RING), lax.rem(j, 2)
        here = y + odd * (x - y)
        step = (4 - 8 * y) + odd * ((2 - 4 * x) - (4 - 8 * y))
        return remote(wc.at[r, 1 - here, :, :half], tc.at[r, :, :half], three_send.at[1, s], three_recv.at[1, r], (z, f + step))

    def three_ab(j, side, half):
        s, r = lax.rem(j, SEND_SLOTS), lax.rem(j, RING)
        return remote(mid.at[r, :, :2 * side], grad.at[r, :, :2 * side], three_send.at[0, s], three_recv.at[0, r], zn)

    def four(j, side, half, which):
        s, r = lax.rem(j, SEND_SLOTS), lax.rem(j, RING)
        cols = half_at(side, half, which)
        return remote(grad.at[r, :, cols], grad.at[r, :, cols], four_send.at[s], four_recv.at[r], zn)

    def out_copy(ref, row, j):
        return pltpu.make_async_copy(grad.at[lax.rem(j, RING)], ref.at[pl.ds(row, ROWS), :],
                                     out_sem.at[lax.rem(j, SEND_SLOTS)])

    norm_zero = remote(norm_part.at[:, :, 1 - c], norm_a, norm_send.at[0], norm_recv.at[0], core)
    norm_one = remote(norm_a.at[:, 1 - x], norm_b, norm_send.at[1], norm_recv.at[1], xn)
    norm_two = remote(norm_b.at[1 - y], norm_c, norm_send.at[2], norm_recv.at[2], yn)
    norm_three = remote(norm_c, norm_d, norm_send.at[3], norm_recv.at[3], zn)

    def when_in(j, body):
        pl.when(jnp.logical_and(j >= 0, j < total))(functools.partial(body, j))

    def after(j, slots, copies):
        @pl.when(j >= slots)
        def _():
            on_plan(j - slots, lambda *args: wait_send(copies(*args)))

    def start(copies):
        for copy in copies:
            copy.start()

    def wait_send(copies):
        for copy in copies:
            copy.wait_send()

    def stage_issue(j):
        after(j, P_SLOTS, ones)

        @pl.when(j >= R_SLOTS)
        def _():
            wait_send(zero_copies(emb, 0, j - R_SLOTS))
            pl.semaphore_wait(credit, 1)

        def body(ref, _, row):
            start(zero_copies(ref, row, j))
            load_copy(ref, row, j).start()

        on_rows(j, body)

    def stage_one(j):
        load_copy(emb, 0, j).wait()
        zero_copies(emb, 0, j)[0].wait_recv()
        part[lax.rem(j, P_SLOTS), :, :, :, CUT:] += recv_zero[lax.rem(j, R_SLOTS), :, :, :, CUT:]
        on_plan(j, lambda *args: start(ones(*args)[:1]))

    def stage_one_more(j):
        zero_copies(emb, 0, j)[1].wait_recv()
        part[lax.rem(j, P_SLOTS), :, :, :, :CUT] += recv_zero[lax.rem(j, R_SLOTS), :, :, :, :CUT]

        @pl.when(j + R_SLOTS < total)
        def _():
            pl.semaphore_signal(credit, inc=1, device_id=core, device_id_type=MESH)

        on_plan(j, lambda *args: start(ones(*args)[1:]))

    def stage_two(j):
        after(j, SEND_SLOTS, lambda *args: twos(*args) + (two_c_even(*args),))

        def body(j, side, half):
            s, r = lax.rem(j, P_SLOTS), lax.rem(j, RING)
            even = lax.rem(j, 2) == 0
            for copy in ones(j, side, half):
                copy.wait_recv()
            zc[r, :, :, :, :half] += part[s, :, :, :, half_at(side, half, z)]
            xa[r, :, :, :side] += part[s, :, x, :, :side]
            yb[r, :, :, :side] += part[s, y, :, :, side:2 * side]
            pl.when(even)(lambda: two_c_even(j, side, half).start())
            pl.when(jnp.logical_not(even))(lambda: two_c_odd(j, side, half).start())
            start(twos(j, side, half))

        on_plan(j, body)

    def stage_three(j):
        after(j, SEND_SLOTS, lambda *args: (three_ab(*args), three_c(*args)))

        def body(j, side, half):
            r = lax.rem(j, RING)
            even = lax.rem(j, 2) == 0
            for copy in twos(j, side, half) + (two_c_even(j, side, half),):
                copy.wait_recv()

            @pl.when(even)
            def _():
                wc[r, :, :, :half] += zc[r, :, x, :, :half]

            @pl.when(jnp.logical_not(even))
            def _():
                wc[r, :, :, :half] += zc[r, y, :, :, :half]

            mid[r, :, :side] += xa[r, y, :, :side]
            mid[r, :, side:2 * side] += yb[r, x, :, :side]
            start((three_c(j, side, half), three_ab(j, side, half)))

        on_plan(j, body)

    def stage_four(j):
        after(j, SEND_SLOTS, lambda *args: (four(*args, z),))

        def body(j, side, half):
            r, odd = lax.rem(j, RING), lax.rem(j, 2)
            here = y + odd * (x - y)
            three_c(j, side, half).wait_recv()
            grad[r, :, half_at(side, half, z)] = (tc[r, :, :half] + wc[r, here, :, :half]) * (1.0 / 16.0)
            four(j, side, half, z).start()

        on_plan(j, body)

    def stage_five(j):
        def body(j, side, half):
            r = lax.rem(j, RING)
            three_ab(j, side, half).wait_recv()
            both = (grad[r, :, :2 * side] + mid[r, :, :2 * side]) * (1.0 / 16.0)
            grad[r, :, :2 * side] = both
            square[:, :2 * side] += both * both
            four(j, side, half, 1 - z).wait_recv()
            rest = grad[r, :, 2 * side:]
            square[:, 2 * side:] += rest * rest

        on_plan(j, body)

        @pl.when(j >= SEND_SLOTS)
        def _():
            out_copy(emb_out, 0, j - SEND_SLOTS).wait()

        def store(_, ref, row):
            out_copy(ref, row, j).start()

        on_rows(j, store)

    def trip(it, carry):
        when_in(it + 1, stage_issue)
        when_in(it - LAG_ZERO, stage_one)
        when_in(it - LAG_ZERO - 4 * LAG, stage_five)
        when_in(it - LAG_ZERO - 3 * LAG, stage_four)
        when_in(it - LAG_ZERO - 2 * LAG, stage_three)
        when_in(it - LAG_ZERO - LAG, stage_two)
        when_in(it - LAG_ZERO, stage_one_more)

        @pl.when(it == 5)
        def _():
            norm_copy.wait()
            for k in range(8):
                for row in range(NORM_ROWS):
                    norm_part[k // 4, (k // 2) % 2, k % 2, row:row + 1, :NORM_COLS] = norm_in[row, :, k * NORM_COLS:(k + 1) * NORM_COLS]
            norm_zero.start()

        @pl.when(it == 8)
        def _():
            norm_zero.wait_recv()
            norm_a[...] += norm_part[:, :, c]
            norm_one.start()

        @pl.when(it == 12)
        def _():
            norm_one.wait_recv()
            norm_b[...] += norm_a[:, x]
            norm_two.start()

        @pl.when(it == 16)
        def _():
            norm_two.wait_recv()
            norm_c[...] += norm_b[y]
            norm_three.start()

        @pl.when(it == 20)
        def _():
            norm_three.wait_recv()
            norm_d[...] = (norm_d[...] + norm_c[...]) * (1.0 / 16.0)
            norm_out[...] = norm_d[...]
            norm_sq = norm_d[...] * norm_d[...]
            square[:, :NORM_PAD[1]] += norm_sq[:ROWS] + norm_sq[ROWS:]

        return carry

    ahead = pltpu.make_async_copy(emb.at[:, :, 1 - c, pl.ds(0, ROWS), :], part.at[P_SLOTS - 1], load_sem.at[P_SLOTS - 1])
    ahead.start()
    load_copy(emb, 0, 0).start()
    norm_part[...] = jnp.zeros_like(norm_part)
    square[...] = jnp.zeros_like(square)
    ahead.wait()
    pl.semaphore_wait(barrier, 4)
    start(exchange(part.at[P_SLOTS - 1], 0))
    lax.fori_loop(0, total + LAG_ZERO + 4 * LAG, trip, 0)

    value = jnp.full((8, 128), jnp.sum(square[...]), F32)
    sum_send[...] = value
    sum_recv[f] = value
    sums = [remote(sum_send, sum_recv.at[f], sum_ssem.at[k], sum_rsem.at[f], dev) for k, dev in enumerate(peers)]
    start(sums)
    wait_send((norm_zero, norm_one, norm_two, norm_three))

    def drain(slots, copies):
        def body(j, carry):
            on_plan(j, lambda *args: wait_send(copies(*args)))
            return carry
        lax.fori_loop(total - slots, total, body, 0)

    drain(P_SLOTS, ones)
    drain(R_SLOTS, lambda j, side, half: zero_copies(emb, 0, j))
    drain(SEND_SLOTS, lambda *args: twos(*args) + (two_c_even(*args), three_ab(*args), three_c(*args), four(*args, z)))

    def last(j, carry):
        out_copy(emb_out, 0, j).wait()
        return carry

    lax.fori_loop(total - SEND_SLOTS, total, last, 0)

    for k in range(1, 8):
        s = lax.rem(f + k, 8)
        remote(sum_send, sum_recv.at[s], sum_ssem.at[0], sum_rsem.at[s], core).wait_recv()
    whole = sum_recv[0]
    for k in range(1, 8):
        whole = whole + sum_recv[k]
    scale_out[...] = jnp.minimum(1.0, CLIP_NORM / jnp.sqrt(whole))
    wait_send(sums)


def reduce_grads(emb_grad, mat_grad, norm_grad):
    emb_rows = emb_grad.shape[0] // 8
    mat_rows = mat_grad.shape[0] // 8
    counts = (emb_rows // ROWS, mat_rows // ROWS)
    dma = pltpu.SemaphoreType.DMA
    scratch = [
        pltpu.VMEM((P_SLOTS, 2, 2, ROWS, WIDTH), F32),
        pltpu.VMEM((R_SLOTS, 2, 2, ROWS, WIDTH), F32),
        pltpu.VMEM((RING, 2, ROWS, SIDE_MAX), F32),
        pltpu.VMEM((RING, 2, ROWS, SIDE_MAX), F32),
        pltpu.VMEM((RING, 2, 2, ROWS, HALF_MAX), F32),
        pltpu.VMEM((RING, ROWS, 2 * SIDE_MAX), F32),
        pltpu.VMEM((RING, 2, ROWS, HALF_MAX), F32),
        pltpu.VMEM((RING, ROWS, HALF_MAX), F32),
        pltpu.VMEM((RING, ROWS, WIDTH), F32),
        pltpu.VMEM((ROWS, WIDTH), F32),
        pltpu.VMEM((NORM_ROWS, 1, WIDTH), F32),
        pltpu.VMEM((2, 2, 2) + NORM_PAD, F32),
        pltpu.VMEM((2, 2) + NORM_PAD, F32),
        pltpu.VMEM((2,) + NORM_PAD, F32),
        pltpu.VMEM(NORM_PAD, F32),
        pltpu.VMEM(NORM_PAD, F32),
        pltpu.VMEM((8, 128), F32),
        pltpu.VMEM((8, 8, 128), F32),
        dma((P_SLOTS,)), dma((2, R_SLOTS)), dma((2, R_SLOTS)), pltpu.SemaphoreType.REGULAR,
        dma((3, P_SLOTS)), dma((3, RING)), dma((3, SEND_SLOTS)), dma((3, RING)),
        dma((2, SEND_SLOTS)), dma((2, RING)), dma((SEND_SLOTS,)), dma((RING,)), dma((SEND_SLOTS,)),
        dma, dma((4,)), dma((4,)), dma((7,)), dma((8,)),
    ]
    hbm = pl.BlockSpec(memory_space=pl.ANY)
    vmem = pl.BlockSpec(memory_space=pltpu.VMEM)
    return pl.pallas_call(
        functools.partial(reduce_kernel, counts),
        out_shape=(
            jax.ShapeDtypeStruct((emb_rows, WIDTH), F32),
            jax.ShapeDtypeStruct((mat_rows, WIDTH), F32),
            jax.ShapeDtypeStruct(NORM_PAD, F32),
            jax.ShapeDtypeStruct((8, 128), F32),
        ),
        in_specs=[pl.BlockSpec(memory_space=pltpu.HBM)] * 3,
        out_specs=(hbm, hbm, vmem, vmem),
        scratch_shapes=scratch,
        compiler_params=pltpu.CompilerParams(
            collective_id=0, has_side_effects=True, vmem_limit_bytes=28 * 1024 * 1024
        ),
        name="reduce_grads",
    )(*(pltpu.with_memory_space_constraint(grad, pltpu.HBM) for grad in (
        emb_grad.reshape(2, 2, 2, emb_rows, WIDTH), mat_grad.reshape(2, 2, 2, mat_rows, WIDTH),
        norm_grad.reshape(NORM_ROWS, 1, WIDTH))))


BLOCK = 16
COLS = 384
SIDE = WIDTH // 2
STORE_SLOTS = 4


def adamw_block(grad, param, mom, var, decay_rate):
    new_mom = BETA_ONE * mom + (1.0 - BETA_ONE) * grad
    new_var = BETA_TWO * var + (1.0 - BETA_TWO) * grad * grad
    root = math.sqrt(1.0 - BETA_TWO ** ADAM_STEP)
    step_dir = new_mom / (jnp.sqrt(new_var) + ADAM_EPS * root)
    rate = LEARN_RATE * root / (1.0 - BETA_ONE ** ADAM_STEP)
    return param - (rate * step_dir + (LEARN_RATE * decay_rate) * param), new_mom, new_var


def adamw_kernel(scale, eg, ep, em, ev, mg, mp, mm, mv, ng, np_, nm, nv,
                 ep_out, em_out, ev_out, eb_out, mp_out, mm_out, mv_out, mb_out, np_out, nm_out, nv_out, nb_out,
                 p_buf, m_buf, v_buf, b_buf, n_bufs, nb_buf, sems, n_sems):
    clip = scale[0:1, 0:1]

    def copies(outs, slot, row, side):
        cols = pl.ds(side * SIDE, SIDE)
        return [pltpu.make_async_copy(buf.at[slot, side], out.at[pl.ds(row, BLOCK), cols], sems.at[k, slot, side])
                for k, (buf, out) in enumerate(zip((p_buf, m_buf, v_buf, b_buf), outs))]

    emb_outs = (ep_out, em_out, ev_out, eb_out)
    mat_outs = (mp_out, mm_out, mv_out, mb_out)
    emb_blocks = eg.shape[0] // BLOCK
    mat_blocks = mg.shape[0] // BLOCK

    def run(first, count, ins, outs):
        def body(i, carry):
            j = first + i
            slot = lax.rem(j, STORE_SLOTS)

            row = pl.multiple_of(i * BLOCK, BLOCK)
            for side in range(2):
                @pl.when(j >= STORE_SLOTS)
                def _():
                    for copy in copies(emb_outs, slot, 0, side):
                        copy.wait()

                for col in range(0, SIDE, COLS):
                    here, cols = pl.ds(col, COLS), pl.ds(side * SIDE + col, COLS)
                    g, p, m, v = (ref[pl.ds(row, BLOCK), cols] for ref in ins)
                    new_p, new_m, new_v = adamw_block(g * clip, p, m, v, WEIGHT_DECAY)
                    p_buf[slot, side, :, here] = new_p
                    m_buf[slot, side, :, here] = new_m
                    v_buf[slot, side, :, here] = new_v
                    b_buf[slot, side, :, here] = new_p.astype(jnp.bfloat16)
                for copy in copies(outs, slot, row, side):
                    copy.start()
            return carry

        lax.fori_loop(0, count, body, 0)

    run(0, emb_blocks, (eg, ep, em, ev), emb_outs)
    run(emb_blocks, mat_blocks, (mg, mp, mm, mv), mat_outs)
    new_p, new_m, new_v = adamw_block(ng[:NORM_ROWS, :NORM_COLS] * clip, np_[...], nm[...], nv[...], 0.0)
    for k, value in enumerate((new_p, new_m, new_v)):
        n_bufs[k] = value
    nb_buf[...] = new_p.astype(jnp.bfloat16)
    norm_copies = [pltpu.make_async_copy(n_bufs.at[k], out, n_sems.at[k]) for k, out in enumerate((np_out, nm_out, nv_out))]
    norm_copies.append(pltpu.make_async_copy(nb_buf, nb_out, n_sems.at[3]))
    for copy in norm_copies:
        copy.start()
    for slot in range(STORE_SLOTS):
        for side in range(2):
            for copy in copies(emb_outs, slot, 0, side):
                copy.wait()
    for copy in norm_copies:
        copy.wait()


def adamw(scale, emb, mat, norm):
    shapes = []
    for ref in (emb[1], mat[1], norm[1]):
        shapes += [jax.ShapeDtypeStruct(ref.shape, F32)] * 3 + [jax.ShapeDtypeStruct(ref.shape, jnp.bfloat16)]
    buf = (STORE_SLOTS, 2, BLOCK, SIDE)
    vmem = pl.BlockSpec(memory_space=pltpu.VMEM)
    hbm = pl.BlockSpec(memory_space=pl.ANY)
    elements = emb[1].size + mat[1].size
    return pl.pallas_call(
        adamw_kernel,
        out_shape=tuple(shapes),
        in_specs=[vmem] * 13,
        out_specs=(hbm,) * 12,
        scratch_shapes=[
            pltpu.VMEM(buf, F32), pltpu.VMEM(buf, F32), pltpu.VMEM(buf, F32), pltpu.VMEM(buf, jnp.bfloat16),
            pltpu.VMEM((3, NORM_ROWS, NORM_COLS), F32), pltpu.VMEM((NORM_ROWS, NORM_COLS), jnp.bfloat16),
            pltpu.SemaphoreType.DMA((4, STORE_SLOTS, 2)), pltpu.SemaphoreType.DMA((4,)),
        ],
        compiler_params=pltpu.CompilerParams(vmem_limit_bytes=8 * 1024 * 1024),
        cost_estimate=pl.CostEstimate(flops=20 * elements, bytes_accessed=30 * elements, transcendentals=2 * elements),
        name="adamw",
    )(scale, *emb, *mat, *norm)


def solution(mesh):
    def local_step(emb_grad, mat_grad, norm_grad, emb_param, emb_mom, emb_var, mat_param, mat_mom, mat_var, norm_param, norm_mom, norm_var):
        emb_mean, mat_mean, norm_mean, scale = reduce_grads(emb_grad[0, 0], mat_grad[0, 0], norm_grad[0, 0])
        return adamw(scale, (emb_mean, emb_param, emb_mom, emb_var), (mat_mean, mat_param, mat_mom, mat_var),
                     (norm_mean, norm_param, norm_mom, norm_var))

    grad_spec = P("dp", "fsdp", None, None)
    row_spec = P("fsdp", None)
    col_spec = P(None, "fsdp")
    in_list = (grad_spec, grad_spec, grad_spec, row_spec, row_spec, row_spec, row_spec, row_spec, row_spec, col_spec, col_spec, col_spec)
    out_list = (row_spec, row_spec, row_spec, row_spec, row_spec, row_spec, row_spec, row_spec, col_spec, col_spec, col_spec, col_spec)
    return jax.shard_map(local_step, mesh=mesh, in_specs=in_list, out_specs=out_list, check_vma=False)
```

```python
import functools
import math

import jax
import jax.numpy as jnp
from jax import lax
from jax.experimental import pallas as pl
from jax.experimental.pallas import tpu as pltpu
from jax.sharding import PartitionSpec as P

LEARN_RATE = 0.003
BETA_ONE = 0.9
BETA_TWO = 0.95
ADAM_EPS = 1e-8
WEIGHT_DECAY = 0.1
CLIP_NORM = 1.0
ADAM_STEP = 10

MESH = pl.DeviceIdType.MESH
F32 = jnp.float32

WIDTH = 5376
NORM_ROWS = 9
NORM_COLS = 672
NORM_PAD = (16, 768)
ROWS = 8
PLANS = ((1792, 896), (2176, 512))
INNER = (14, 46)
CUT = 2 * min(side for side, _ in PLANS)
SIDE_MAX = max(side for side, _ in PLANS)
HALF_MAX = max(half for _, half in PLANS)
LAG_ZERO = 0
LAG = 2
P_SLOTS = 10
R_SLOTS = 6
SEND_SLOTS = 8
RING = 16


def reduce_kernel(counts, emb, mat, norm, emb_out, mat_out, norm_out, scale_out,
                  part, recv_zero, xa, yb, zc, mid, wc, tc, grad, square,
                  norm_in, norm_part, norm_a, norm_b, norm_c, norm_d, sum_send, sum_recv,
                  load_sem, zero_send, zero_recv, credit,
                  one_send, one_recv, two_send, two_recv, three_send, three_recv, four_send, four_recv, out_sem,
                  norm_load, norm_send, norm_recv, sum_ssem, sum_rsem):
    emb_count, mat_count = counts
    total = emb_count + mat_count
    z = lax.axis_index("dp")
    f = lax.axis_index("fsdp")
    c = lax.rem(f, 2)
    x = lax.rem(lax.div(f, 2), 2)
    y = lax.div(f, 4)
    core = (z, f + 1 - 2 * c)
    xn = (z, f + 2 - 4 * x)
    yn = (z, f + 4 - 8 * y)
    zn = (1 - z, f)
    peers = [(z, lax.rem(f + k, 8)) for k in range(1, 8)]

    def remote(src, dst, ssem, rsem, dev):
        return pltpu.make_async_remote_copy(src_ref=src, dst_ref=dst, send_sem=ssem, recv_sem=rsem,
                                            device_id=dev, device_id_type=MESH)

    def on_plan(j, body):
        inner = jnp.logical_and(j >= INNER[0], j < INNER[1])
        pl.when(jnp.logical_not(inner))(lambda: body(j, *PLANS[0]))
        pl.when(inner)(lambda: body(j, *PLANS[1]))

    def half_at(side, half, which):
        return pl.ds(pl.multiple_of(2 * side + which * half, 128), half)

    barrier = pltpu.get_barrier_semaphore()
    for dev in (core, xn, yn, zn):
        pl.semaphore_signal(barrier, inc=1, device_id=dev, device_id_type=MESH)
    norm_copy = pltpu.make_async_copy(norm, norm_in, norm_load)
    norm_copy.start()

    def on_rows(j, body):
        @pl.when(j < emb_count)
        def _():
            body(emb, emb_out, pl.multiple_of(j * ROWS, ROWS))

        @pl.when(j >= emb_count)
        def _():
            body(mat, mat_out, pl.multiple_of((j - emb_count) * ROWS, ROWS))

    def load_copy(ref, row, j):
        s = lax.rem(j, P_SLOTS)
        return pltpu.make_async_copy(ref.at[:, :, c, pl.ds(row, ROWS), :], part.at[s], load_sem.at[s])

    def exchange(source, s):
        return [remote(source.at[:, :, :, cols], recv_zero.at[s, :, :, :, cols], zero_send.at[k, s], zero_recv.at[k, s], core)
                for k, cols in enumerate((pl.ds(CUT, WIDTH - CUT), pl.ds(0, CUT)))]

    def zero_copies(ref, row, j):
        return exchange(ref.at[:, :, 1 - c, pl.ds(row, ROWS)], lax.rem(j, R_SLOTS))

    def ones(j, side, half):
        s, r = lax.rem(j, P_SLOTS), lax.rem(j, RING)
        return (remote(part.at[s, :, :, :, half_at(side, half, 1 - z)], zc.at[r, :, :, :, :half], one_send.at[2, s], one_recv.at[2, r], zn),
                remote(part.at[s, :, 1 - x, :, :side], xa.at[r, :, :, :side], one_send.at[0, s], one_recv.at[0, r], xn),
                remote(part.at[s, 1 - y, :, :, side:2 * side], yb.at[r, :, :, :side], one_send.at[1, s], one_recv.at[1, r], yn))

    def two_c_even(j, side, half):
        s, r = lax.rem(j, SEND_SLOTS), lax.rem(j, RING)
        return remote(zc.at[r, :, 1 - x, :, :half], wc.at[r, :, :, :half], two_send.at[2, s], two_recv.at[2, r], xn)

    def two_c_odd(j, side, half):
        s, r = lax.rem(j, SEND_SLOTS), lax.rem(j, RING)
        return remote(zc.at[r, 1 - y, :, :, :half], wc.at[r, :, :, :half], two_send.at[2, s], two_recv.at[2, r], yn)

    def twos(j, side, half):
        s, r = lax.rem(j, SEND_SLOTS), lax.rem(j, RING)
        return (remote(xa.at[r, 1 - y, :, :side], mid.at[r, :, :side], two_send.at[0, s], two_recv.at[0, r], yn),
                remote(yb.at[r, 1 - x, :, :side], mid.at[r, :, side:2 * side], two_send.at[1, s], two_recv.at[1, r], xn))

    def three_c(j, side, half):
        s, r, odd = lax.rem(j, SEND_SLOTS), lax.rem(j, RING), lax.rem(j, 2)
        here = y + odd * (x - y)
        step = (4 - 8 * y) + odd * ((2 - 4 * x) - (4 - 8 * y))
        return remote(wc.at[r, 1 - here, :, :half], tc.at[r, :, :half], three_send.at[1, s], three_recv.at[1, r], (z, f + step))

    def three_ab(j, side, half):
        s, r = lax.rem(j, SEND_SLOTS), lax.rem(j, RING)
        return remote(mid.at[r, :, :2 * side], grad.at[r, :, :2 * side], three_send.at[0, s], three_recv.at[0, r], zn)

    def four(j, side, half, which):
        s, r = lax.rem(j, SEND_SLOTS), lax.rem(j, RING)
        cols = half_at(side, half, which)
        return remote(grad.at[r, :, cols], grad.at[r, :, cols], four_send.at[s], four_recv.at[r], zn)

    def out_copy(ref, row, j):
        return pltpu.make_async_copy(grad.at[lax.rem(j, RING)], ref.at[pl.ds(row, ROWS), :],
                                     out_sem.at[lax.rem(j, SEND_SLOTS)])

    norm_zero = remote(norm_part.at[:, :, 1 - c], norm_a, norm_send.at[0], norm_recv.at[0], core)
    norm_one = remote(norm_a.at[:, 1 - x], norm_b, norm_send.at[1], norm_recv.at[1], xn)
    norm_two = remote(norm_b.at[1 - y], norm_c, norm_send.at[2], norm_recv.at[2], yn)
    norm_three = remote(norm_c, norm_d, norm_send.at[3], norm_recv.at[3], zn)

    def when_in(j, body):
        pl.when(jnp.logical_and(j >= 0, j < total))(functools.partial(body, j))

    def after(j, slots, copies):
        @pl.when(j >= slots)
        def _():
            on_plan(j - slots, lambda *args: wait_send(copies(*args)))

    def start(copies):
        for copy in copies:
            copy.start()

    def wait_send(copies):
        for copy in copies:
            copy.wait_send()

    def stage_issue(j):
        after(j, P_SLOTS, ones)

        @pl.when(j >= R_SLOTS)
        def _():
            wait_send(zero_copies(emb, 0, j - R_SLOTS))
            pl.semaphore_wait(credit, 1)

        def body(ref, _, row):
            start(zero_copies(ref, row, j))
            load_copy(ref, row, j).start()

        on_rows(j, body)

    def stage_one(j):
        load_copy(emb, 0, j).wait()
        zero_copies(emb, 0, j)[0].wait_recv()
        part[lax.rem(j, P_SLOTS), :, :, :, CUT:] += recv_zero[lax.rem(j, R_SLOTS), :, :, :, CUT:]
        on_plan(j, lambda *args: start(ones(*args)[:1]))

    def stage_one_more(j):
        zero_copies(emb, 0, j)[1].wait_recv()
        part[lax.rem(j, P_SLOTS), :, :, :, :CUT] += recv_zero[lax.rem(j, R_SLOTS), :, :, :, :CUT]

        @pl.when(j + R_SLOTS < total)
        def _():
            pl.semaphore_signal(credit, inc=1, device_id=core, device_id_type=MESH)

        on_plan(j, lambda *args: start(ones(*args)[1:]))

    def stage_two(j):
        after(j, SEND_SLOTS, lambda *args: twos(*args) + (two_c_even(*args),))

        def body(j, side, half):
            s, r = lax.rem(j, P_SLOTS), lax.rem(j, RING)
            even = lax.rem(j, 2) == 0
            for copy in ones(j, side, half):
                copy.wait_recv()
            zc[r, :, :, :, :half] += part[s, :, :, :, half_at(side, half, z)]
            xa[r, :, :, :side] += part[s, :, x, :, :side]
            yb[r, :, :, :side] += part[s, y, :, :, side:2 * side]
            pl.when(even)(lambda: two_c_even(j, side, half).start())
            pl.when(jnp.logical_not(even))(lambda: two_c_odd(j, side, half).start())
            start(twos(j, side, half))

        on_plan(j, body)

    def stage_three(j):
        after(j, SEND_SLOTS, lambda *args: (three_ab(*args), three_c(*args)))

        def body(j, side, half):
            r = lax.rem(j, RING)
            even = lax.rem(j, 2) == 0
            for copy in twos(j, side, half) + (two_c_even(j, side, half),):
                copy.wait_recv()

            @pl.when(even)
            def _():
                wc[r, :, :, :half] += zc[r, :, x, :, :half]

            @pl.when(jnp.logical_not(even))
            def _():
                wc[r, :, :, :half] += zc[r, y, :, :, :half]

            mid[r, :, :side] += xa[r, y, :, :side]
            mid[r, :, side:2 * side] += yb[r, x, :, :side]
            start((three_c(j, side, half), three_ab(j, side, half)))

        on_plan(j, body)

    def stage_four(j):
        after(j, SEND_SLOTS, lambda *args: (four(*args, z),))

        def body(j, side, half):
            r, odd = lax.rem(j, RING), lax.rem(j, 2)
            here = y + odd * (x - y)
            three_c(j, side, half).wait_recv()
            grad[r, :, half_at(side, half, z)] = (tc[r, :, :half] + wc[r, here, :, :half]) * (1.0 / 16.0)
            four(j, side, half, z).start()

        on_plan(j, body)

    def stage_five(j):
        def body(j, side, half):
            r = lax.rem(j, RING)
            three_ab(j, side, half).wait_recv()
            both = (grad[r, :, :2 * side] + mid[r, :, :2 * side]) * (1.0 / 16.0)
            grad[r, :, :2 * side] = both
            square[:, :2 * side] += both * both
            four(j, side, half, 1 - z).wait_recv()
            rest = grad[r, :, 2 * side:]
            square[:, 2 * side:] += rest * rest

        on_plan(j, body)

        @pl.when(j >= SEND_SLOTS)
        def _():
            out_copy(emb_out, 0, j - SEND_SLOTS).wait()

        def store(_, ref, row):
            out_copy(ref, row, j).start()

        on_rows(j, store)

    def trip(it, carry):
        when_in(it + 1, stage_issue)
        when_in(it - LAG_ZERO, stage_one)
        when_in(it - LAG_ZERO - 4 * LAG, stage_five)
        when_in(it - LAG_ZERO - 3 * LAG, stage_four)
        when_in(it - LAG_ZERO - 2 * LAG, stage_three)
        when_in(it - LAG_ZERO - LAG, stage_two)
        when_in(it - LAG_ZERO, stage_one_more)

        @pl.when(it == 5)
        def _():
            norm_copy.wait()
            for k in range(8):
                for row in range(NORM_ROWS):
                    norm_part[k // 4, (k // 2) % 2, k % 2, row:row + 1, :NORM_COLS] = norm_in[row, :, k * NORM_COLS:(k + 1) * NORM_COLS]
            norm_zero.start()

        @pl.when(it == 8)
        def _():
            norm_zero.wait_recv()
            norm_a[...] += norm_part[:, :, c]
            norm_one.start()

        @pl.when(it == 12)
        def _():
            norm_one.wait_recv()
            norm_b[...] += norm_a[:, x]
            norm_two.start()

        @pl.when(it == 16)
        def _():
            norm_two.wait_recv()
            norm_c[...] += norm_b[y]
            norm_three.start()

        @pl.when(it == 20)
        def _():
            norm_three.wait_recv()
            norm_d[...] = (norm_d[...] + norm_c[...]) * (1.0 / 16.0)
            norm_out[...] = norm_d[...]
            norm_sq = norm_d[...] * norm_d[...]
            square[:, :NORM_PAD[1]] += norm_sq[:ROWS] + norm_sq[ROWS:]

        return carry

    ahead = pltpu.make_async_copy(emb.at[:, :, 1 - c, pl.ds(0, ROWS), :], part.at[P_SLOTS - 1], load_sem.at[P_SLOTS - 1])
    ahead.start()
    load_copy(emb, 0, 0).start()
    norm_part[...] = jnp.zeros_like(norm_part)
    square[...] = jnp.zeros_like(square)
    ahead.wait()
    pl.semaphore_wait(barrier, 4)
    start(exchange(part.at[P_SLOTS - 1], 0))
    lax.fori_loop(0, total + LAG_ZERO + 4 * LAG, trip, 0)

    value = jnp.full((8, 128), jnp.sum(square[...]), F32)
    sum_send[...] = value
    sum_recv[f] = value
    sums = [remote(sum_send, sum_recv.at[f], sum_ssem.at[k], sum_rsem.at[f], dev) for k, dev in enumerate(peers)]
    start(sums)
    wait_send((norm_zero, norm_one, norm_two, norm_three))

    def drain(slots, copies):
        def body(j, carry):
            on_plan(j, lambda *args: wait_send(copies(*args)))
            return carry
        lax.fori_loop(total - slots, total, body, 0)

    drain(P_SLOTS, ones)
    drain(R_SLOTS, lambda j, side, half: zero_copies(emb, 0, j))
    drain(SEND_SLOTS, lambda *args: twos(*args) + (two_c_even(*args), three_ab(*args), three_c(*args), four(*args, z)))

    def last(j, carry):
        out_copy(emb_out, 0, j).wait()
        return carry

    lax.fori_loop(total - SEND_SLOTS, total, last, 0)

    for k in range(1, 8):
        s = lax.rem(f + k, 8)
        remote(sum_send, sum_recv.at[s], sum_ssem.at[0], sum_rsem.at[s], core).wait_recv()
    whole = sum_recv[0]
    for k in range(1, 8):
        whole = whole + sum_recv[k]
    scale_out[...] = jnp.minimum(1.0, CLIP_NORM / jnp.sqrt(whole))
    wait_send(sums)


def reduce_grads(emb_grad, mat_grad, norm_grad):
    emb_rows = emb_grad.shape[0] // 8
    mat_rows = mat_grad.shape[0] // 8
    counts = (emb_rows // ROWS, mat_rows // ROWS)
    dma = pltpu.SemaphoreType.DMA
    scratch = [
        pltpu.VMEM((P_SLOTS, 2, 2, ROWS, WIDTH), F32),
        pltpu.VMEM((R_SLOTS, 2, 2, ROWS, WIDTH), F32),
        pltpu.VMEM((RING, 2, ROWS, SIDE_MAX), F32),
        pltpu.VMEM((RING, 2, ROWS, SIDE_MAX), F32),
        pltpu.VMEM((RING, 2, 2, ROWS, HALF_MAX), F32),
        pltpu.VMEM((RING, ROWS, 2 * SIDE_MAX), F32),
        pltpu.VMEM((RING, 2, ROWS, HALF_MAX), F32),
        pltpu.VMEM((RING, ROWS, HALF_MAX), F32),
        pltpu.VMEM((RING, ROWS, WIDTH), F32),
        pltpu.VMEM((ROWS, WIDTH), F32),
        pltpu.VMEM((NORM_ROWS, 1, WIDTH), F32),
        pltpu.VMEM((2, 2, 2) + NORM_PAD, F32),
        pltpu.VMEM((2, 2) + NORM_PAD, F32),
        pltpu.VMEM((2,) + NORM_PAD, F32),
        pltpu.VMEM(NORM_PAD, F32),
        pltpu.VMEM(NORM_PAD, F32),
        pltpu.VMEM((8, 128), F32),
        pltpu.VMEM((8, 8, 128), F32),
        dma((P_SLOTS,)), dma((2, R_SLOTS)), dma((2, R_SLOTS)), pltpu.SemaphoreType.REGULAR,
        dma((3, P_SLOTS)), dma((3, RING)), dma((3, SEND_SLOTS)), dma((3, RING)),
        dma((2, SEND_SLOTS)), dma((2, RING)), dma((SEND_SLOTS,)), dma((RING,)), dma((SEND_SLOTS,)),
        dma, dma((4,)), dma((4,)), dma((7,)), dma((8,)),
    ]
    hbm = pl.BlockSpec(memory_space=pl.ANY)
    vmem = pl.BlockSpec(memory_space=pltpu.VMEM)
    return pl.pallas_call(
        functools.partial(reduce_kernel, counts),
        out_shape=(
            jax.ShapeDtypeStruct((emb_rows, WIDTH), F32),
            jax.ShapeDtypeStruct((mat_rows, WIDTH), F32),
            jax.ShapeDtypeStruct(NORM_PAD, F32),
            jax.ShapeDtypeStruct((8, 128), F32),
        ),
        in_specs=[pl.BlockSpec(memory_space=pltpu.HBM)] * 3,
        out_specs=(hbm, hbm, vmem, vmem),
        scratch_shapes=scratch,
        compiler_params=pltpu.CompilerParams(
            collective_id=0, has_side_effects=True, vmem_limit_bytes=28 * 1024 * 1024
        ),
        name="reduce_grads",
    )(*(pltpu.with_memory_space_constraint(grad, pltpu.HBM) for grad in (
        emb_grad.reshape(2, 2, 2, emb_rows, WIDTH), mat_grad.reshape(2, 2, 2, mat_rows, WIDTH),
        norm_grad.reshape(NORM_ROWS, 1, WIDTH))))


BLOCK = 16
COLS = 384
SIDE = WIDTH // 2
STORE_SLOTS = 4


def adamw_block(grad, param, mom, var, decay_rate):
    new_mom = BETA_ONE * mom + (1.0 - BETA_ONE) * grad
    new_var = BETA_TWO * var + (1.0 - BETA_TWO) * grad * grad
    root = math.sqrt(1.0 - BETA_TWO ** ADAM_STEP)
    step_dir = new_mom / (jnp.sqrt(new_var) + ADAM_EPS * root)
    rate = LEARN_RATE * root / (1.0 - BETA_ONE ** ADAM_STEP)
    return param - (rate * step_dir + (LEARN_RATE * decay_rate) * param), new_mom, new_var


def adamw_kernel(scale, eg, ep, em, ev, mg, mp, mm, mv, ng, np_, nm, nv,
                 ep_out, em_out, ev_out, eb_out, mp_out, mm_out, mv_out, mb_out, np_out, nm_out, nv_out, nb_out,
                 p_buf, m_buf, v_buf, b_buf, n_bufs, nb_buf, sems, n_sems):
    clip = scale[0:1, 0:1]

    def copies(outs, slot, row, side):
        cols = pl.ds(side * SIDE, SIDE)
        return [pltpu.make_async_copy(buf.at[slot, side], out.at[pl.ds(row, BLOCK), cols], sems.at[k, slot, side])
                for k, (buf, out) in enumerate(zip((p_buf, m_buf, v_buf, b_buf), outs))]

    emb_outs = (ep_out, em_out, ev_out, eb_out)
    mat_outs = (mp_out, mm_out, mv_out, mb_out)
    emb_blocks = eg.shape[0] // BLOCK
    mat_blocks = mg.shape[0] // BLOCK

    def run(first, count, ins, outs):
        def body(i, carry):
            j = first + i
            slot = lax.rem(j, STORE_SLOTS)

            row = pl.multiple_of(i * BLOCK, BLOCK)
            for side in range(2):
                @pl.when(j >= STORE_SLOTS)
                def _():
                    for copy in copies(emb_outs, slot, 0, side):
                        copy.wait()

                for col in range(0, SIDE, COLS):
                    here, cols = pl.ds(col, COLS), pl.ds(side * SIDE + col, COLS)
                    g, p, m, v = (ref[pl.ds(row, BLOCK), cols] for ref in ins)
                    new_p, new_m, new_v = adamw_block(g * clip, p, m, v, WEIGHT_DECAY)
                    p_buf[slot, side, :, here] = new_p
                    m_buf[slot, side, :, here] = new_m
                    v_buf[slot, side, :, here] = new_v
                    b_buf[slot, side, :, here] = new_p.astype(jnp.bfloat16)
                for copy in copies(outs, slot, row, side):
                    copy.start()
            return carry

        lax.fori_loop(0, count, body, 0)

    run(0, emb_blocks, (eg, ep, em, ev), emb_outs)
    run(emb_blocks, mat_blocks, (mg, mp, mm, mv), mat_outs)
    new_p, new_m, new_v = adamw_block(ng[:NORM_ROWS, :NORM_COLS] * clip, np_[...], nm[...], nv[...], 0.0)
    for k, value in enumerate((new_p, new_m, new_v)):
        n_bufs[k] = value
    nb_buf[...] = new_p.astype(jnp.bfloat16)
    norm_copies = [pltpu.make_async_copy(n_bufs.at[k], out, n_sems.at[k]) for k, out in enumerate((np_out, nm_out, nv_out))]
    norm_copies.append(pltpu.make_async_copy(nb_buf, nb_out, n_sems.at[3]))
    for copy in norm_copies:
        copy.start()
    for slot in range(STORE_SLOTS):
        for side in range(2):
            for copy in copies(emb_outs, slot, 0, side):
                copy.wait()
    for copy in norm_copies:
        copy.wait()


def adamw(scale, emb, mat, norm):
    shapes = []
    for ref in (emb[1], mat[1], norm[1]):
        shapes += [jax.ShapeDtypeStruct(ref.shape, F32)] * 3 + [jax.ShapeDtypeStruct(ref.shape, jnp.bfloat16)]
    buf = (STORE_SLOTS, 2, BLOCK, SIDE)
    vmem = pl.BlockSpec(memory_space=pltpu.VMEM)
    hbm = pl.BlockSpec(memory_space=pl.ANY)
    elements = emb[1].size + mat[1].size
    return pl.pallas_call(
        adamw_kernel,
        out_shape=tuple(shapes),
        in_specs=[vmem] * 13,
        out_specs=(hbm,) * 12,
        scratch_shapes=[
            pltpu.VMEM(buf, F32), pltpu.VMEM(buf, F32), pltpu.VMEM(buf, F32), pltpu.VMEM(buf, jnp.bfloat16),
            pltpu.VMEM((3, NORM_ROWS, NORM_COLS), F32), pltpu.VMEM((NORM_ROWS, NORM_COLS), jnp.bfloat16),
            pltpu.SemaphoreType.DMA((4, STORE_SLOTS, 2)), pltpu.SemaphoreType.DMA((4,)),
        ],
        compiler_params=pltpu.CompilerParams(vmem_limit_bytes=8 * 1024 * 1024),
        cost_estimate=pl.CostEstimate(flops=20 * elements, bytes_accessed=30 * elements, transcendentals=2 * elements),
        name="adamw",
    )(scale, *emb, *mat, *norm)


def solution(mesh):
    def local_step(emb_grad, mat_grad, norm_grad, emb_param, emb_mom, emb_var, mat_param, mat_mom, mat_var, norm_param, norm_mom, norm_var):
        emb_mean, mat_mean, norm_mean, scale = reduce_grads(emb_grad[0, 0], mat_grad[0, 0], norm_grad[0, 0])
        return adamw(scale, (emb_mean, emb_param, emb_mom, emb_var), (mat_mean, mat_param, mat_mom, mat_var),
                     (norm_mean, norm_param, norm_mom, norm_var))

    grad_spec = P("dp", "fsdp", None, None)
    row_spec = P("fsdp", None)
    col_spec = P(None, "fsdp")
    in_list = (grad_spec, grad_spec, grad_spec, row_spec, row_spec, row_spec, row_spec, row_spec, row_spec, col_spec, col_spec, col_spec)
    out_list = (row_spec, row_spec, row_spec, row_spec, row_spec, row_spec, row_spec, row_spec, col_spec, col_spec, col_spec, col_spec)
    return jax.shard_map(local_step, mesh=mesh, in_specs=in_list, out_specs=out_list, check_vma=False)
```

```python
import functools
import math

import jax
import jax.numpy as jnp
from jax import lax
from jax.experimental import pallas as pl
from jax.experimental.pallas import tpu as pltpu
from jax.sharding import PartitionSpec as P

LEARN_RATE = 0.003
BETA_ONE = 0.9
BETA_TWO = 0.95
ADAM_EPS = 1e-8
WEIGHT_DECAY = 0.1
CLIP_NORM = 1.0
ADAM_STEP = 10

MESH = pl.DeviceIdType.MESH
F32 = jnp.float32

WIDTH = 5376
NORM_ROWS = 9
NORM_COLS = 672
NORM_PAD = (16, 768)
ROWS = 8
PLANS = ((1792, 896), (2176, 512))
INNER = (12, 44)
CUT = 2 * min(side for side, _ in PLANS)
SIDE_MAX = max(side for side, _ in PLANS)
HALF_MAX = max(half for _, half in PLANS)
LAG_ZERO = 0
LAG = 2
P_SLOTS = 10
R_SLOTS = 6
SEND_SLOTS = 8
RING = 16


def reduce_kernel(counts, emb, mat, norm, emb_out, mat_out, norm_out, scale_out,
                  part, recv_zero, xa, yb, zc, mid, wc, tc, grad, square,
                  norm_in, norm_part, norm_a, norm_b, norm_c, norm_d, sum_send, sum_recv,
                  load_sem, zero_send, zero_recv, credit,
                  one_send, one_recv, two_send, two_recv, three_send, three_recv, four_send, four_recv, out_sem,
                  norm_load, norm_send, norm_recv, sum_ssem, sum_rsem):
    emb_count, mat_count = counts
    total = emb_count + mat_count
    z = lax.axis_index("dp")
    f = lax.axis_index("fsdp")
    c = lax.rem(f, 2)
    x = lax.rem(lax.div(f, 2), 2)
    y = lax.div(f, 4)
    core = (z, f + 1 - 2 * c)
    xn = (z, f + 2 - 4 * x)
    yn = (z, f + 4 - 8 * y)
    zn = (1 - z, f)
    peers = [(z, lax.rem(f + k, 8)) for k in range(1, 8)]

    def remote(src, dst, ssem, rsem, dev):
        return pltpu.make_async_remote_copy(src_ref=src, dst_ref=dst, send_sem=ssem, recv_sem=rsem,
                                            device_id=dev, device_id_type=MESH)

    def on_plan(j, body):
        inner = jnp.logical_and(j >= INNER[0], j < INNER[1])
        pl.when(jnp.logical_not(inner))(lambda: body(j, *PLANS[0]))
        pl.when(inner)(lambda: body(j, *PLANS[1]))

    def half_at(side, half, which):
        return pl.ds(pl.multiple_of(2 * side + which * half, 128), half)

    barrier = pltpu.get_barrier_semaphore()
    for dev in (core, xn, yn, zn):
        pl.semaphore_signal(barrier, inc=1, device_id=dev, device_id_type=MESH)
    norm_copy = pltpu.make_async_copy(norm, norm_in, norm_load)
    norm_copy.start()

    def on_rows(j, body):
        @pl.when(j < emb_count)
        def _():
            body(emb, emb_out, pl.multiple_of(j * ROWS, ROWS))

        @pl.when(j >= emb_count)
        def _():
            body(mat, mat_out, pl.multiple_of((j - emb_count) * ROWS, ROWS))

    def load_copy(ref, row, j):
        s = lax.rem(j, P_SLOTS)
        return pltpu.make_async_copy(ref.at[:, :, c, pl.ds(row, ROWS), :], part.at[s], load_sem.at[s])

    def exchange(source, s):
        return [remote(source.at[:, :, :, cols], recv_zero.at[s, :, :, :, cols], zero_send.at[k, s], zero_recv.at[k, s], core)
                for k, cols in enumerate((pl.ds(CUT, WIDTH - CUT), pl.ds(0, CUT)))]

    def zero_copies(ref, row, j):
        return exchange(ref.at[:, :, 1 - c, pl.ds(row, ROWS)], lax.rem(j, R_SLOTS))

    def ones(j, side, half):
        s, r = lax.rem(j, P_SLOTS), lax.rem(j, RING)
        return (remote(part.at[s, :, :, :, half_at(side, half, 1 - z)], zc.at[r, :, :, :, :half], one_send.at[2, s], one_recv.at[2, r], zn),
                remote(part.at[s, :, 1 - x, :, :side], xa.at[r, :, :, :side], one_send.at[0, s], one_recv.at[0, r], xn),
                remote(part.at[s, 1 - y, :, :, side:2 * side], yb.at[r, :, :, :side], one_send.at[1, s], one_recv.at[1, r], yn))

    def two_c_even(j, side, half):
        s, r = lax.rem(j, SEND_SLOTS), lax.rem(j, RING)
        return remote(zc.at[r, :, 1 - x, :, :half], wc.at[r, :, :, :half], two_send.at[2, s], two_recv.at[2, r], xn)

    def two_c_odd(j, side, half):
        s, r = lax.rem(j, SEND_SLOTS), lax.rem(j, RING)
        return remote(zc.at[r, 1 - y, :, :, :half], wc.at[r, :, :, :half], two_send.at[2, s], two_recv.at[2, r], yn)

    def twos(j, side, half):
        s, r = lax.rem(j, SEND_SLOTS), lax.rem(j, RING)
        return (remote(xa.at[r, 1 - y, :, :side], mid.at[r, :, :side], two_send.at[0, s], two_recv.at[0, r], yn),
                remote(yb.at[r, 1 - x, :, :side], mid.at[r, :, side:2 * side], two_send.at[1, s], two_recv.at[1, r], xn))

    def three_c(j, side, half):
        s, r, odd = lax.rem(j, SEND_SLOTS), lax.rem(j, RING), lax.rem(j, 2)
        here = y + odd * (x - y)
        step = (4 - 8 * y) + odd * ((2 - 4 * x) - (4 - 8 * y))
        return remote(wc.at[r, 1 - here, :, :half], tc.at[r, :, :half], three_send.at[1, s], three_recv.at[1, r], (z, f + step))

    def three_ab(j, side, half):
        s, r = lax.rem(j, SEND_SLOTS), lax.rem(j, RING)
        return remote(mid.at[r, :, :2 * side], grad.at[r, :, :2 * side], three_send.at[0, s], three_recv.at[0, r], zn)

    def four(j, side, half, which):
        s, r = lax.rem(j, SEND_SLOTS), lax.rem(j, RING)
        cols = half_at(side, half, which)
        return remote(grad.at[r, :, cols], grad.at[r, :, cols], four_send.at[s], four_recv.at[r], zn)

    def out_copy(ref, row, j):
        return pltpu.make_async_copy(grad.at[lax.rem(j, RING)], ref.at[pl.ds(row, ROWS), :],
                                     out_sem.at[lax.rem(j, SEND_SLOTS)])

    norm_zero = remote(norm_part.at[:, :, 1 - c], norm_a, norm_send.at[0], norm_recv.at[0], core)
    norm_one = remote(norm_a.at[:, 1 - x], norm_b, norm_send.at[1], norm_recv.at[1], xn)
    norm_two = remote(norm_b.at[1 - y], norm_c, norm_send.at[2], norm_recv.at[2], yn)
    norm_three = remote(norm_c, norm_d, norm_send.at[3], norm_recv.at[3], zn)

    def when_in(j, body):
        pl.when(jnp.logical_and(j >= 0, j < total))(functools.partial(body, j))

    def after(j, slots, copies):
        @pl.when(j >= slots)
        def _():
            on_plan(j - slots, lambda *args: wait_send(copies(*args)))

    def start(copies):
        for copy in copies:
            copy.start()

    def wait_send(copies):
        for copy in copies:
            copy.wait_send()

    def stage_issue(j):
        after(j, P_SLOTS, ones)

        @pl.when(j >= R_SLOTS)
        def _():
            wait_send(zero_copies(emb, 0, j - R_SLOTS))
            pl.semaphore_wait(credit, 1)

        def body(ref, _, row):
            start(zero_copies(ref, row, j))
            load_copy(ref, row, j).start()

        on_rows(j, body)

    def stage_one(j):
        load_copy(emb, 0, j).wait()
        zero_copies(emb, 0, j)[0].wait_recv()
        part[lax.rem(j, P_SLOTS), :, :, :, CUT:] += recv_zero[lax.rem(j, R_SLOTS), :, :, :, CUT:]
        on_plan(j, lambda *args: start(ones(*args)[:1]))

    def stage_one_more(j):
        zero_copies(emb, 0, j)[1].wait_recv()
        part[lax.rem(j, P_SLOTS), :, :, :, :CUT] += recv_zero[lax.rem(j, R_SLOTS), :, :, :, :CUT]

        @pl.when(j + R_SLOTS < total)
        def _():
            pl.semaphore_signal(credit, inc=1, device_id=core, device_id_type=MESH)

        on_plan(j, lambda *args: start(ones(*args)[1:]))

    def stage_two(j):
        after(j, SEND_SLOTS, lambda *args: twos(*args) + (two_c_even(*args),))

        def body(j, side, half):
            s, r = lax.rem(j, P_SLOTS), lax.rem(j, RING)
            even = lax.rem(j, 2) == 0
            for copy in ones(j, side, half):
                copy.wait_recv()
            zc[r, :, :, :, :half] += part[s, :, :, :, half_at(side, half, z)]
            xa[r, :, :, :side] += part[s, :, x, :, :side]
            yb[r, :, :, :side] += part[s, y, :, :, side:2 * side]
            pl.when(even)(lambda: two_c_even(j, side, half).start())
            pl.when(jnp.logical_not(even))(lambda: two_c_odd(j, side, half).start())
            start(twos(j, side, half))

        on_plan(j, body)

    def stage_three(j):
        after(j, SEND_SLOTS, lambda *args: (three_ab(*args), three_c(*args)))

        def body(j, side, half):
            r = lax.rem(j, RING)
            even = lax.rem(j, 2) == 0
            for copy in twos(j, side, half) + (two_c_even(j, side, half),):
                copy.wait_recv()

            @pl.when(even)
            def _():
                wc[r, :, :, :half] += zc[r, :, x, :, :half]

            @pl.when(jnp.logical_not(even))
            def _():
                wc[r, :, :, :half] += zc[r, y, :, :, :half]

            mid[r, :, :side] += xa[r, y, :, :side]
            mid[r, :, side:2 * side] += yb[r, x, :, :side]
            start((three_c(j, side, half), three_ab(j, side, half)))

        on_plan(j, body)

    def stage_four(j):
        after(j, SEND_SLOTS, lambda *args: (four(*args, z),))

        def body(j, side, half):
            r, odd = lax.rem(j, RING), lax.rem(j, 2)
            here = y + odd * (x - y)
            three_c(j, side, half).wait_recv()
            grad[r, :, half_at(side, half, z)] = (tc[r, :, :half] + wc[r, here, :, :half]) * (1.0 / 16.0)
            four(j, side, half, z).start()

        on_plan(j, body)

    def stage_five(j):
        def body(j, side, half):
            r = lax.rem(j, RING)
            three_ab(j, side, half).wait_recv()
            both = (grad[r, :, :2 * side] + mid[r, :, :2 * side]) * (1.0 / 16.0)
            grad[r, :, :2 * side] = both
            square[:, :2 * side] += both * both
            four(j, side, half, 1 - z).wait_recv()
            rest = grad[r, :, 2 * side:]
            square[:, 2 * side:] += rest * rest

        on_plan(j, body)

        @pl.when(j >= SEND_SLOTS)
        def _():
            out_copy(emb_out, 0, j - SEND_SLOTS).wait()

        def store(_, ref, row):
            out_copy(ref, row, j).start()

        on_rows(j, store)

    def trip(it, carry):
        when_in(it + 1, stage_issue)
        when_in(it - LAG_ZERO, stage_one)
        when_in(it - LAG_ZERO - 4 * LAG, stage_five)
        when_in(it - LAG_ZERO - 3 * LAG, stage_four)
        when_in(it - LAG_ZERO - 2 * LAG, stage_three)
        when_in(it - LAG_ZERO - LAG, stage_two)
        when_in(it - LAG_ZERO, stage_one_more)

        @pl.when(it == 5)
        def _():
            norm_copy.wait()
            for k in range(8):
                for row in range(NORM_ROWS):
                    norm_part[k // 4, (k // 2) % 2, k % 2, row:row + 1, :NORM_COLS] = norm_in[row, :, k * NORM_COLS:(k + 1) * NORM_COLS]
            norm_zero.start()

        @pl.when(it == 8)
        def _():
            norm_zero.wait_recv()
            norm_a[...] += norm_part[:, :, c]
            norm_one.start()

        @pl.when(it == 12)
        def _():
            norm_one.wait_recv()
            norm_b[...] += norm_a[:, x]
            norm_two.start()

        @pl.when(it == 16)
        def _():
            norm_two.wait_recv()
            norm_c[...] += norm_b[y]
            norm_three.start()

        @pl.when(it == 20)
        def _():
            norm_three.wait_recv()
            norm_d[...] = (norm_d[...] + norm_c[...]) * (1.0 / 16.0)
            norm_out[...] = norm_d[...]
            norm_sq = norm_d[...] * norm_d[...]
            square[:, :NORM_PAD[1]] += norm_sq[:ROWS] + norm_sq[ROWS:]

        return carry

    ahead = pltpu.make_async_copy(emb.at[:, :, 1 - c, pl.ds(0, ROWS), :], part.at[P_SLOTS - 1], load_sem.at[P_SLOTS - 1])
    ahead.start()
    load_copy(emb, 0, 0).start()
    norm_part[...] = jnp.zeros_like(norm_part)
    square[...] = jnp.zeros_like(square)
    pl.semaphore_wait(barrier, 4)
    ahead.wait()
    start(exchange(part.at[P_SLOTS - 1], 0))
    lax.fori_loop(0, total + LAG_ZERO + 4 * LAG, trip, 0)

    value = jnp.full((8, 128), jnp.sum(square[...]), F32)
    sum_send[...] = value
    sum_recv[f] = value
    sums = [remote(sum_send, sum_recv.at[f], sum_ssem.at[k], sum_rsem.at[f], dev) for k, dev in enumerate(peers)]
    start(sums)
    wait_send((norm_zero, norm_one, norm_two, norm_three))

    def drain(slots, copies):
        def body(j, carry):
            on_plan(j, lambda *args: wait_send(copies(*args)))
            return carry
        lax.fori_loop(total - slots, total, body, 0)

    drain(P_SLOTS, ones)
    drain(R_SLOTS, lambda j, side, half: zero_copies(emb, 0, j))
    drain(SEND_SLOTS, lambda *args: twos(*args) + (two_c_even(*args), three_ab(*args), three_c(*args), four(*args, z)))

    def last(j, carry):
        out_copy(emb_out, 0, j).wait()
        return carry

    lax.fori_loop(total - SEND_SLOTS, total, last, 0)

    for k in range(1, 8):
        s = lax.rem(f + k, 8)
        remote(sum_send, sum_recv.at[s], sum_ssem.at[0], sum_rsem.at[s], core).wait_recv()
    whole = sum_recv[0]
    for k in range(1, 8):
        whole = whole + sum_recv[k]
    scale_out[...] = jnp.minimum(1.0, CLIP_NORM / jnp.sqrt(whole))
    wait_send(sums)


def reduce_grads(emb_grad, mat_grad, norm_grad):
    emb_rows = emb_grad.shape[0] // 8
    mat_rows = mat_grad.shape[0] // 8
    counts = (emb_rows // ROWS, mat_rows // ROWS)
    dma = pltpu.SemaphoreType.DMA
    scratch = [
        pltpu.VMEM((P_SLOTS, 2, 2, ROWS, WIDTH), F32),
        pltpu.VMEM((R_SLOTS, 2, 2, ROWS, WIDTH), F32),
        pltpu.VMEM((RING, 2, ROWS, SIDE_MAX), F32),
        pltpu.VMEM((RING, 2, ROWS, SIDE_MAX), F32),
        pltpu.VMEM((RING, 2, 2, ROWS, HALF_MAX), F32),
        pltpu.VMEM((RING, ROWS, 2 * SIDE_MAX), F32),
        pltpu.VMEM((RING, 2, ROWS, HALF_MAX), F32),
        pltpu.VMEM((RING, ROWS, HALF_MAX), F32),
        pltpu.VMEM((RING, ROWS, WIDTH), F32),
        pltpu.VMEM((ROWS, WIDTH), F32),
        pltpu.VMEM((NORM_ROWS, 1, WIDTH), F32),
        pltpu.VMEM((2, 2, 2) + NORM_PAD, F32),
        pltpu.VMEM((2, 2) + NORM_PAD, F32),
        pltpu.VMEM((2,) + NORM_PAD, F32),
        pltpu.VMEM(NORM_PAD, F32),
        pltpu.VMEM(NORM_PAD, F32),
        pltpu.VMEM((8, 128), F32),
        pltpu.VMEM((8, 8, 128), F32),
        dma((P_SLOTS,)), dma((2, R_SLOTS)), dma((2, R_SLOTS)), pltpu.SemaphoreType.REGULAR,
        dma((3, P_SLOTS)), dma((3, RING)), dma((3, SEND_SLOTS)), dma((3, RING)),
        dma((2, SEND_SLOTS)), dma((2, RING)), dma((SEND_SLOTS,)), dma((RING,)), dma((SEND_SLOTS,)),
        dma, dma((4,)), dma((4,)), dma((7,)), dma((8,)),
    ]
    hbm = pl.BlockSpec(memory_space=pl.ANY)
    vmem = pl.BlockSpec(memory_space=pltpu.VMEM)
    return pl.pallas_call(
        functools.partial(reduce_kernel, counts),
        out_shape=(
            jax.ShapeDtypeStruct((emb_rows, WIDTH), F32),
            jax.ShapeDtypeStruct((mat_rows, WIDTH), F32),
            jax.ShapeDtypeStruct(NORM_PAD, F32),
            jax.ShapeDtypeStruct((8, 128), F32),
        ),
        in_specs=[pl.BlockSpec(memory_space=pltpu.HBM)] * 3,
        out_specs=(hbm, hbm, vmem, vmem),
        scratch_shapes=scratch,
        compiler_params=pltpu.CompilerParams(
            collective_id=0, has_side_effects=True, vmem_limit_bytes=28 * 1024 * 1024
        ),
        name="reduce_grads",
    )(*(pltpu.with_memory_space_constraint(grad, pltpu.HBM) for grad in (
        emb_grad.reshape(2, 2, 2, emb_rows, WIDTH), mat_grad.reshape(2, 2, 2, mat_rows, WIDTH),
        norm_grad.reshape(NORM_ROWS, 1, WIDTH))))


BLOCK = 16
COLS = 384
SIDE = WIDTH // 2
STORE_SLOTS = 4


def adamw_block(grad, param, mom, var, decay_rate):
    new_mom = BETA_ONE * mom + (1.0 - BETA_ONE) * grad
    new_var = BETA_TWO * var + (1.0 - BETA_TWO) * grad * grad
    root = math.sqrt(1.0 - BETA_TWO ** ADAM_STEP)
    step_dir = new_mom / (jnp.sqrt(new_var) + ADAM_EPS * root)
    rate = LEARN_RATE * root / (1.0 - BETA_ONE ** ADAM_STEP)
    return param - (rate * step_dir + (LEARN_RATE * decay_rate) * param), new_mom, new_var


def adamw_kernel(scale, eg, ep, em, ev, mg, mp, mm, mv, ng, np_, nm, nv,
                 ep_out, em_out, ev_out, eb_out, mp_out, mm_out, mv_out, mb_out, np_out, nm_out, nv_out, nb_out,
                 p_buf, m_buf, v_buf, b_buf, n_bufs, nb_buf, sems, n_sems):
    clip = scale[0:1, 0:1]

    def copies(outs, slot, row, side):
        cols = pl.ds(side * SIDE, SIDE)
        return [pltpu.make_async_copy(buf.at[slot, side], out.at[pl.ds(row, BLOCK), cols], sems.at[k, slot, side])
                for k, (buf, out) in enumerate(zip((p_buf, m_buf, v_buf, b_buf), outs))]

    emb_outs = (ep_out, em_out, ev_out, eb_out)
    mat_outs = (mp_out, mm_out, mv_out, mb_out)
    emb_blocks = eg.shape[0] // BLOCK
    mat_blocks = mg.shape[0] // BLOCK

    def run(first, count, ins, outs):
        def body(i, carry):
            j = first + i
            slot = lax.rem(j, STORE_SLOTS)

            row = pl.multiple_of(i * BLOCK, BLOCK)
            for side in range(2):
                @pl.when(j >= STORE_SLOTS)
                def _():
                    for copy in copies(emb_outs, slot, 0, side):
                        copy.wait()

                for col in range(0, SIDE, COLS):
                    here, cols = pl.ds(col, COLS), pl.ds(side * SIDE + col, COLS)
                    g, p, m, v = (ref[pl.ds(row, BLOCK), cols] for ref in ins)
                    new_p, new_m, new_v = adamw_block(g * clip, p, m, v, WEIGHT_DECAY)
                    p_buf[slot, side, :, here] = new_p
                    m_buf[slot, side, :, here] = new_m
                    v_buf[slot, side, :, here] = new_v
                    b_buf[slot, side, :, here] = new_p.astype(jnp.bfloat16)
                for copy in copies(outs, slot, row, side):
                    copy.start()
            return carry

        lax.fori_loop(0, count, body, 0)

    run(0, emb_blocks, (eg, ep, em, ev), emb_outs)
    run(emb_blocks, mat_blocks, (mg, mp, mm, mv), mat_outs)
    new_p, new_m, new_v = adamw_block(ng[:NORM_ROWS, :NORM_COLS] * clip, np_[...], nm[...], nv[...], 0.0)
    for k, value in enumerate((new_p, new_m, new_v)):
        n_bufs[k] = value
    nb_buf[...] = new_p.astype(jnp.bfloat16)
    norm_copies = [pltpu.make_async_copy(n_bufs.at[k], out, n_sems.at[k]) for k, out in enumerate((np_out, nm_out, nv_out))]
    norm_copies.append(pltpu.make_async_copy(nb_buf, nb_out, n_sems.at[3]))
    for copy in norm_copies:
        copy.start()
    for slot in range(STORE_SLOTS):
        for side in range(2):
            for copy in copies(emb_outs, slot, 0, side):
                copy.wait()
    for copy in norm_copies:
        copy.wait()


def adamw(scale, emb, mat, norm):
    shapes = []
    for ref in (emb[1], mat[1], norm[1]):
        shapes += [jax.ShapeDtypeStruct(ref.shape, F32)] * 3 + [jax.ShapeDtypeStruct(ref.shape, jnp.bfloat16)]
    buf = (STORE_SLOTS, 2, BLOCK, SIDE)
    vmem = pl.BlockSpec(memory_space=pltpu.VMEM)
    hbm = pl.BlockSpec(memory_space=pl.ANY)
    elements = emb[1].size + mat[1].size
    return pl.pallas_call(
        adamw_kernel,
        out_shape=tuple(shapes),
        in_specs=[vmem] * 13,
        out_specs=(hbm,) * 12,
        scratch_shapes=[
            pltpu.VMEM(buf, F32), pltpu.VMEM(buf, F32), pltpu.VMEM(buf, F32), pltpu.VMEM(buf, jnp.bfloat16),
            pltpu.VMEM((3, NORM_ROWS, NORM_COLS), F32), pltpu.VMEM((NORM_ROWS, NORM_COLS), jnp.bfloat16),
            pltpu.SemaphoreType.DMA((4, STORE_SLOTS, 2)), pltpu.SemaphoreType.DMA((4,)),
        ],
        compiler_params=pltpu.CompilerParams(vmem_limit_bytes=8 * 1024 * 1024),
        cost_estimate=pl.CostEstimate(flops=20 * elements, bytes_accessed=30 * elements, transcendentals=2 * elements),
        name="adamw",
    )(scale, *emb, *mat, *norm)


def solution(mesh):
    def local_step(emb_grad, mat_grad, norm_grad, emb_param, emb_mom, emb_var, mat_param, mat_mom, mat_var, norm_param, norm_mom, norm_var):
        emb_mean, mat_mean, norm_mean, scale = reduce_grads(emb_grad[0, 0], mat_grad[0, 0], norm_grad[0, 0])
        return adamw(scale, (emb_mean, emb_param, emb_mom, emb_var), (mat_mean, mat_param, mat_mom, mat_var),
                     (norm_mean, norm_param, norm_mom, norm_var))

    grad_spec = P("dp", "fsdp", None, None)
    row_spec = P("fsdp", None)
    col_spec = P(None, "fsdp")
    in_list = (grad_spec, grad_spec, grad_spec, row_spec, row_spec, row_spec, row_spec, row_spec, row_spec, col_spec, col_spec, col_spec)
    out_list = (row_spec, row_spec, row_spec, row_spec, row_spec, row_spec, row_spec, row_spec, col_spec, col_spec, col_spec, col_spec)
    return jax.shard_map(local_step, mesh=mesh, in_specs=in_list, out_specs=out_list, check_vma=False)
```

```python
import functools
import math

import jax
import jax.numpy as jnp
from jax import lax
from jax.experimental import pallas as pl
from jax.experimental.pallas import tpu as pltpu
from jax.sharding import PartitionSpec as P

LEARN_RATE = 0.003
BETA_ONE = 0.9
BETA_TWO = 0.95
ADAM_EPS = 1e-8
WEIGHT_DECAY = 0.1
CLIP_NORM = 1.0
ADAM_STEP = 10

MESH = pl.DeviceIdType.MESH
F32 = jnp.float32

WIDTH = 5376
NORM_ROWS = 9
NORM_COLS = 672
NORM_PAD = (16, 768)
ROWS = 8
PLANS = ((1792, 896), (2176, 512))
INNER = (13, 44)
CUT = 2 * min(side for side, _ in PLANS)
SIDE_MAX = max(side for side, _ in PLANS)
HALF_MAX = max(half for _, half in PLANS)
LAG_ZERO = 0
LAG = 2
P_SLOTS = 10
R_SLOTS = 6
SEND_SLOTS = 8
RING = 16


def reduce_kernel(counts, emb, mat, norm, emb_out, mat_out, norm_out, scale_out,
                  part, recv_zero, xa, yb, zc, mid, wc, tc, grad, square,
                  norm_in, norm_part, norm_a, norm_b, norm_c, norm_d, sum_send, sum_recv,
                  load_sem, zero_send, zero_recv, credit,
                  one_send, one_recv, two_send, two_recv, three_send, three_recv, four_send, four_recv, out_sem,
                  norm_load, norm_send, norm_recv, sum_ssem, sum_rsem):
    emb_count, mat_count = counts
    total = emb_count + mat_count
    z = lax.axis_index("dp")
    f = lax.axis_index("fsdp")
    c = lax.rem(f, 2)
    x = lax.rem(lax.div(f, 2), 2)
    y = lax.div(f, 4)
    core = (z, f + 1 - 2 * c)
    xn = (z, f + 2 - 4 * x)
    yn = (z, f + 4 - 8 * y)
    zn = (1 - z, f)
    dc, dx, dy = 1 - 2 * c, 2 - 4 * x, 4 - 8 * y
    peers = [(z, f + step) for step in (dx + dy + dc, dx + dy, dy + dc, dx + dc, dy, dx, dc)]

    def remote(src, dst, ssem, rsem, dev):
        return pltpu.make_async_remote_copy(src_ref=src, dst_ref=dst, send_sem=ssem, recv_sem=rsem,
                                            device_id=dev, device_id_type=MESH)

    def on_plan(j, body):
        inner = jnp.logical_and(j >= INNER[0], j < INNER[1])
        pl.when(jnp.logical_not(inner))(lambda: body(j, *PLANS[0]))
        pl.when(inner)(lambda: body(j, *PLANS[1]))

    def half_at(side, half, which):
        return pl.ds(pl.multiple_of(2 * side + which * half, 128), half)

    barrier = pltpu.get_barrier_semaphore()
    for dev in (core, xn, yn, zn):
        pl.semaphore_signal(barrier, inc=1, device_id=dev, device_id_type=MESH)
    norm_copy = pltpu.make_async_copy(norm, norm_in, norm_load)
    norm_copy.start()

    def on_rows(j, body):
        @pl.when(j < emb_count)
        def _():
            body(emb, emb_out, pl.multiple_of(j * ROWS, ROWS))

        @pl.when(j >= emb_count)
        def _():
            body(mat, mat_out, pl.multiple_of((j - emb_count) * ROWS, ROWS))

    def load_copy(ref, row, j):
        s = lax.rem(j, P_SLOTS)
        return pltpu.make_async_copy(ref.at[:, :, c, pl.ds(row, ROWS), :], part.at[s], load_sem.at[s])

    def exchange(source, s):
        return [remote(source.at[:, :, :, cols], recv_zero.at[s, :, :, :, cols], zero_send.at[k, s], zero_recv.at[k, s], core)
                for k, cols in enumerate((pl.ds(CUT, WIDTH - CUT), pl.ds(0, CUT)))]

    def zero_copies(ref, row, j):
        return exchange(ref.at[:, :, 1 - c, pl.ds(row, ROWS)], lax.rem(j, R_SLOTS))

    def ones(j, side, half):
        s, r = lax.rem(j, P_SLOTS), lax.rem(j, RING)
        return (remote(part.at[s, :, :, :, half_at(side, half, 1 - z)], zc.at[r, :, :, :, :half], one_send.at[2, s], one_recv.at[2, r], zn),
                remote(part.at[s, :, 1 - x, :, :side], xa.at[r, :, :, :side], one_send.at[0, s], one_recv.at[0, r], xn),
                remote(part.at[s, 1 - y, :, :, side:2 * side], yb.at[r, :, :, :side], one_send.at[1, s], one_recv.at[1, r], yn))

    def two_c_even(j, side, half):
        s, r = lax.rem(j, SEND_SLOTS), lax.rem(j, RING)
        return remote(zc.at[r, :, 1 - x, :, :half], wc.at[r, :, :, :half], two_send.at[2, s], two_recv.at[2, r], xn)

    def two_c_odd(j, side, half):
        s, r = lax.rem(j, SEND_SLOTS), lax.rem(j, RING)
        return remote(zc.at[r, 1 - y, :, :, :half], wc.at[r, :, :, :half], two_send.at[2, s], two_recv.at[2, r], yn)

    def twos(j, side, half):
        s, r = lax.rem(j, SEND_SLOTS), lax.rem(j, RING)
        return (remote(xa.at[r, 1 - y, :, :side], mid.at[r, :, :side], two_send.at[0, s], two_recv.at[0, r], yn),
                remote(yb.at[r, 1 - x, :, :side], mid.at[r, :, side:2 * side], two_send.at[1, s], two_recv.at[1, r], xn))

    def three_c(j, side, half):
        s, r, odd = lax.rem(j, SEND_SLOTS), lax.rem(j, RING), lax.rem(j, 2)
        here = y + odd * (x - y)
        step = (4 - 8 * y) + odd * ((2 - 4 * x) - (4 - 8 * y))
        return remote(wc.at[r, 1 - here, :, :half], tc.at[r, :, :half], three_send.at[1, s], three_recv.at[1, r], (z, f + step))

    def three_ab(j, side, half):
        s, r = lax.rem(j, SEND_SLOTS), lax.rem(j, RING)
        return remote(mid.at[r, :, :2 * side], grad.at[r, :, :2 * side], three_send.at[0, s], three_recv.at[0, r], zn)

    def four(j, side, half, which):
        s, r = lax.rem(j, SEND_SLOTS), lax.rem(j, RING)
        cols = half_at(side, half, which)
        return remote(grad.at[r, :, cols], grad.at[r, :, cols], four_send.at[s], four_recv.at[r], zn)

    def out_copy(ref, row, j):
        return pltpu.make_async_copy(grad.at[lax.rem(j, RING)], ref.at[pl.ds(row, ROWS), :],
                                     out_sem.at[lax.rem(j, SEND_SLOTS)])

    norm_zero = remote(norm_part.at[:, :, 1 - c], norm_a, norm_send.at[0], norm_recv.at[0], core)
    norm_one = remote(norm_a.at[:, 1 - x], norm_b, norm_send.at[1], norm_recv.at[1], xn)
    norm_two = remote(norm_b.at[1 - y], norm_c, norm_send.at[2], norm_recv.at[2], yn)
    norm_three = remote(norm_c, norm_d, norm_send.at[3], norm_recv.at[3], zn)

    def when_in(j, body):
        pl.when(jnp.logical_and(j >= 0, j < total))(functools.partial(body, j))

    def after(j, slots, copies):
        @pl.when(j >= slots)
        def _():
            on_plan(j - slots, lambda *args: wait_send(copies(*args)))

    def start(copies):
        for copy in copies:
            copy.start()

    def wait_send(copies):
        for copy in copies:
            copy.wait_send()

    def stage_issue(j):
        after(j, P_SLOTS, ones)

        @pl.when(j >= R_SLOTS)
        def _():
            wait_send(zero_copies(emb, 0, j - R_SLOTS))
            pl.semaphore_wait(credit, 1)

        def body(ref, _, row):
            start(zero_copies(ref, row, j))
            load_copy(ref, row, j).start()

        on_rows(j, body)

    def stage_one(j):
        load_copy(emb, 0, j).wait()
        zero_copies(emb, 0, j)[0].wait_recv()
        part[lax.rem(j, P_SLOTS), :, :, :, CUT:] += recv_zero[lax.rem(j, R_SLOTS), :, :, :, CUT:]
        on_plan(j, lambda *args: start(ones(*args)[:1]))

    def stage_one_more(j):
        zero_copies(emb, 0, j)[1].wait_recv()
        part[lax.rem(j, P_SLOTS), :, :, :, :CUT] += recv_zero[lax.rem(j, R_SLOTS), :, :, :, :CUT]

        @pl.when(j + R_SLOTS < total)
        def _():
            pl.semaphore_signal(credit, inc=1, device_id=core, device_id_type=MESH)

        on_plan(j, lambda *args: start(ones(*args)[1:]))

    def stage_two(j):
        after(j, SEND_SLOTS, lambda *args: twos(*args) + (two_c_even(*args),))

        def body(j, side, half):
            s, r = lax.rem(j, P_SLOTS), lax.rem(j, RING)
            even = lax.rem(j, 2) == 0
            for copy in ones(j, side, half):
                copy.wait_recv()
            zc[r, :, :, :, :half] += part[s, :, :, :, half_at(side, half, z)]
            xa[r, :, :, :side] += part[s, :, x, :, :side]
            yb[r, :, :, :side] += part[s, y, :, :, side:2 * side]
            pl.when(even)(lambda: two_c_even(j, side, half).start())
            pl.when(jnp.logical_not(even))(lambda: two_c_odd(j, side, half).start())
            start(twos(j, side, half))

        on_plan(j, body)

    def stage_three(j):
        after(j, SEND_SLOTS, lambda *args: (three_ab(*args), three_c(*args)))

        def body(j, side, half):
            r = lax.rem(j, RING)
            even = lax.rem(j, 2) == 0
            for copy in twos(j, side, half) + (two_c_even(j, side, half),):
                copy.wait_recv()

            @pl.when(even)
            def _():
                wc[r, :, :, :half] += zc[r, :, x, :, :half]

            @pl.when(jnp.logical_not(even))
            def _():
                wc[r, :, :, :half] += zc[r, y, :, :, :half]

            mid[r, :, :side] += xa[r, y, :, :side]
            mid[r, :, side:2 * side] += yb[r, x, :, :side]
            start((three_c(j, side, half), three_ab(j, side, half)))

        on_plan(j, body)

    def stage_four(j):
        after(j, SEND_SLOTS, lambda *args: (four(*args, z),))

        def body(j, side, half):
            r, odd = lax.rem(j, RING), lax.rem(j, 2)
            here = y + odd * (x - y)
            three_c(j, side, half).wait_recv()
            grad[r, :, half_at(side, half, z)] = (tc[r, :, :half] + wc[r, here, :, :half]) * (1.0 / 16.0)
            four(j, side, half, z).start()

        on_plan(j, body)

    def stage_five(j):
        def body(j, side, half):
            r = lax.rem(j, RING)
            three_ab(j, side, half).wait_recv()
            both = (grad[r, :, :2 * side] + mid[r, :, :2 * side]) * (1.0 / 16.0)
            grad[r, :, :2 * side] = both
            square[:, :2 * side] += both * both
            four(j, side, half, 1 - z).wait_recv()
            rest = grad[r, :, 2 * side:]
            square[:, 2 * side:] += rest * rest

        on_plan(j, body)

        @pl.when(j >= SEND_SLOTS)
        def _():
            out_copy(emb_out, 0, j - SEND_SLOTS).wait()

        def store(_, ref, row):
            out_copy(ref, row, j).start()

        on_rows(j, store)

    def trip(it, carry):
        when_in(it + 1, stage_issue)
        when_in(it - LAG_ZERO, stage_one)
        when_in(it - LAG_ZERO - 4 * LAG, stage_five)
        when_in(it - LAG_ZERO - 3 * LAG, stage_four)
        when_in(it - LAG_ZERO - 2 * LAG, stage_three)
        when_in(it - LAG_ZERO - LAG, stage_two)
        when_in(it - LAG_ZERO, stage_one_more)

        @pl.when(it == 5)
        def _():
            norm_copy.wait()
            for k in range(8):
                for row in range(NORM_ROWS):
                    norm_part[k // 4, (k // 2) % 2, k % 2, row:row + 1, :NORM_COLS] = norm_in[row, :, k * NORM_COLS:(k + 1) * NORM_COLS]
            norm_zero.start()

        @pl.when(it == 8)
        def _():
            norm_zero.wait_recv()
            norm_a[...] += norm_part[:, :, c]
            norm_one.start()

        @pl.when(it == 12)
        def _():
            norm_one.wait_recv()
            norm_b[...] += norm_a[:, x]
            norm_two.start()

        @pl.when(it == 16)
        def _():
            norm_two.wait_recv()
            norm_c[...] += norm_b[y]
            norm_three.start()

        @pl.when(it == 20)
        def _():
            norm_three.wait_recv()
            norm_d[...] = (norm_d[...] + norm_c[...]) * (1.0 / 16.0)
            norm_out[...] = norm_d[...]
            norm_sq = norm_d[...] * norm_d[...]
            square[:, :NORM_PAD[1]] += norm_sq[:ROWS] + norm_sq[ROWS:]

        return carry

    ahead = pltpu.make_async_copy(emb.at[:, :, 1 - c, pl.ds(0, ROWS), :], part.at[P_SLOTS - 1], load_sem.at[P_SLOTS - 1])
    ahead.start()
    load_copy(emb, 0, 0).start()
    norm_part[...] = jnp.zeros_like(norm_part)
    square[...] = jnp.zeros_like(square)
    pl.semaphore_wait(barrier, 4)
    ahead.wait()
    start(exchange(part.at[P_SLOTS - 1], 0))
    lax.fori_loop(0, total + LAG_ZERO + 4 * LAG, trip, 0)

    value = jnp.full((8, 128), jnp.sum(square[...]), F32)
    sum_send[...] = value
    sum_recv[f] = value
    sums = [remote(sum_send, sum_recv.at[f], sum_ssem.at[k], sum_rsem.at[f], dev) for k, dev in enumerate(peers)]
    start(sums)
    wait_send((norm_zero, norm_one, norm_two, norm_three))

    def drain(slots, copies):
        def body(j, carry):
            on_plan(j, lambda *args: wait_send(copies(*args)))
            return carry
        lax.fori_loop(total - slots, total, body, 0)

    drain(P_SLOTS, ones)
    drain(R_SLOTS, lambda j, side, half: zero_copies(emb, 0, j))
    drain(SEND_SLOTS, lambda *args: twos(*args) + (two_c_even(*args), three_ab(*args), three_c(*args), four(*args, z)))

    def last(j, carry):
        out_copy(emb_out, 0, j).wait()
        return carry

    lax.fori_loop(total - SEND_SLOTS, total, last, 0)

    for k in range(1, 8):
        s = lax.rem(f + k, 8)
        remote(sum_send, sum_recv.at[s], sum_ssem.at[0], sum_rsem.at[s], core).wait_recv()
    whole = sum_recv[0]
    for k in range(1, 8):
        whole = whole + sum_recv[k]
    scale_out[...] = jnp.minimum(1.0, CLIP_NORM / jnp.sqrt(whole))
    wait_send(sums)


def reduce_grads(emb_grad, mat_grad, norm_grad):
    emb_rows = emb_grad.shape[0] // 8
    mat_rows = mat_grad.shape[0] // 8
    counts = (emb_rows // ROWS, mat_rows // ROWS)
    dma = pltpu.SemaphoreType.DMA
    scratch = [
        pltpu.VMEM((P_SLOTS, 2, 2, ROWS, WIDTH), F32),
        pltpu.VMEM((R_SLOTS, 2, 2, ROWS, WIDTH), F32),
        pltpu.VMEM((RING, 2, ROWS, SIDE_MAX), F32),
        pltpu.VMEM((RING, 2, ROWS, SIDE_MAX), F32),
        pltpu.VMEM((RING, 2, 2, ROWS, HALF_MAX), F32),
        pltpu.VMEM((RING, ROWS, 2 * SIDE_MAX), F32),
        pltpu.VMEM((RING, 2, ROWS, HALF_MAX), F32),
        pltpu.VMEM((RING, ROWS, HALF_MAX), F32),
        pltpu.VMEM((RING, ROWS, WIDTH), F32),
        pltpu.VMEM((ROWS, WIDTH), F32),
        pltpu.VMEM((NORM_ROWS, 1, WIDTH), F32),
        pltpu.VMEM((2, 2, 2) + NORM_PAD, F32),
        pltpu.VMEM((2, 2) + NORM_PAD, F32),
        pltpu.VMEM((2,) + NORM_PAD, F32),
        pltpu.VMEM(NORM_PAD, F32),
        pltpu.VMEM(NORM_PAD, F32),
        pltpu.VMEM((8, 128), F32),
        pltpu.VMEM((8, 8, 128), F32),
        dma((P_SLOTS,)), dma((2, R_SLOTS)), dma((2, R_SLOTS)), pltpu.SemaphoreType.REGULAR,
        dma((3, P_SLOTS)), dma((3, RING)), dma((3, SEND_SLOTS)), dma((3, RING)),
        dma((2, SEND_SLOTS)), dma((2, RING)), dma((SEND_SLOTS,)), dma((RING,)), dma((SEND_SLOTS,)),
        dma, dma((4,)), dma((4,)), dma((7,)), dma((8,)),
    ]
    hbm = pl.BlockSpec(memory_space=pl.ANY)
    vmem = pl.BlockSpec(memory_space=pltpu.VMEM)
    return pl.pallas_call(
        functools.partial(reduce_kernel, counts),
        out_shape=(
            jax.ShapeDtypeStruct((emb_rows, WIDTH), F32),
            jax.ShapeDtypeStruct((mat_rows, WIDTH), F32),
            jax.ShapeDtypeStruct(NORM_PAD, F32),
            jax.ShapeDtypeStruct((8, 128), F32),
        ),
        in_specs=[pl.BlockSpec(memory_space=pltpu.HBM)] * 3,
        out_specs=(hbm, hbm, vmem, vmem),
        scratch_shapes=scratch,
        compiler_params=pltpu.CompilerParams(
            collective_id=0, has_side_effects=True, vmem_limit_bytes=28 * 1024 * 1024
        ),
        name="reduce_grads",
    )(*(pltpu.with_memory_space_constraint(grad, pltpu.HBM) for grad in (
        emb_grad.reshape(2, 2, 2, emb_rows, WIDTH), mat_grad.reshape(2, 2, 2, mat_rows, WIDTH),
        norm_grad.reshape(NORM_ROWS, 1, WIDTH))))


BLOCK = 16
COLS = 384
SIDE = WIDTH // 2
STORE_SLOTS = 4


def adamw_block(grad, param, mom, var, decay_rate):
    new_mom = BETA_ONE * mom + (1.0 - BETA_ONE) * grad
    new_var = BETA_TWO * var + (1.0 - BETA_TWO) * grad * grad
    root = math.sqrt(1.0 - BETA_TWO ** ADAM_STEP)
    step_dir = new_mom / (jnp.sqrt(new_var) + ADAM_EPS * root)
    rate = LEARN_RATE * root / (1.0 - BETA_ONE ** ADAM_STEP)
    return param - (rate * step_dir + (LEARN_RATE * decay_rate) * param), new_mom, new_var


def adamw_kernel(scale, eg, ep, em, ev, mg, mp, mm, mv, ng, np_, nm, nv,
                 ep_out, em_out, ev_out, eb_out, mp_out, mm_out, mv_out, mb_out, np_out, nm_out, nv_out, nb_out,
                 p_buf, m_buf, v_buf, b_buf, n_bufs, nb_buf, sems, n_sems):
    clip = scale[0:1, 0:1]

    def copies(outs, slot, row, side):
        cols = pl.ds(side * SIDE, SIDE)
        return [pltpu.make_async_copy(buf.at[slot, side], out.at[pl.ds(row, BLOCK), cols], sems.at[k, slot, side])
                for k, (buf, out) in enumerate(zip((p_buf, m_buf, v_buf, b_buf), outs))]

    emb_outs = (ep_out, em_out, ev_out, eb_out)
    mat_outs = (mp_out, mm_out, mv_out, mb_out)
    emb_blocks = eg.shape[0] // BLOCK
    mat_blocks = mg.shape[0] // BLOCK

    def run(first, count, ins, outs):
        def body(i, carry):
            j = first + i
            slot = lax.rem(j, STORE_SLOTS)

            row = pl.multiple_of(i * BLOCK, BLOCK)
            for side in range(2):
                @pl.when(j >= STORE_SLOTS)
                def _():
                    for copy in copies(emb_outs, slot, 0, side):
                        copy.wait()

                for col in range(0, SIDE, COLS):
                    here, cols = pl.ds(col, COLS), pl.ds(side * SIDE + col, COLS)
                    g, p, m, v = (ref[pl.ds(row, BLOCK), cols] for ref in ins)
                    new_p, new_m, new_v = adamw_block(g * clip, p, m, v, WEIGHT_DECAY)
                    p_buf[slot, side, :, here] = new_p
                    m_buf[slot, side, :, here] = new_m
                    v_buf[slot, side, :, here] = new_v
                    b_buf[slot, side, :, here] = new_p.astype(jnp.bfloat16)
                for copy in copies(outs, slot, row, side):
                    copy.start()
            return carry

        lax.fori_loop(0, count, body, 0)

    run(0, emb_blocks, (eg, ep, em, ev), emb_outs)
    run(emb_blocks, mat_blocks, (mg, mp, mm, mv), mat_outs)
    new_p, new_m, new_v = adamw_block(ng[:NORM_ROWS, :NORM_COLS] * clip, np_[...], nm[...], nv[...], 0.0)
    for k, value in enumerate((new_p, new_m, new_v)):
        n_bufs[k] = value
    nb_buf[...] = new_p.astype(jnp.bfloat16)
    norm_copies = [pltpu.make_async_copy(n_bufs.at[k], out, n_sems.at[k]) for k, out in enumerate((np_out, nm_out, nv_out))]
    norm_copies.append(pltpu.make_async_copy(nb_buf, nb_out, n_sems.at[3]))
    for copy in norm_copies:
        copy.start()
    for slot in range(STORE_SLOTS):
        for side in range(2):
            for copy in copies(emb_outs, slot, 0, side):
                copy.wait()
    for copy in norm_copies:
        copy.wait()


def adamw(scale, emb, mat, norm):
    shapes = []
    for ref in (emb[1], mat[1], norm[1]):
        shapes += [jax.ShapeDtypeStruct(ref.shape, F32)] * 3 + [jax.ShapeDtypeStruct(ref.shape, jnp.bfloat16)]
    buf = (STORE_SLOTS, 2, BLOCK, SIDE)
    vmem = pl.BlockSpec(memory_space=pltpu.VMEM)
    hbm = pl.BlockSpec(memory_space=pl.ANY)
    elements = emb[1].size + mat[1].size
    return pl.pallas_call(
        adamw_kernel,
        out_shape=tuple(shapes),
        in_specs=[vmem] * 13,
        out_specs=(hbm,) * 12,
        scratch_shapes=[
            pltpu.VMEM(buf, F32), pltpu.VMEM(buf, F32), pltpu.VMEM(buf, F32), pltpu.VMEM(buf, jnp.bfloat16),
            pltpu.VMEM((3, NORM_ROWS, NORM_COLS), F32), pltpu.VMEM((NORM_ROWS, NORM_COLS), jnp.bfloat16),
            pltpu.SemaphoreType.DMA((4, STORE_SLOTS, 2)), pltpu.SemaphoreType.DMA((4,)),
        ],
        compiler_params=pltpu.CompilerParams(vmem_limit_bytes=8 * 1024 * 1024),
        cost_estimate=pl.CostEstimate(flops=20 * elements, bytes_accessed=30 * elements, transcendentals=2 * elements),
        name="adamw",
    )(scale, *emb, *mat, *norm)


def solution(mesh):
    def local_step(emb_grad, mat_grad, norm_grad, emb_param, emb_mom, emb_var, mat_param, mat_mom, mat_var, norm_param, norm_mom, norm_var):
        emb_mean, mat_mean, norm_mean, scale = reduce_grads(emb_grad[0, 0], mat_grad[0, 0], norm_grad[0, 0])
        return adamw(scale, (emb_mean, emb_param, emb_mom, emb_var), (mat_mean, mat_param, mat_mom, mat_var),
                     (norm_mean, norm_param, norm_mom, norm_var))

    grad_spec = P("dp", "fsdp", None, None)
    row_spec = P("fsdp", None)
    col_spec = P(None, "fsdp")
    in_list = (grad_spec, grad_spec, grad_spec, row_spec, row_spec, row_spec, row_spec, row_spec, row_spec, col_spec, col_spec, col_spec)
    out_list = (row_spec, row_spec, row_spec, row_spec, row_spec, row_spec, row_spec, row_spec, col_spec, col_spec, col_spec, col_spec)
    return jax.shard_map(local_step, mesh=mesh, in_specs=in_list, out_specs=out_list, check_vma=False)
```

```python
import functools
import math

import jax
import jax.numpy as jnp
from jax import lax
from jax.experimental import pallas as pl
from jax.experimental.pallas import tpu as pltpu
from jax.sharding import PartitionSpec as P

LEARN_RATE = 0.003
BETA_ONE = 0.9
BETA_TWO = 0.95
ADAM_EPS = 1e-8
WEIGHT_DECAY = 0.1
CLIP_NORM = 1.0
ADAM_STEP = 10

MESH = pl.DeviceIdType.MESH
F32 = jnp.float32

WIDTH = 5376
NORM_ROWS = 9
NORM_COLS = 672
NORM_PAD = (16, 768)
ROWS = 8
PLANS = ((1792, 896), (2176, 512))
INNER = (14, 45)
CUT = 2 * min(side for side, _ in PLANS)
SIDE_MAX = max(side for side, _ in PLANS)
HALF_MAX = max(half for _, half in PLANS)
LAG_ZERO = 0
LAG = 2
P_SLOTS = 10
R_SLOTS = 6
SEND_SLOTS = 8
RING = 16


def reduce_kernel(counts, emb, mat, norm, emb_out, mat_out, norm_out, scale_out,
                  part, recv_zero, xa, yb, zc, mid, wc, tc, grad, square,
                  norm_in, norm_part, norm_a, norm_b, norm_c, norm_d, sum_send, sum_recv,
                  load_sem, zero_send, zero_recv, credit,
                  one_send, one_recv, two_send, two_recv, three_send, three_recv, four_send, four_recv, out_sem,
                  norm_load, norm_send, norm_recv, sum_ssem, sum_rsem):
    emb_count, mat_count = counts
    total = emb_count + mat_count
    z = lax.axis_index("dp")
    f = lax.axis_index("fsdp")
    c = lax.rem(f, 2)
    x = lax.rem(lax.div(f, 2), 2)
    y = lax.div(f, 4)
    core = (z, f + 1 - 2 * c)
    xn = (z, f + 2 - 4 * x)
    yn = (z, f + 4 - 8 * y)
    zn = (1 - z, f)
    dc, dx, dy = 1 - 2 * c, 2 - 4 * x, 4 - 8 * y
    peers = [(z, f + step) for step in (dx + dy + dc, dx + dy, dy + dc, dx + dc, dy, dx, dc)]

    def remote(src, dst, ssem, rsem, dev):
        return pltpu.make_async_remote_copy(src_ref=src, dst_ref=dst, send_sem=ssem, recv_sem=rsem,
                                            device_id=dev, device_id_type=MESH)

    def on_plan(j, body):
        inner = jnp.logical_and(j >= INNER[0], j < INNER[1])
        pl.when(jnp.logical_not(inner))(lambda: body(j, *PLANS[0]))
        pl.when(inner)(lambda: body(j, *PLANS[1]))

    def half_at(side, half, which):
        return pl.ds(pl.multiple_of(2 * side + which * half, 128), half)

    barrier = pltpu.get_barrier_semaphore()
    for dev in (core, xn, yn, zn):
        pl.semaphore_signal(barrier, inc=1, device_id=dev, device_id_type=MESH)
    norm_copy = pltpu.make_async_copy(norm, norm_in, norm_load)
    norm_copy.start()

    def on_rows(j, body):
        @pl.when(j < emb_count)
        def _():
            body(emb, emb_out, pl.multiple_of(j * ROWS, ROWS))

        @pl.when(j >= emb_count)
        def _():
            body(mat, mat_out, pl.multiple_of((j - emb_count) * ROWS, ROWS))

    def load_copy(ref, row, j):
        s = lax.rem(j, P_SLOTS)
        return pltpu.make_async_copy(ref.at[:, :, c, pl.ds(row, ROWS), :], part.at[s], load_sem.at[s])

    def exchange(source, s):
        return [remote(source.at[:, :, :, cols], recv_zero.at[s, :, :, :, cols], zero_send.at[k, s], zero_recv.at[k, s], core)
                for k, cols in enumerate((pl.ds(CUT, WIDTH - CUT), pl.ds(0, CUT)))]

    def zero_copies(ref, row, j):
        return exchange(ref.at[:, :, 1 - c, pl.ds(row, ROWS)], lax.rem(j, R_SLOTS))

    def ones(j, side, half):
        s, r = lax.rem(j, P_SLOTS), lax.rem(j, RING)
        return (remote(part.at[s, :, :, :, half_at(side, half, 1 - z)], zc.at[r, :, :, :, :half], one_send.at[2, s], one_recv.at[2, r], zn),
                remote(part.at[s, :, 1 - x, :, :side], xa.at[r, :, :, :side], one_send.at[0, s], one_recv.at[0, r], xn),
                remote(part.at[s, 1 - y, :, :, side:2 * side], yb.at[r, :, :, :side], one_send.at[1, s], one_recv.at[1, r], yn))

    def two_c_even(j, side, half):
        s, r = lax.rem(j, SEND_SLOTS), lax.rem(j, RING)
        return remote(zc.at[r, :, 1 - x, :, :half], wc.at[r, :, :, :half], two_send.at[2, s], two_recv.at[2, r], xn)

    def two_c_odd(j, side, half):
        s, r = lax.rem(j, SEND_SLOTS), lax.rem(j, RING)
        return remote(zc.at[r, 1 - y, :, :, :half], wc.at[r, :, :, :half], two_send.at[2, s], two_recv.at[2, r], yn)

    def twos(j, side, half):
        s, r = lax.rem(j, SEND_SLOTS), lax.rem(j, RING)
        return (remote(xa.at[r, 1 - y, :, :side], mid.at[r, :, :side], two_send.at[0, s], two_recv.at[0, r], yn),
                remote(yb.at[r, 1 - x, :, :side], mid.at[r, :, side:2 * side], two_send.at[1, s], two_recv.at[1, r], xn))

    def three_c(j, side, half):
        s, r, odd = lax.rem(j, SEND_SLOTS), lax.rem(j, RING), lax.rem(j, 2)
        here = y + odd * (x - y)
        step = (4 - 8 * y) + odd * ((2 - 4 * x) - (4 - 8 * y))
        return remote(wc.at[r, 1 - here, :, :half], tc.at[r, :, :half], three_send.at[1, s], three_recv.at[1, r], (z, f + step))

    def three_ab(j, side, half):
        s, r = lax.rem(j, SEND_SLOTS), lax.rem(j, RING)
        return remote(mid.at[r, :, :2 * side], grad.at[r, :, :2 * side], three_send.at[0, s], three_recv.at[0, r], zn)

    def four(j, side, half, which):
        s, r = lax.rem(j, SEND_SLOTS), lax.rem(j, RING)
        cols = half_at(side, half, which)
        return remote(grad.at[r, :, cols], grad.at[r, :, cols], four_send.at[s], four_recv.at[r], zn)

    def out_copy(ref, row, j):
        return pltpu.make_async_copy(grad.at[lax.rem(j, RING)], ref.at[pl.ds(row, ROWS), :],
                                     out_sem.at[lax.rem(j, SEND_SLOTS)])

    norm_zero = remote(norm_part.at[:, :, 1 - c], norm_a, norm_send.at[0], norm_recv.at[0], core)
    norm_one = remote(norm_a.at[:, 1 - x], norm_b, norm_send.at[1], norm_recv.at[1], xn)
    norm_two = remote(norm_b.at[1 - y], norm_c, norm_send.at[2], norm_recv.at[2], yn)
    norm_three = remote(norm_c, norm_d, norm_send.at[3], norm_recv.at[3], zn)

    def when_in(j, body):
        pl.when(jnp.logical_and(j >= 0, j < total))(functools.partial(body, j))

    def after(j, slots, copies):
        @pl.when(j >= slots)
        def _():
            on_plan(j - slots, lambda *args: wait_send(copies(*args)))

    def start(copies):
        for copy in copies:
            copy.start()

    def wait_send(copies):
        for copy in copies:
            copy.wait_send()

    def stage_issue(j):
        after(j, P_SLOTS, ones)

        @pl.when(j >= R_SLOTS)
        def _():
            wait_send(zero_copies(emb, 0, j - R_SLOTS))
            pl.semaphore_wait(credit, 1)

        def body(ref, _, row):
            start(zero_copies(ref, row, j))
            load_copy(ref, row, j).start()

        on_rows(j, body)

    def stage_one(j):
        load_copy(emb, 0, j).wait()
        zero_copies(emb, 0, j)[0].wait_recv()
        part[lax.rem(j, P_SLOTS), :, :, :, CUT:] += recv_zero[lax.rem(j, R_SLOTS), :, :, :, CUT:]
        on_plan(j, lambda *args: start(ones(*args)[:1]))

    def stage_one_more(j):
        zero_copies(emb, 0, j)[1].wait_recv()
        part[lax.rem(j, P_SLOTS), :, :, :, :CUT] += recv_zero[lax.rem(j, R_SLOTS), :, :, :, :CUT]

        @pl.when(j + R_SLOTS < total)
        def _():
            pl.semaphore_signal(credit, inc=1, device_id=core, device_id_type=MESH)

        on_plan(j, lambda *args: start(ones(*args)[1:]))

    def stage_two(j):
        after(j, SEND_SLOTS, lambda *args: twos(*args) + (two_c_even(*args),))

        def body(j, side, half):
            s, r = lax.rem(j, P_SLOTS), lax.rem(j, RING)
            even = lax.rem(j, 2) == 0
            for copy in ones(j, side, half):
                copy.wait_recv()
            zc[r, :, :, :, :half] += part[s, :, :, :, half_at(side, half, z)]
            xa[r, :, :, :side] += part[s, :, x, :, :side]
            yb[r, :, :, :side] += part[s, y, :, :, side:2 * side]
            pl.when(even)(lambda: two_c_even(j, side, half).start())
            pl.when(jnp.logical_not(even))(lambda: two_c_odd(j, side, half).start())
            start(twos(j, side, half))

        on_plan(j, body)

    def stage_three(j):
        after(j, SEND_SLOTS, lambda *args: (three_ab(*args), three_c(*args)))

        def body(j, side, half):
            r = lax.rem(j, RING)
            even = lax.rem(j, 2) == 0
            for copy in twos(j, side, half) + (two_c_even(j, side, half),):
                copy.wait_recv()

            @pl.when(even)
            def _():
                wc[r, :, :, :half] += zc[r, :, x, :, :half]

            @pl.when(jnp.logical_not(even))
            def _():
                wc[r, :, :, :half] += zc[r, y, :, :, :half]

            mid[r, :, :side] += xa[r, y, :, :side]
            mid[r, :, side:2 * side] += yb[r, x, :, :side]
            start((three_c(j, side, half), three_ab(j, side, half)))

        on_plan(j, body)

    def stage_four(j):
        after(j, SEND_SLOTS, lambda *args: (four(*args, z),))

        def body(j, side, half):
            r, odd = lax.rem(j, RING), lax.rem(j, 2)
            here = y + odd * (x - y)
            three_c(j, side, half).wait_recv()
            grad[r, :, half_at(side, half, z)] = (tc[r, :, :half] + wc[r, here, :, :half]) * (1.0 / 16.0)
            four(j, side, half, z).start()

        on_plan(j, body)

    def stage_five(j):
        def body(j, side, half):
            r = lax.rem(j, RING)
            three_ab(j, side, half).wait_recv()
            both = (grad[r, :, :2 * side] + mid[r, :, :2 * side]) * (1.0 / 16.0)
            grad[r, :, :2 * side] = both
            square[:, :2 * side] += both * both
            four(j, side, half, 1 - z).wait_recv()
            rest = grad[r, :, 2 * side:]
            square[:, 2 * side:] += rest * rest

        on_plan(j, body)

        @pl.when(j >= SEND_SLOTS)
        def _():
            out_copy(emb_out, 0, j - SEND_SLOTS).wait()

        def store(_, ref, row):
            out_copy(ref, row, j).start()

        on_rows(j, store)

    def trip(it, carry):
        when_in(it + 1, stage_issue)
        when_in(it - LAG_ZERO, stage_one)
        when_in(it - LAG_ZERO - 4 * LAG, stage_five)
        when_in(it - LAG_ZERO - 3 * LAG, stage_four)
        when_in(it - LAG_ZERO - 2 * LAG, stage_three)
        when_in(it - LAG_ZERO - LAG, stage_two)
        when_in(it - LAG_ZERO, stage_one_more)

        @pl.when(it == 5)
        def _():
            norm_copy.wait()
            for k in range(8):
                for row in range(NORM_ROWS):
                    norm_part[k // 4, (k // 2) % 2, k % 2, row:row + 1, :NORM_COLS] = norm_in[row, :, k * NORM_COLS:(k + 1) * NORM_COLS]
            norm_zero.start()

        @pl.when(it == 8)
        def _():
            norm_zero.wait_recv()
            norm_a[...] += norm_part[:, :, c]
            norm_one.start()

        @pl.when(it == 12)
        def _():
            norm_one.wait_recv()
            norm_b[...] += norm_a[:, x]
            norm_two.start()

        @pl.when(it == 16)
        def _():
            norm_two.wait_recv()
            norm_c[...] += norm_b[y]
            norm_three.start()

        @pl.when(it == 20)
        def _():
            norm_three.wait_recv()
            norm_d[...] = (norm_d[...] + norm_c[...]) * (1.0 / 16.0)
            norm_out[...] = norm_d[...]
            norm_sq = norm_d[...] * norm_d[...]
            square[:, :NORM_PAD[1]] += norm_sq[:ROWS] + norm_sq[ROWS:]

        return carry

    ahead = pltpu.make_async_copy(emb.at[:, :, 1 - c, pl.ds(0, ROWS), :], part.at[P_SLOTS - 1], load_sem.at[P_SLOTS - 1])
    ahead.start()
    load_copy(emb, 0, 0).start()
    norm_part[...] = jnp.zeros_like(norm_part)
    square[...] = jnp.zeros_like(square)
    pl.semaphore_wait(barrier, 4)
    ahead.wait()
    start(exchange(part.at[P_SLOTS - 1], 0))
    lax.fori_loop(0, total + LAG_ZERO + 4 * LAG, trip, 0)

    value = jnp.full((8, 128), jnp.sum(square[...]), F32)
    sum_send[...] = value
    sum_recv[f] = value
    sums = [remote(sum_send, sum_recv.at[f], sum_ssem.at[k], sum_rsem.at[f], dev) for k, dev in enumerate(peers)]
    start(sums)
    wait_send((norm_zero, norm_one, norm_two, norm_three))

    def drain(slots, copies):
        def body(j, carry):
            on_plan(j, lambda *args: wait_send(copies(*args)))
            return carry
        lax.fori_loop(total - slots, total, body, 0)

    drain(P_SLOTS, ones)
    drain(R_SLOTS, lambda j, side, half: zero_copies(emb, 0, j))
    drain(SEND_SLOTS, lambda *args: twos(*args) + (two_c_even(*args), three_ab(*args), three_c(*args), four(*args, z)))

    def last(j, carry):
        out_copy(emb_out, 0, j).wait()
        return carry

    lax.fori_loop(total - SEND_SLOTS, total, last, 0)

    for k in range(1, 8):
        s = lax.rem(f + k, 8)
        remote(sum_send, sum_recv.at[s], sum_ssem.at[0], sum_rsem.at[s], core).wait_recv()
    whole = sum_recv[0]
    for k in range(1, 8):
        whole = whole + sum_recv[k]
    scale_out[...] = jnp.minimum(1.0, CLIP_NORM / jnp.sqrt(whole))
    wait_send(sums)


def reduce_grads(emb_grad, mat_grad, norm_grad):
    emb_rows = emb_grad.shape[0] // 8
    mat_rows = mat_grad.shape[0] // 8
    counts = (emb_rows // ROWS, mat_rows // ROWS)
    dma = pltpu.SemaphoreType.DMA
    scratch = [
        pltpu.VMEM((P_SLOTS, 2, 2, ROWS, WIDTH), F32),
        pltpu.VMEM((R_SLOTS, 2, 2, ROWS, WIDTH), F32),
        pltpu.VMEM((RING, 2, ROWS, SIDE_MAX), F32),
        pltpu.VMEM((RING, 2, ROWS, SIDE_MAX), F32),
        pltpu.VMEM((RING, 2, 2, ROWS, HALF_MAX), F32),
        pltpu.VMEM((RING, ROWS, 2 * SIDE_MAX), F32),
        pltpu.VMEM((RING, 2, ROWS, HALF_MAX), F32),
        pltpu.VMEM((RING, ROWS, HALF_MAX), F32),
        pltpu.VMEM((RING, ROWS, WIDTH), F32),
        pltpu.VMEM((ROWS, WIDTH), F32),
        pltpu.VMEM((NORM_ROWS, 1, WIDTH), F32),
        pltpu.VMEM((2, 2, 2) + NORM_PAD, F32),
        pltpu.VMEM((2, 2) + NORM_PAD, F32),
        pltpu.VMEM((2,) + NORM_PAD, F32),
        pltpu.VMEM(NORM_PAD, F32),
        pltpu.VMEM(NORM_PAD, F32),
        pltpu.VMEM((8, 128), F32),
        pltpu.VMEM((8, 8, 128), F32),
        dma((P_SLOTS,)), dma((2, R_SLOTS)), dma((2, R_SLOTS)), pltpu.SemaphoreType.REGULAR,
        dma((3, P_SLOTS)), dma((3, RING)), dma((3, SEND_SLOTS)), dma((3, RING)),
        dma((2, SEND_SLOTS)), dma((2, RING)), dma((SEND_SLOTS,)), dma((RING,)), dma((SEND_SLOTS,)),
        dma, dma((4,)), dma((4,)), dma((7,)), dma((8,)),
    ]
    hbm = pl.BlockSpec(memory_space=pl.ANY)
    vmem = pl.BlockSpec(memory_space=pltpu.VMEM)
    return pl.pallas_call(
        functools.partial(reduce_kernel, counts),
        out_shape=(
            jax.ShapeDtypeStruct((emb_rows, WIDTH), F32),
            jax.ShapeDtypeStruct((mat_rows, WIDTH), F32),
            jax.ShapeDtypeStruct(NORM_PAD, F32),
            jax.ShapeDtypeStruct((8, 128), F32),
        ),
        in_specs=[pl.BlockSpec(memory_space=pltpu.HBM)] * 3,
        out_specs=(hbm, hbm, vmem, vmem),
        scratch_shapes=scratch,
        compiler_params=pltpu.CompilerParams(
            collective_id=0, has_side_effects=True, vmem_limit_bytes=28 * 1024 * 1024
        ),
        name="reduce_grads",
    )(*(pltpu.with_memory_space_constraint(grad, pltpu.HBM) for grad in (
        emb_grad.reshape(2, 2, 2, emb_rows, WIDTH), mat_grad.reshape(2, 2, 2, mat_rows, WIDTH),
        norm_grad.reshape(NORM_ROWS, 1, WIDTH))))


BLOCK = 16
COLS = 384
SIDE = WIDTH // 2
STORE_SLOTS = 4


def adamw_block(grad, param, mom, var, decay_rate):
    new_mom = BETA_ONE * mom + (1.0 - BETA_ONE) * grad
    new_var = BETA_TWO * var + (1.0 - BETA_TWO) * grad * grad
    root = math.sqrt(1.0 - BETA_TWO ** ADAM_STEP)
    step_dir = new_mom / (jnp.sqrt(new_var) + ADAM_EPS * root)
    rate = LEARN_RATE * root / (1.0 - BETA_ONE ** ADAM_STEP)
    return param - (rate * step_dir + (LEARN_RATE * decay_rate) * param), new_mom, new_var


def adamw_kernel(scale, eg, ep, em, ev, mg, mp, mm, mv, ng, np_, nm, nv,
                 ep_out, em_out, ev_out, eb_out, mp_out, mm_out, mv_out, mb_out, np_out, nm_out, nv_out, nb_out,
                 p_buf, m_buf, v_buf, b_buf, n_bufs, nb_buf, sems, n_sems):
    clip = scale[0:1, 0:1]

    def copies(outs, slot, row, side):
        cols = pl.ds(side * SIDE, SIDE)
        return [pltpu.make_async_copy(buf.at[slot, side], out.at[pl.ds(row, BLOCK), cols], sems.at[k, slot, side])
                for k, (buf, out) in enumerate(zip((p_buf, m_buf, v_buf, b_buf), outs))]

    emb_outs = (ep_out, em_out, ev_out, eb_out)
    mat_outs = (mp_out, mm_out, mv_out, mb_out)
    emb_blocks = eg.shape[0] // BLOCK
    mat_blocks = mg.shape[0] // BLOCK

    def run(first, count, ins, outs):
        def body(i, carry):
            j = first + i
            slot = lax.rem(j, STORE_SLOTS)

            row = pl.multiple_of(i * BLOCK, BLOCK)
            for side in range(2):
                @pl.when(j >= STORE_SLOTS)
                def _():
                    for copy in copies(emb_outs, slot, 0, side):
                        copy.wait()

                for col in range(0, SIDE, COLS):
                    here, cols = pl.ds(col, COLS), pl.ds(side * SIDE + col, COLS)
                    g, p, m, v = (ref[pl.ds(row, BLOCK), cols] for ref in ins)
                    new_p, new_m, new_v = adamw_block(g * clip, p, m, v, WEIGHT_DECAY)
                    p_buf[slot, side, :, here] = new_p
                    m_buf[slot, side, :, here] = new_m
                    v_buf[slot, side, :, here] = new_v
                    b_buf[slot, side, :, here] = new_p.astype(jnp.bfloat16)
                for copy in copies(outs, slot, row, side):
                    copy.start()
            return carry

        lax.fori_loop(0, count, body, 0)

    run(0, emb_blocks, (eg, ep, em, ev), emb_outs)
    run(emb_blocks, mat_blocks, (mg, mp, mm, mv), mat_outs)
    new_p, new_m, new_v = adamw_block(ng[:NORM_ROWS, :NORM_COLS] * clip, np_[...], nm[...], nv[...], 0.0)
    for k, value in enumerate((new_p, new_m, new_v)):
        n_bufs[k] = value
    nb_buf[...] = new_p.astype(jnp.bfloat16)
    norm_copies = [pltpu.make_async_copy(n_bufs.at[k], out, n_sems.at[k]) for k, out in enumerate((np_out, nm_out, nv_out))]
    norm_copies.append(pltpu.make_async_copy(nb_buf, nb_out, n_sems.at[3]))
    for copy in norm_copies:
        copy.start()
    for slot in range(STORE_SLOTS):
        for side in range(2):
            for copy in copies(emb_outs, slot, 0, side):
                copy.wait()
    for copy in norm_copies:
        copy.wait()


def adamw(scale, emb, mat, norm):
    shapes = []
    for ref in (emb[1], mat[1], norm[1]):
        shapes += [jax.ShapeDtypeStruct(ref.shape, F32)] * 3 + [jax.ShapeDtypeStruct(ref.shape, jnp.bfloat16)]
    buf = (STORE_SLOTS, 2, BLOCK, SIDE)
    vmem = pl.BlockSpec(memory_space=pltpu.VMEM)
    hbm = pl.BlockSpec(memory_space=pl.ANY)
    elements = emb[1].size + mat[1].size
    return pl.pallas_call(
        adamw_kernel,
        out_shape=tuple(shapes),
        in_specs=[vmem] * 13,
        out_specs=(hbm,) * 12,
        scratch_shapes=[
            pltpu.VMEM(buf, F32), pltpu.VMEM(buf, F32), pltpu.VMEM(buf, F32), pltpu.VMEM(buf, jnp.bfloat16),
            pltpu.VMEM((3, NORM_ROWS, NORM_COLS), F32), pltpu.VMEM((NORM_ROWS, NORM_COLS), jnp.bfloat16),
            pltpu.SemaphoreType.DMA((4, STORE_SLOTS, 2)), pltpu.SemaphoreType.DMA((4,)),
        ],
        compiler_params=pltpu.CompilerParams(vmem_limit_bytes=8 * 1024 * 1024),
        cost_estimate=pl.CostEstimate(flops=20 * elements, bytes_accessed=30 * elements, transcendentals=2 * elements),
        name="adamw",
    )(scale, *emb, *mat, *norm)


def solution(mesh):
    def local_step(emb_grad, mat_grad, norm_grad, emb_param, emb_mom, emb_var, mat_param, mat_mom, mat_var, norm_param, norm_mom, norm_var):
        emb_mean, mat_mean, norm_mean, scale = reduce_grads(emb_grad[0, 0], mat_grad[0, 0], norm_grad[0, 0])
        return adamw(scale, (emb_mean, emb_param, emb_mom, emb_var), (mat_mean, mat_param, mat_mom, mat_var),
                     (norm_mean, norm_param, norm_mom, norm_var))

    grad_spec = P("dp", "fsdp", None, None)
    row_spec = P("fsdp", None)
    col_spec = P(None, "fsdp")
    in_list = (grad_spec, grad_spec, grad_spec, row_spec, row_spec, row_spec, row_spec, row_spec, row_spec, col_spec, col_spec, col_spec)
    out_list = (row_spec, row_spec, row_spec, row_spec, row_spec, row_spec, row_spec, row_spec, col_spec, col_spec, col_spec, col_spec)
    return jax.shard_map(local_step, mesh=mesh, in_specs=in_list, out_specs=out_list, check_vma=False)
```
